32 devices in a mesh: dp: 2 (over x), expert: 16 (over z, y, core).
Axes of the slice: x: 2, y: 2, z: 4, core: 2. Of those that a mesh axis runs over, the one named last changes fastest.
Arguments:
- tokens: bfloat16 [4096, 1024], P(('dp', 'expert')), may hold values from -6 to 6
- out_grad: bfloat16 [4096, 1024], P(('dp', 'expert')), may hold values from -6 to 6
- expert_ids: int32 [4096, 3], P(('dp', 'expert')), may hold values from 0 to 15, all different within a row; in each aligned block of 128 rows (0 to 127, 128 to 255, ...) at most 30 rows name the same one
- gate_probs: float32 [4096, 3], P(('dp', 'expert')), may hold values from 0.1 to 0.6
- saved_pre: bfloat16 [2, 16, 480, 1536], P('dp', 'expert'), may hold values from -6 to 6
- gate_weight: bfloat16 [16, 1024, 768], P('expert', 'dp'), may hold values from -0.1875 to 0.1875
- up_weight: bfloat16 [16, 1024, 768], P('expert', 'dp'), may hold values from -0.1875 to 0.1875
- down_weight: bfloat16 [16, 1024, 768], P('expert', 'dp'), may hold values from -0.21875 to 0.21875
- basis: bfloat16 [16, 1024, 256], P('expert', 'dp'), may hold values from -0.1875 to 0.1875
Outputs:
- in_grad: bfloat16 [4096, 1024], P(('dp', 'expert'))
- proj_grads: float32 [16, 3, 256, 768], P('expert', None, 'dp')
The draws below stay inside these ranges and needn't reach their ends.
Inputs may be any that keep to these rules, and one draw needn't show every extreme that they name: `expert_ids`: each token names 3 different experts. The rows of one device name one expert at most 30 times, and on some devices some expert exactly 30 times.
All inputs are finite; a program needn't handle non-finite values.
Results may differ from the reference program's by a relative error of at most 0.0091.
Values may be sent and summed in bfloat16 or wider, within the bound.
A program may use at most 64 MiB of HBM per device.

```python
import math
import jax
import jax.numpy as jnp
import numpy as np
from jax import lax

D = 1024
FF = 768
RANK = 256
TOPK = 3
TOK_DEV = 128
EXPERTS = 16
CAP = 30
SLOTS = 480
TOKENS = 4096
N_DP = 2
N_EXPERT = 16


def block_scale(stream_key, extent, cuts, smallest, largest):
    loudness, own = 1.0, jax.random.fold_in(stream_key, 6)
    for dim, blocks in cuts:
        draws = jnp.exp(jax.random.uniform(jax.random.fold_in(own, dim), (blocks,), jnp.float32, smallest / len(cuts), largest / len(cuts)))
        loudness = loudness * jnp.repeat(draws, extent[dim] // blocks).reshape([-1 if axis == dim else 1 for axis in range(len(extent))])
    return loudness


def assign_block(own_key, own, number, rows, amount, top, reach, slope):
    order = jax.random.permutation(own_key, amount)
    packed, ordinary = load_shares(amount, rows * top, reach, slope, True), load_shares(amount, rows * top, reach, slope, False)
    places = jnp.arange(amount)

    def named(sizes, rotation):
        used = int((sizes > 0).sum())
        fixed = max(1, used // 4)
        moved = fixed + (places - fixed + rotation * (used - fixed)) % max(1, amount - fixed)
        return jnp.zeros((amount,), jnp.int32).at[order[jnp.where(places < fixed, places, moved)]].set(jnp.asarray(sizes, jnp.int32))

    sizes = jnp.where(number % 4 == 0, named(packed, number // 4), named(ordinary, number - number // 4 - 1))
    mixed = jax.random.permutation(jax.random.fold_in(own, 3), amount)
    source_of, sink = mixed[0:amount // 2 * 2:2], mixed[1:amount // 2 * 2:2]
    margin = jnp.minimum(sizes[source_of] - 1, reach - sizes[sink]) // 2
    margin = jnp.where((source_of == order[0]) | (sink == order[0]) | (sizes[sink] == 0), 0, jnp.maximum(margin, 0))
    moved = jax.random.randint(jax.random.fold_in(own, 4), (amount // 2,), 0, 1 << 20) % (margin + 1)
    sizes = sizes.at[source_of].add(-moved).at[sink].add(moved)
    members = jnp.searchsorted(jnp.cumsum(sizes), jnp.arange(rows * top), side="right").astype(jnp.int32)
    grid = members.reshape(top, rows).T
    grid = grid[jax.random.permutation(jax.random.fold_in(own, 1), rows)]
    rotation = jax.random.randint(jax.random.fold_in(own, 2), (rows, 1), 0, top)
    return jnp.take_along_axis(grid, (jnp.arange(top)[None, :] + rotation) % top, axis=1)


def load_shares(count, total, limit, skew, full):
    portions = [(1 << 20) // math.isqrt(grade ** skew) + 1 for grade in range(1, count + 1)]
    largest = limit if full else min(limit, max(-(-total // count), total * portions[0] // sum(portions)))
    least = 1 if total - largest >= count - 1 else 0
    counts, surplus = [largest] + [least] * (count - 1), total - largest - least * (count - 1)
    while surplus > 0:
        candidates = [i for i in range(1, count) if counts[i] < largest] or [i for i in range(1, count) if counts[i] < limit]
        mass, budget = sum([portions[i] for i in candidates]), surplus
        for i in candidates:
            addition = min(limit - counts[i], max(1, budget * portions[i] // mass), surplus)
            counts[i] = counts[i] + addition
            surplus = surplus - addition
    return np.array(counts)


def scatter_about(rng, dims, width, reach, shards=(), kind=jnp.bfloat16):
    entries = width * jax.random.normal(rng, dims, jnp.float32)
    if shards:
        entries = entries * block_scale(rng, dims, shards, -0.22, 0.18)
    return jnp.clip(entries, -reach, reach).astype(kind)


def setup_inputs(seed: int = 0) -> dict:
    arg_keys = jax.random.split(jax.random.key(seed), 10)
    tokens = scatter_about(arg_keys[0], (TOKENS, D), 1.0, 6.0, ((0, 32),))
    out_grad = scatter_about(arg_keys[1], (TOKENS, D), 1.0, 6.0, ((0, 32),))
    expert_ids_keys = jax.random.split(jax.random.fold_in(arg_keys[2], 1), TOKENS // TOK_DEV)
    expert_ids_turns = jax.random.permutation(jax.random.fold_in(arg_keys[2], 3), TOKENS // TOK_DEV)
    expert_ids = jax.vmap(lambda own, number: assign_block(jax.random.fold_in(arg_keys[2], 2), own, number, TOK_DEV, EXPERTS, TOPK, CAP, 2))(expert_ids_keys, expert_ids_turns).reshape((TOKENS, TOPK))
    gate_probs = jnp.clip(0.1 + 0.5 * jax.random.uniform(arg_keys[3], (TOKENS, TOPK), jnp.float32) ** block_scale(arg_keys[3], (TOKENS, TOPK), ((0, 32),), -0.2, 0.2), 0.1, 0.6)
    saved_pre = scatter_about(arg_keys[4], (N_DP, EXPERTS, SLOTS, 2 * FF), 1.5, 6.0, ((0, 2), (1, 16)))
    gate_weight = scatter_about(arg_keys[5], (EXPERTS, D, FF), D ** -0.5, 0.1875, ((0, 16), (1, 2)))
    up_weight = scatter_about(arg_keys[6], (EXPERTS, D, FF), D ** -0.5, 0.1875, ((0, 16), (1, 2)))
    down_weight = scatter_about(arg_keys[7], (EXPERTS, D, FF), FF ** -0.5, 0.21875, ((0, 16), (1, 2)))
    basis = scatter_about(arg_keys[8], (EXPERTS, D, RANK), D ** -0.5, 0.1875, ((0, 16), (1, 2)))
    return {"tokens": tokens, "out_grad": out_grad, "expert_ids": expert_ids, "gate_probs": gate_probs, "saved_pre": saved_pre, "gate_weight": gate_weight, "up_weight": up_weight, "down_weight": down_weight, "basis": basis}


def slot_tables(expert_ids):
    devices = N_DP * N_EXPERT
    ids = expert_ids.reshape(devices, TOK_DEV, TOPK)
    onehot = (ids[:, :, :, None] == jnp.arange(EXPERTS, dtype=jnp.int32)[None, None, None, :]).astype(jnp.int32)
    per_token = jnp.sum(onehot, axis=2)
    before = jnp.cumsum(per_token, axis=1) - per_token
    position = jnp.sum(onehot * before[:, :, None, :], axis=3)
    device = jnp.arange(devices, dtype=jnp.int32)[:, None, None]
    group = device // N_EXPERT
    source = device % N_EXPERT
    flat = (group * EXPERTS + ids) * SLOTS + source * CAP + position
    token_index = device * TOK_DEV + jnp.arange(TOK_DEV, dtype=jnp.int32)[None, :, None]
    token_index = jnp.broadcast_to(token_index, ids.shape)
    choice_index = jnp.broadcast_to(jnp.arange(TOPK, dtype=jnp.int32)[None, None, :], ids.shape)
    table_token = jnp.full((N_DP * EXPERTS * SLOTS,), -1, jnp.int32).at[flat.reshape(-1)].set(token_index.reshape(-1))
    table_choice = jnp.zeros((N_DP * EXPERTS * SLOTS,), jnp.int32).at[flat.reshape(-1)].set(choice_index.reshape(-1))
    return table_token.reshape(N_DP, EXPERTS, SLOTS), table_choice.reshape(N_DP, EXPERTS, SLOTS)


def reference(tokens, out_grad, expert_ids, gate_probs, saved_pre, gate_weight, up_weight, down_weight, basis):
    table_token, table_choice = slot_tables(expert_ids)

    def per_expert(accum, expert):
        w_gate = gate_weight[expert]
        w_up = up_weight[expert]
        w_down = down_weight[expert]
        w_basis = basis[expert]

        def per_group(carry, group):
            total, projected = carry
            taken = table_token[group, expert]
            chosen = table_choice[group, expert]
            filled = taken >= 0
            picked = jnp.maximum(taken, 0).astype(jnp.int32)
            x_rows = jnp.where(filled[:, None], tokens[picked], jnp.zeros((), jnp.bfloat16))
            weight_pick = gate_probs[picked, chosen]
            scaled = (out_grad[picked].astype(jnp.float32) * weight_pick[:, None]).astype(jnp.bfloat16)
            dy_rows = jnp.where(filled[:, None], scaled, jnp.zeros((), jnp.bfloat16))
            pre = saved_pre[group, expert].astype(jnp.float32)
            gate_pre = pre[:, :FF]
            up_pre = pre[:, FF:]
            hidden_grad = jnp.dot(dy_rows, w_down, preferred_element_type=jnp.float32)
            x_proj = jnp.dot(x_rows, w_basis, preferred_element_type=jnp.float32).astype(jnp.bfloat16)
            dy_proj = jnp.dot(dy_rows, w_basis, preferred_element_type=jnp.float32).astype(jnp.bfloat16)
            sig = jax.nn.sigmoid(gate_pre)
            hid = (gate_pre * sig * up_pre).astype(jnp.bfloat16)
            up_grad = (hidden_grad * gate_pre * sig).astype(jnp.bfloat16)
            gate_grad = (hidden_grad * up_pre * sig * (1.0 + gate_pre * (1.0 - sig))).astype(jnp.bfloat16)
            terms = jnp.stack([
                jnp.dot(x_proj.T, gate_grad, preferred_element_type=jnp.float32),
                jnp.dot(x_proj.T, up_grad, preferred_element_type=jnp.float32),
                jnp.dot(dy_proj.T, hid, preferred_element_type=jnp.float32)])
            row_grad = jnp.dot(gate_grad, w_gate.T, preferred_element_type=jnp.float32)
            row_grad = row_grad + jnp.dot(up_grad, w_up.T, preferred_element_type=jnp.float32)
            row_grad = row_grad.astype(jnp.bfloat16).astype(jnp.float32)
            row_grad = jnp.where(filled[:, None], row_grad, jnp.zeros((), jnp.float32))
            total = total.at[picked].add(row_grad)
            return (total, projected + terms), None

        start = (accum, jnp.zeros((3, RANK, FF), jnp.float32))
        (accum, projected), unused = lax.scan(per_group, start, jnp.arange(N_DP, dtype=jnp.int32))
        return accum, projected

    accum = jnp.zeros((TOKENS, D), jnp.float32)
    accum, proj_grads = lax.scan(per_expert, accum, jnp.arange(EXPERTS, dtype=jnp.int32))
    return accum.astype(jnp.bfloat16), proj_grads
```

```python
import functools
import jax
import jax.numpy as jnp
from jax import lax
from jax.experimental import pallas as pl
from jax.experimental.pallas import tpu as pltpu
from jax.sharding import PartitionSpec as P

MESH = pl.DeviceIdType.MESH
F32 = jnp.float32
BF16 = jnp.bfloat16
LEVELS = 4


def dot(left, right, dims):
    return lax.dot_general(left, right, (dims, ((), ())), preferred_element_type=F32)


NN = ((1,), (0,))
TN = ((0,), (0,))
NT = ((1,), (1,))


def kernel(
    n_dp, n_ex, cap, cp,
    ids, probs, tok_h, og_h, pre_h, gw_h, uw_h, dw, bs,
    in_h, proj_h,
    tok, og, tok2, ids2, idsd, pick_v, sx, sg, rx, rg, dyc, spr, dfull, bfull, gw, uw, pre,
    act_a, act_b, hid, gu, px, pdy, rs, rr, in_v, psend, prec, term, total,
    local_sem, pre_sem, dy_s, dy_r, x_s, x_r, relay_s, relay_r, down_s, down_r, base_s, base_r,
    gu_s, gu_r, ret_s, ret_r, px_s, px_r, proj_s, proj_r, in_s, in_r, ids_s, ids_r, out_s,
):
    my_dp = lax.axis_index("dp")
    me = lax.axis_index("expert")
    rows = n_ex * cp
    half = n_ex // 2
    nl = n_ex // LEVELS
    lrows = nl * cp
    lcap = nl * cap
    tokens, width = tok.shape
    topk = ids.shape[0]
    hidden = dfull.shape[1]
    part = width // n_dp
    rank = bfull.shape[1]
    rk = rank // n_dp
    shift = cp.bit_length() - 1
    fw = 256

    z = lax.div(me, nl)
    spot = lax.rem(me, nl)
    mate = lax.rem(me + half, n_ex)
    half0 = lax.div(me, half) * half
    levels = [z + 1 - 2 * lax.rem(z, 2), lax.rem(z + 2, LEVELS), LEVELS - 1 - z, z]
    own = LEVELS - 1

    def block(owner):
        return pl.ds(pl.multiple_of(owner * cp, cp), cp)

    def wpart(owner):
        return pl.ds(pl.multiple_of(owner * part, part), part)

    def rpart(owner):
        return pl.ds(pl.multiple_of(owner * rk, rk), rk)

    def rank_cols(owner):
        line = lax.broadcasted_iota(jnp.int32, (rank, rk), 0)
        lane = lax.broadcasted_iota(jnp.int32, (rank, rk), 1) + owner * rk
        return jnp.where(line == lane, one, zero).astype(BF16)

    def lpart(j):
        return pl.ds(pl.multiple_of(levels[j] * lrows, lrows), lrows)

    def ex_peer(k):
        return lax.rem(me + k, n_ex)

    def half_peer(k):
        return half0 + lax.rem(me - half0 + k, half)

    def in_level(j, t):
        return levels[j] * nl + lax.rem(spot + t, nl)

    def dp_peer(i):
        return lax.rem(my_dp + i, n_dp)

    def dp_from(i):
        return lax.rem(my_dp + n_dp - i, n_dp)

    pad = gu.shape[3] - lcap
    if pad:
        for j in range(LEVELS):
            pre[j, lcap:, :] = jnp.zeros((pad, 2 * hidden), BF16)
            for i in range(1, n_dp):
                for s in range(2):
                    gu[i, j, s, lcap:, :] = jnp.zeros((pad, hidden), BF16)

    barrier = pltpu.get_barrier_semaphore()

    for i in range(1, n_dp):
        pl.semaphore_signal(barrier, inc=1, device_id={"dp": dp_peer(i)}, device_id_type=MESH)

    @pl.loop(1, n_ex)
    def _(k):
        pl.semaphore_signal(barrier, inc=1, device_id={"expert": ex_peer(k)}, device_id_type=MESH)

    local = [
        pltpu.make_async_copy(og_h, og, local_sem.at[0]),
        pltpu.make_async_copy(tok_h, tok, local_sem.at[1]),
        pltpu.make_async_copy(dw.at[0], dfull.at[wpart(my_dp)], local_sem.at[2]),
        pltpu.make_async_copy(bs.at[0], bfull.at[wpart(my_dp)], local_sem.at[3]),
        pltpu.make_async_copy(gw_h.at[0], gw, local_sem.at[4]),
        pltpu.make_async_copy(uw_h.at[0], uw, local_sem.at[5]),
    ]
    pre_copy = []
    for j in range(LEVELS):
        src = pl.ds(pl.multiple_of(levels[j] * lcap, 8), lcap)
        pre_copy.append(
            pltpu.make_async_copy(pre_h.at[0, 0, src], pre.at[j, pl.ds(0, lcap)], pre_sem.at[j])
        )
    for copy in local[:2] + pre_copy + local[2:]:
        copy.start()

    one, zero = jnp.ones((), F32), jnp.zeros((), F32)
    earlier = lax.broadcasted_iota(jnp.int32, (tokens, tokens), 0) < lax.broadcasted_iota(
        jnp.int32, (tokens, tokens), 1
    )
    earlier = jnp.where(earlier, one, zero).astype(BF16)

    def pick_of(names_of, first, count):
        line = lax.broadcasted_iota(jnp.int32, (count, tokens), 0)
        line_expert = lax.shift_right_logical(line, shift) + first
        line_slot = lax.bitwise_and(line, cp - 1)
        names = [names_of[k : k + 1, :] == line_expert for k in range(topk)]
        any_name = functools.reduce(jnp.logical_or, names)
        named = jnp.where(any_name, one, zero).astype(BF16)
        before = dot(named, earlier, NN)
        at_slot = before == line_slot.astype(F32)
        pick = jnp.where(jnp.logical_and(any_name, at_slot), one, zero).astype(BF16)
        return pick, names, at_slot

    pick, names, at_slot = pick_of(ids, 0, rows)
    pick_v[0] = pick
    weights = functools.reduce(
        jnp.add, [jnp.where(name, probs[k : k + 1, :], zero) for k, name in enumerate(names)]
    )
    weight = jnp.sum(jnp.where(at_slot, weights, zero), axis=1, keepdims=True)

    pl.semaphore_wait(barrier, n_ex - 1 + n_dp - 1)

    def down_copy(i, owner, peer):
        return pltpu.make_async_remote_copy(
            dw.at[0], dfull.at[wpart(owner)], down_s.at[i], down_r.at[i],
            device_id={"dp": peer}, device_id_type=MESH,
        )

    def base_copy(i, owner, peer):
        return pltpu.make_async_remote_copy(
            bs.at[0], bfull.at[wpart(owner)], base_s.at[i], base_r.at[i],
            device_id={"dp": peer}, device_id_type=MESH,
        )

    def ids_copy(i, peer):
        return pltpu.make_async_remote_copy(
            ids, idsd.at[i - 1], ids_s.at[i], ids_r.at[i],
            device_id={"dp": peer}, device_id_type=MESH,
        )

    def mate_ids():
        return pltpu.make_async_remote_copy(
            ids, ids2, ids_s.at[0], ids_r.at[0], device_id={"expert": mate}, device_id_type=MESH
        )

    def mate_tok():
        return pltpu.make_async_remote_copy(
            tok, tok2, relay_s, relay_r, device_id={"expert": mate}, device_id_type=MESH
        )

    def dy_copy(peer, owner):
        return pltpu.make_async_remote_copy(
            sg.at[block(peer)], rg.at[block(owner)], dy_s.at[peer], dy_r.at[owner],
            device_id={"expert": peer}, device_id_type=MESH,
        )

    def x_copy(m, peer, owner):
        return pltpu.make_async_remote_copy(
            sx.at[m, block(peer - half0)], rx.at[block(owner)], x_s.at[m, peer - half0], x_r.at[owner],
            device_id={"expert": peer}, device_id_type=MESH,
        )

    def gu_copy(i, j, peer):
        used = pl.ds(0, lcap)
        return pltpu.make_async_remote_copy(
            gu.at[0, j, :, used], gu.at[i, j, :, used], gu_s.at[i, j], gu_r.at[i, j],
            device_id={"dp": peer}, device_id_type=MESH,
        )

    def px_copy(i, peer):
        return pltpu.make_async_remote_copy(
            px.at[i - 1], px.at[n_dp - 1 + i], px_s.at[i], px_r.at[i],
            device_id={"dp": peer}, device_id_type=MESH,
        )

    def ret_copy(i, j, peer, owner):
        return pltpu.make_async_remote_copy(
            rs.at[i, j, block(lax.rem(peer, nl))], rr.at[i, block(owner)],
            ret_s.at[i, peer], ret_r.at[i, owner],
            device_id={"expert": peer}, device_id_type=MESH,
        )

    def proj_copy(i, peer):
        return pltpu.make_async_remote_copy(
            psend.at[i - 1], prec.at[i - 1], proj_s.at[i], proj_r.at[i],
            device_id={"dp": peer}, device_id_type=MESH,
        )

    def in_copy(i, owner, peer):
        return pltpu.make_async_remote_copy(
            in_v.at[i], in_h.at[:, wpart(owner)], in_s.at[i], in_r.at[i],
            device_id={"dp": peer}, device_id_type=MESH,
        )

    for i in range(1, n_dp):
        down_copy(i, my_dp, dp_peer(i)).start()
    for i in range(1, n_dp):
        base_copy(i, my_dp, dp_peer(i)).start()
    mate_ids().start()
    for i in range(1, n_dp):
        ids_copy(i, dp_peer(i)).start()

    local[0].wait()
    sg[...] = (dot(pick, og[...], NN) * weight).astype(BF16)
    for j in range(LEVELS):

        @pl.loop(int(j == own), nl)
        def _(t, j=j):
            dy_copy(in_level(j, t), me).start()

    rg[block(me), :] = sg[block(me), :]

    local[1].wait()
    mate_tok().start()
    half_rows = pl.ds(pl.multiple_of(half0 * cp, cp), half * cp)
    sx[0] = dot(pick_v[0, half_rows], tok[...], NN).astype(BF16)

    @pl.loop(1, half)
    def _(k):
        x_copy(0, half_peer(k), me).start()

    rx[block(me), :] = sx[0, block(me - half0), :]

    grid = (gu.shape[3], lrows)
    line = lax.broadcasted_iota(jnp.int32, grid, 1)
    inner = lax.bitwise_and(line, cp - 1)
    target = lax.shift_right_logical(line, shift) * cap + inner
    spread = jnp.logical_and(target == lax.broadcasted_iota(jnp.int32, grid, 0), inner < cap)
    spr[...] = jnp.where(spread, one, zero).astype(BF16)

    for j in range(LEVELS):
        pre_copy[j].wait()
        for f in range(0, hidden, fw):
            cols = slice(f, f + fw)
            g = pre[j, :, f : f + fw].astype(F32)
            u = pre[j, :, hidden + f : hidden + f + fw].astype(F32)
            sig = jax.nn.sigmoid(g)
            gs = g * sig
            act_a[j, :, cols] = gs
            hid[j, :, cols] = (gs * u).astype(BF16)
            act_b[j, :, cols] = u * sig * (1.0 + g * (1.0 - sig))

    def row_grad(i, j):
        out = dot(gu[i, j, 0], gw[...], NT) + dot(gu[i, j, 1], uw[...], NT)
        rs[i, j] = dot(spr[...], out.astype(BF16), TN).astype(BF16)

        @pl.loop(int(j == own), nl)
        def _(t):
            ret_copy(i, j, in_level(j, t), me).start()

        if j == own:
            rr[i, block(me), :] = rs[i, j, block(spot), :]

    local[2].wait()
    for i in range(1, n_dp):
        down_copy(i, dp_from(i), dp_peer(i)).wait_recv()

    for j in range(LEVELS):

        @pl.loop(int(j == own), nl)
        def _(t, j=j):
            src = in_level(j, t)
            dy_copy(src, src).wait_recv()

        dyc[j] = dot(spr[...], rg[lpart(j), :], NN).astype(BF16)
        for f in range(0, hidden, fw):
            cols = slice(f, f + fw)
            hg = dot(dyc[j], dfull[:, cols], NN)
            gu[0, j, 1, :, cols] = (hg * act_a[j, :, cols]).astype(BF16)
            gu[0, j, 0, :, cols] = (hg * act_b[j, :, cols]).astype(BF16)
        for i in range(1, n_dp):
            gu_copy(i, j, dp_peer(i)).start()
        if j == 0:
            local[4].wait()
            local[5].wait()
        row_grad(0, j)

    local[3].wait()
    for i in range(1, n_dp):
        base_copy(i, dp_from(i), dp_peer(i)).wait_recv()
    for j in range(LEVELS):
        pdy[j] = dot(dyc[j], bfull[...], NN).astype(BF16)

    def project(left, right):
        return functools.reduce(jnp.add, [dot(left(j), right(j), TN) for j in range(LEVELS)])

    term[...] = project(lambda j: pdy[j], lambda j: hid[j])
    for i in range(1, n_dp):
        psend[i - 1] = term[rpart(dp_peer(i)), :].astype(BF16)
        proj_copy(i, dp_peer(i)).start()
    total[2] = term[rpart(my_dp), :]

    mate_ids().wait_recv()
    pick2, _, _ = pick_of(ids2, half0, half * cp)
    mate_tok().wait_recv()
    sx[1] = dot(pick2, tok2[...], NN).astype(BF16)

    @pl.loop(1, half)
    def _(k):
        x_copy(1, half_peer(k), mate).start()

    rx[block(mate), :] = sx[1, block(me - half0), :]

    for i in range(1, n_dp):
        ids_copy(i, dp_peer(i)).wait_recv()
        pick_v[i] = pick_of(idsd.at[i - 1], 0, rows)[0]

    def theirs(j):
        for i in range(1, n_dp):
            gu_copy(i, j, dp_peer(i)).wait_recv()
            row_grad(i, j)

    theirs(0)
    theirs(1)

    @pl.loop(1, n_ex)
    def _(k):
        src = ex_peer(k)

        @pl.when(src != mate)
        def _():
            x_copy(0, half0, src).wait_recv()

    for j in range(LEVELS):
        xj = dot(spr[...], rx[lpart(j), :], NN).astype(BF16)
        if rk % 128:
            xp = dot(xj, bfull[...], NN).astype(BF16)
        for i in range(n_dp):
            if rk % 128:
                pj = dot(xp, rank_cols(dp_peer(i)), NN)
            else:
                pj = dot(xj, bfull[:, rpart(dp_peer(i))], NN)
            px[(i + n_dp - 1) % n_dp, j] = pj.astype(BF16)
    for i in range(1, n_dp):
        px_copy(i, dp_peer(i)).start()

    theirs(2)

    def x_term(s, i):
        left = px.at[n_dp - 1 + i]
        return project(lambda j: left[j], lambda j: gu[i, j, s])

    for s in range(2):
        total[s] = x_term(s, 0)

    stored = []

    def combine(i):
        @pl.loop(1, n_ex)
        def _(k):
            src = ex_peer(k)
            ret_copy(i, 0, src, src).wait_recv()

        in_v[i] = dot(pick_v[i], rr[i], TN).astype(BF16)

    combine(0)
    stored.append(pltpu.make_async_copy(in_v.at[0], in_h.at[:, wpart(my_dp)], out_s.at[3]))
    stored[-1].start()

    for i in range(1, n_dp):
        proj_copy(i, dp_peer(i)).wait_recv()
        total[2] += prec[i - 1].astype(F32)
    stored.append(pltpu.make_async_copy(total.at[2], proj_h.at[2], out_s.at[2]))
    stored[-1].start()

    theirs(3)
    for i in range(1, n_dp):
        px_copy(i, dp_peer(i)).wait_recv()
        for s in range(2):
            total[s] += x_term(s, i)
    for s in range(2):
        stored.append(pltpu.make_async_copy(total.at[s], proj_h.at[s], out_s.at[s]))
        stored[-1].start()
    for i in range(1, n_dp):
        combine(i)
        in_copy(i, my_dp, dp_from(i)).start()

    for i in range(1, n_dp):
        down_copy(i, my_dp, dp_peer(i)).wait_send()
        base_copy(i, my_dp, dp_peer(i)).wait_send()
        ids_copy(i, dp_peer(i)).wait_send()
        px_copy(i, dp_peer(i)).wait_send()
        proj_copy(i, dp_peer(i)).wait_send()
        for j in range(LEVELS):
            gu_copy(i, j, dp_peer(i)).wait_send()
    mate_ids().wait_send()
    mate_tok().wait_send()

    @pl.loop(1, n_ex)
    def _(k):
        dy_copy(ex_peer(k), me).wait_send()

    @pl.loop(1, half)
    def _(k):
        x_copy(0, half_peer(k), me).wait_send()
        x_copy(1, half_peer(k), mate).wait_send()

    for i in range(n_dp):

        @pl.loop(1, n_ex)
        def _(k, i=i):
            ret_copy(i, 0, ex_peer(k), me).wait_send()

    for copy in stored:
        copy.wait()
    for i in range(1, n_dp):
        in_copy(i, my_dp, dp_from(i)).wait_send()
        in_copy(i, dp_peer(i), dp_from(i)).wait_recv()


def finish(in_h, proj_h, in_ref, proj_ref, rows, proj, load_s, store_s):
    n = proj.shape[0]
    loads = [pltpu.make_async_copy(proj_h.at[t], proj.at[t], load_s.at[t]) for t in range(n)]
    loads.append(pltpu.make_async_copy(in_h, rows, load_s.at[n]))
    stores = [
        pltpu.make_async_copy(proj.at[t], proj_ref.at[0, t], store_s.at[t]) for t in range(n)
    ]
    stores.append(pltpu.make_async_copy(rows, in_ref, store_s.at[n]))
    for copy in loads:
        copy.start()
    for load, store in zip(loads, stores):
        load.wait()
        store.start()
    for copy in stores:
        copy.wait()


def body(
    tokens, out_grad, expert_ids, gate_probs, saved_pre, gate_weight, up_weight, down_weight, basis
):
    n_dp, n_ex = lax.axis_size("dp"), lax.axis_size("expert")
    tok_rows, width = tokens.shape
    topk = expert_ids.shape[1]
    slots, hidden2 = saved_pre.shape[2:]
    hidden = hidden2 // 2
    cap = slots // n_ex
    cp = max(16, 1 << (cap - 1).bit_length())
    rows = n_ex * cp
    nl = n_ex // LEVELS
    lrows = nl * cp
    lpad = -(-nl * cap // 16) * 16
    part = gate_weight.shape[1]
    rank = basis.shape[2]
    rk = rank // n_dp
    vmem = pl.BlockSpec(memory_space=pltpu.VMEM)
    hbm = pl.BlockSpec(memory_space=pl.ANY)
    dma = pltpu.SemaphoreType.DMA
    scratch = [
        pltpu.VMEM((tok_rows, width), BF16),
        pltpu.VMEM((tok_rows, width), BF16),
        pltpu.VMEM((tok_rows, width), BF16),
        pltpu.VMEM((topk, tok_rows), jnp.int32),
        pltpu.VMEM((n_dp - 1, topk, tok_rows), jnp.int32),
        pltpu.VMEM((n_dp, rows, tok_rows), BF16),
        pltpu.VMEM((2, rows // 2, width), BF16),
        pltpu.VMEM((rows, width), BF16),
        pltpu.VMEM((rows, width), BF16),
        pltpu.VMEM((rows, width), BF16),
        pltpu.VMEM((LEVELS, lpad, width), BF16),
        pltpu.VMEM((lpad, lrows), BF16),
        pltpu.VMEM((width, hidden), BF16),
        pltpu.VMEM((width, rank), BF16),
        pltpu.VMEM((part, hidden), BF16),
        pltpu.VMEM((part, hidden), BF16),
        pltpu.VMEM((LEVELS, lpad, hidden2), BF16),
        pltpu.VMEM((LEVELS, lpad, hidden), F32),
        pltpu.VMEM((LEVELS, lpad, hidden), F32),
        pltpu.VMEM((LEVELS, lpad, hidden), BF16),
        pltpu.VMEM((n_dp, LEVELS, 2, lpad, hidden), BF16),
        pltpu.VMEM((2 * n_dp - 1, LEVELS, lpad, rk), BF16),
        pltpu.VMEM((LEVELS, lpad, rank), BF16),
        pltpu.VMEM((n_dp, LEVELS, lrows, part), BF16),
        pltpu.VMEM((n_dp, rows, part), BF16),
        pltpu.VMEM((n_dp, tok_rows, part), BF16),
        pltpu.VMEM((n_dp - 1, rk, hidden), BF16),
        pltpu.VMEM((n_dp - 1, rk, hidden), BF16),
        pltpu.VMEM((rank, hidden), F32),
        pltpu.VMEM((3, rk, hidden), F32),
        dma((6,)), dma((LEVELS,)),
        dma((n_ex,)), dma((n_ex,)), dma((2, n_ex // 2)), dma((n_ex,)), dma, dma,
        dma((n_dp,)), dma((n_dp,)), dma((n_dp,)), dma((n_dp,)),
        dma((n_dp, LEVELS)), dma((n_dp, LEVELS)), dma((n_dp, n_ex)), dma((n_dp, n_ex)),
        dma((n_dp,)), dma((n_dp,)), dma((n_dp,)), dma((n_dp,)),
        dma((n_dp,)), dma((n_dp,)), dma((n_dp,)), dma((n_dp,)), dma((4,)),
    ]
    in_part, proj = pl.pallas_call(
        functools.partial(kernel, n_dp, n_ex, cap, cp),
        out_shape=(
            jax.ShapeDtypeStruct((tok_rows, width), BF16),
            jax.ShapeDtypeStruct((3, rk, hidden), F32),
        ),
        in_specs=[vmem] * 2 + [hbm] * 7,
        out_specs=(hbm, hbm),
        scratch_shapes=scratch,
        compiler_params=pltpu.CompilerParams(
            collective_id=0, has_side_effects=True, vmem_limit_bytes=60 * 1024 * 1024
        ),
    )(
        expert_ids.T, gate_probs.T, tokens, out_grad, saved_pre,
        gate_weight, up_weight, down_weight, basis,
    )
    return pl.pallas_call(
        finish,
        out_shape=(
            jax.ShapeDtypeStruct((tok_rows, width), BF16),
            jax.ShapeDtypeStruct((1, 3, rk, hidden), F32),
        ),
        in_specs=[hbm, hbm],
        out_specs=(hbm, hbm),
        scratch_shapes=[
            pltpu.VMEM((tok_rows, width), BF16),
            pltpu.VMEM((3, rk, hidden), F32),
            dma((4,)), dma((4,)),
        ],
    )(in_part, proj)


def solution(mesh):
    return jax.shard_map(
        body,
        mesh=mesh,
        in_specs=(
            P(("dp", "expert"), None),
            P(("dp", "expert"), None),
            P(("dp", "expert"), None),
            P(("dp", "expert"), None),
            P("dp", "expert", None, None),
            P("expert", "dp", None),
            P("expert", "dp", None),
            P("expert", "dp", None),
            P("expert", "dp", None),
        ),
        out_specs=(P(("dp", "expert"), None), P("expert", None, "dp", None)),
        check_vma=False,
    )
```

```python
import functools
import jax
import jax.numpy as jnp
from jax import lax
from jax.experimental import pallas as pl
from jax.experimental.pallas import tpu as pltpu
from jax.sharding import PartitionSpec as P

MESH = pl.DeviceIdType.MESH
F32 = jnp.float32
BF16 = jnp.bfloat16
LEVELS = 4


def dot(left, right, dims):
    return lax.dot_general(left, right, (dims, ((), ())), preferred_element_type=F32)


NN = ((1,), (0,))
TN = ((0,), (0,))
NT = ((1,), (1,))


def kernel(
    n_dp, n_ex, cap, cp,
    ids_h, probs_h, tok_h, og_h, pre_h, gw_h, uw_h, dw, bs,
    in_h, proj_h,
    ids, probs, tok, og, tok2, ids2, idsd, pick_v, pick_m, sx, sg, rx, rg, dyc, spr, dfull, bfull, gw, uw, pre,
    act_a, act_b, hid, gu, px, pdy, rs, rr, in_v, psend, prec, term, total,
    local_sem, pre_sem, dy_s, dy_r, x_s, x_r, relay_s, relay_r, down_s, down_r, base_s, base_r,
    gu_s, gu_r, ret_s, ret_r, px_s, px_r, proj_s, proj_r, in_s, in_r, ids_s, ids_r, out_s,
):
    my_dp = lax.axis_index("dp")
    me = lax.axis_index("expert")
    rows = n_ex * cp
    half = n_ex // 2
    nl = n_ex // LEVELS
    lrows = nl * cp
    lcap = nl * cap
    tokens, width = tok.shape
    topk = ids.shape[0]
    hidden = dfull.shape[1]
    part = width // n_dp
    rank = bfull.shape[1]
    rk = rank // n_dp
    shift = cp.bit_length() - 1
    fw = 256

    z = lax.div(me, nl)
    spot = lax.rem(me, nl)
    mate = lax.rem(me + half, n_ex)
    half0 = lax.div(me, half) * half
    levels = [z + 1 - 2 * lax.rem(z, 2), lax.rem(z + 2, LEVELS), LEVELS - 1 - z, z]
    own = LEVELS - 1

    def block(owner):
        return pl.ds(pl.multiple_of(owner * cp, cp), cp)

    def wpart(owner):
        return pl.ds(pl.multiple_of(owner * part, part), part)

    def rpart(owner):
        return pl.ds(pl.multiple_of(owner * rk, rk), rk)

    def rank_cols(owner):
        line = lax.broadcasted_iota(jnp.int32, (rank, rk), 0)
        lane = lax.broadcasted_iota(jnp.int32, (rank, rk), 1) + owner * rk
        return jnp.where(line == lane, one, zero).astype(BF16)

    def lpart(j):
        return pl.ds(pl.multiple_of(levels[j] * lrows, lrows), lrows)

    def ex_peer(k):
        return lax.rem(me + k, n_ex)

    def half_peer(k):
        return half0 + lax.rem(me - half0 + k, half)

    def in_level(j, t):
        return levels[j] * nl + lax.rem(spot + t, nl)

    def dp_peer(i):
        return lax.rem(my_dp + i, n_dp)

    def dp_from(i):
        return lax.rem(my_dp + n_dp - i, n_dp)

    first = [
        pltpu.make_async_copy(ids_h, ids, local_sem.at[6]),
        pltpu.make_async_copy(probs_h, probs, local_sem.at[7]),
    ]
    for copy in first:
        copy.start()

    pad = gu.shape[3] - lcap
    if pad:
        for j in range(LEVELS):
            pre[j, lcap:, :] = jnp.zeros((pad, 2 * hidden), BF16)
            for i in range(1, n_dp):
                for s in range(2):
                    gu[i, j, s, lcap:, :] = jnp.zeros((pad, hidden), BF16)

    barrier = pltpu.get_barrier_semaphore()

    for i in range(1, n_dp):
        pl.semaphore_signal(barrier, inc=1, device_id={"dp": dp_peer(i)}, device_id_type=MESH)

    @pl.loop(1, n_ex)
    def _(k):
        pl.semaphore_signal(barrier, inc=1, device_id={"expert": ex_peer(k)}, device_id_type=MESH)

    local = [
        pltpu.make_async_copy(og_h, og, local_sem.at[0]),
        pltpu.make_async_copy(tok_h, tok, local_sem.at[1]),
        pltpu.make_async_copy(dw.at[0], dfull.at[wpart(my_dp)], local_sem.at[2]),
        pltpu.make_async_copy(bs.at[0], bfull.at[wpart(my_dp)], local_sem.at[3]),
        pltpu.make_async_copy(gw_h.at[0], gw, local_sem.at[4]),
        pltpu.make_async_copy(uw_h.at[0], uw, local_sem.at[5]),
    ]
    pre_copy = []
    for j in range(LEVELS):
        src = pl.ds(pl.multiple_of(levels[j] * lcap, 8), lcap)
        pre_copy.append(
            pltpu.make_async_copy(pre_h.at[0, 0, src], pre.at[j, pl.ds(0, lcap)], pre_sem.at[j])
        )
    for copy in local[:2] + pre_copy + local[2:]:
        copy.start()

    one, zero = jnp.ones((), F32), jnp.zeros((), F32)
    earlier = lax.broadcasted_iota(jnp.int32, (tokens, tokens), 0) < lax.broadcasted_iota(
        jnp.int32, (tokens, tokens), 1
    )
    earlier = jnp.where(earlier, one, zero).astype(BF16)

    def pick_of(names_of, first, count):
        line = lax.broadcasted_iota(jnp.int32, (count, tokens), 0)
        line_expert = lax.shift_right_logical(line, shift) + first
        line_slot = lax.bitwise_and(line, cp - 1)
        names = [names_of[k : k + 1, :] == line_expert for k in range(topk)]
        any_name = functools.reduce(jnp.logical_or, names)
        named = jnp.where(any_name, one, zero).astype(BF16)
        before = dot(named, earlier, NN)
        at_slot = before == line_slot.astype(F32)
        pick = jnp.where(jnp.logical_and(any_name, at_slot), one, zero).astype(BF16)
        return pick, names, at_slot

    for copy in first:
        copy.wait()
    pick, names, at_slot = pick_of(ids, 0, rows)
    pick_v[0] = pick
    weights = functools.reduce(
        jnp.add, [jnp.where(name, probs[k : k + 1, :], zero) for k, name in enumerate(names)]
    )
    weight = jnp.sum(jnp.where(at_slot, weights, zero), axis=1, keepdims=True)

    pl.semaphore_wait(barrier, n_ex - 1 + n_dp - 1)

    def down_copy(i, owner, peer):
        return pltpu.make_async_remote_copy(
            dw.at[0], dfull.at[wpart(owner)], down_s.at[i], down_r.at[i],
            device_id={"dp": peer}, device_id_type=MESH,
        )

    def base_copy(i, owner, peer):
        return pltpu.make_async_remote_copy(
            bs.at[0], bfull.at[wpart(owner)], base_s.at[i], base_r.at[i],
            device_id={"dp": peer}, device_id_type=MESH,
        )

    def ids_copy(i, peer):
        return pltpu.make_async_remote_copy(
            ids, idsd.at[i - 1], ids_s.at[i], ids_r.at[i],
            device_id={"dp": peer}, device_id_type=MESH,
        )

    def mate_ids():
        return pltpu.make_async_remote_copy(
            ids, ids2, ids_s.at[0], ids_r.at[0], device_id={"expert": mate}, device_id_type=MESH
        )

    def mate_tok():
        return pltpu.make_async_remote_copy(
            tok, tok2, relay_s, relay_r, device_id={"expert": mate}, device_id_type=MESH
        )

    def dy_copy(peer, owner):
        return pltpu.make_async_remote_copy(
            sg.at[block(peer)], rg.at[block(owner)], dy_s.at[peer], dy_r.at[owner],
            device_id={"expert": peer}, device_id_type=MESH,
        )

    def x_copy(m, peer, owner):
        return pltpu.make_async_remote_copy(
            sx.at[m, block(peer - half0)], rx.at[block(owner)], x_s.at[m, peer - half0], x_r.at[owner],
            device_id={"expert": peer}, device_id_type=MESH,
        )

    def gu_copy(i, j, peer):
        used = pl.ds(0, lcap)
        return pltpu.make_async_remote_copy(
            gu.at[0, j, :, used], gu.at[i, j, :, used], gu_s.at[i, j], gu_r.at[i, j],
            device_id={"dp": peer}, device_id_type=MESH,
        )

    def px_copy(i, peer):
        return pltpu.make_async_remote_copy(
            px.at[i - 1], px.at[n_dp - 1 + i], px_s.at[i], px_r.at[i],
            device_id={"dp": peer}, device_id_type=MESH,
        )

    def ret_copy(i, j, peer, owner):
        return pltpu.make_async_remote_copy(
            rs.at[i, j, block(lax.rem(peer, nl))], rr.at[i, block(owner)],
            ret_s.at[i, peer], ret_r.at[i, owner],
            device_id={"expert": peer}, device_id_type=MESH,
        )

    def proj_copy(i, peer):
        return pltpu.make_async_remote_copy(
            psend.at[i - 1], prec.at[i - 1], proj_s.at[i], proj_r.at[i],
            device_id={"dp": peer}, device_id_type=MESH,
        )

    def in_copy(i, owner, peer):
        return pltpu.make_async_remote_copy(
            in_v.at[i], in_h.at[:, wpart(owner)], in_s.at[i], in_r.at[i],
            device_id={"dp": peer}, device_id_type=MESH,
        )

    for i in range(1, n_dp):
        down_copy(i, my_dp, dp_peer(i)).start()
    for i in range(1, n_dp):
        base_copy(i, my_dp, dp_peer(i)).start()
    mate_ids().start()
    for i in range(1, n_dp):
        ids_copy(i, dp_peer(i)).start()

    local[0].wait()
    sg[...] = (dot(pick, og[...], NN) * weight).astype(BF16)
    for j in range(LEVELS):

        @pl.loop(int(j == own), nl)
        def _(t, j=j):
            dy_copy(in_level(j, t), me).start()

    rg[block(me), :] = sg[block(me), :]

    local[1].wait()
    mate_tok().start()
    half_rows = pl.ds(pl.multiple_of(half0 * cp, cp), half * cp)
    sx[0] = dot(pick_v[0, half_rows], tok[...], NN).astype(BF16)

    @pl.loop(1, half)
    def _(k):
        x_copy(0, half_peer(k), me).start()

    rx[block(me), :] = sx[0, block(me - half0), :]

    grid = (gu.shape[3], lrows)
    line = lax.broadcasted_iota(jnp.int32, grid, 1)
    inner = lax.bitwise_and(line, cp - 1)
    target = lax.shift_right_logical(line, shift) * cap + inner
    spread = jnp.logical_and(target == lax.broadcasted_iota(jnp.int32, grid, 0), inner < cap)
    spr[...] = jnp.where(spread, one, zero).astype(BF16)

    for j in range(LEVELS):
        pre_copy[j].wait()
        for f in range(0, hidden, fw):
            cols = slice(f, f + fw)
            g = pre[j, :, f : f + fw].astype(F32)
            u = pre[j, :, hidden + f : hidden + f + fw].astype(F32)
            sig = jax.nn.sigmoid(g)
            gs = g * sig
            act_a[j, :, cols] = gs
            hid[j, :, cols] = (gs * u).astype(BF16)
            act_b[j, :, cols] = u * sig * (1.0 + g * (1.0 - sig))

    def row_grad(i, j):
        out = dot(gu[i, j, 0], gw[...], NT) + dot(gu[i, j, 1], uw[...], NT)
        rs[i, j] = dot(spr[...], out.astype(BF16), TN).astype(BF16)

        @pl.loop(int(j == own), nl)
        def _(t):
            ret_copy(i, j, in_level(j, t), me).start()

        if j == own:
            rr[i, block(me), :] = rs[i, j, block(spot), :]

    local[2].wait()
    for i in range(1, n_dp):
        down_copy(i, dp_from(i), dp_peer(i)).wait_recv()

    for j in range(LEVELS):

        @pl.loop(int(j == own), nl)
        def _(t, j=j):
            src = in_level(j, t)
            dy_copy(src, src).wait_recv()

        dyc[j] = dot(spr[...], rg[lpart(j), :], NN).astype(BF16)
        for f in range(0, hidden, fw):
            cols = slice(f, f + fw)
            hg = dot(dyc[j], dfull[:, cols], NN)
            gu[0, j, 1, :, cols] = (hg * act_a[j, :, cols]).astype(BF16)
            gu[0, j, 0, :, cols] = (hg * act_b[j, :, cols]).astype(BF16)
        for i in range(1, n_dp):
            gu_copy(i, j, dp_peer(i)).start()
        if j == 0:
            local[4].wait()
            local[5].wait()
        row_grad(0, j)

    local[3].wait()
    for i in range(1, n_dp):
        base_copy(i, dp_from(i), dp_peer(i)).wait_recv()
    for j in range(LEVELS):
        pdy[j] = dot(dyc[j], bfull[...], NN).astype(BF16)

    def project(left, right):
        return functools.reduce(jnp.add, [dot(left(j), right(j), TN) for j in range(LEVELS)])

    term[...] = project(lambda j: pdy[j], lambda j: hid[j])
    for i in range(1, n_dp):
        psend[i - 1] = term[rpart(dp_peer(i)), :].astype(BF16)
        proj_copy(i, dp_peer(i)).start()
    total[2] = term[rpart(my_dp), :]

    for i in range(1, n_dp):
        ids_copy(i, dp_peer(i)).wait_recv()
        pick_v[i] = pick_of(idsd.at[i - 1], 0, rows)[0]
    mate_ids().wait_recv()
    pick2, _, _ = pick_of(ids2, half0, half * cp)
    pick_m[...] = pick2

    def theirs(j):
        for i in range(1, n_dp):
            gu_copy(i, j, dp_peer(i)).wait_recv()
            row_grad(i, j)

    theirs(0)

    mate_tok().wait_recv()
    sx[1] = dot(pick_m[...], tok2[...], NN).astype(BF16)

    @pl.loop(1, half)
    def _(k):
        x_copy(1, half_peer(k), mate).start()

    rx[block(mate), :] = sx[1, block(me - half0), :]

    theirs(1)

    @pl.loop(1, n_ex)
    def _(k):
        src = ex_peer(k)

        @pl.when(src != mate)
        def _():
            x_copy(0, half0, src).wait_recv()

    for j in range(LEVELS):
        xj = dot(spr[...], rx[lpart(j), :], NN).astype(BF16)
        if rk % 128:
            xp = dot(xj, bfull[...], NN).astype(BF16)
        for i in range(n_dp):
            if rk % 128:
                pj = dot(xp, rank_cols(dp_peer(i)), NN)
            else:
                pj = dot(xj, bfull[:, rpart(dp_peer(i))], NN)
            px[(i + n_dp - 1) % n_dp, j] = pj.astype(BF16)
    for i in range(1, n_dp):
        px_copy(i, dp_peer(i)).start()

    theirs(2)
    theirs(3)

    def x_term(s, i):
        left = px.at[n_dp - 1 + i]
        return project(lambda j: left[j], lambda j: gu[i, j, s])

    for s in range(2):
        total[s] = x_term(s, 0)

    stored = []

    def combine(i):
        @pl.loop(1, n_ex)
        def _(k):
            src = ex_peer(k)
            ret_copy(i, 0, src, src).wait_recv()

        in_v[i] = dot(pick_v[i], rr[i], TN).astype(BF16)

    combine(0)
    stored.append(pltpu.make_async_copy(in_v.at[0], in_h.at[:, wpart(my_dp)], out_s.at[3]))
    stored[-1].start()
    for i in range(1, n_dp):
        combine(i)
        in_copy(i, my_dp, dp_from(i)).start()

    for i in range(1, n_dp):
        proj_copy(i, dp_peer(i)).wait_recv()
        total[2] += prec[i - 1].astype(F32)
    stored.append(pltpu.make_async_copy(total.at[2], proj_h.at[2], out_s.at[2]))
    stored[-1].start()
    for i in range(1, n_dp):
        px_copy(i, dp_peer(i)).wait_recv()
        for s in range(2):
            total[s] += x_term(s, i)
    for s in range(2):
        stored.append(pltpu.make_async_copy(total.at[s], proj_h.at[s], out_s.at[s]))
        stored[-1].start()

    for i in range(1, n_dp):
        down_copy(i, my_dp, dp_peer(i)).wait_send()
        base_copy(i, my_dp, dp_peer(i)).wait_send()
        ids_copy(i, dp_peer(i)).wait_send()
        px_copy(i, dp_peer(i)).wait_send()
        proj_copy(i, dp_peer(i)).wait_send()
        for j in range(LEVELS):
            gu_copy(i, j, dp_peer(i)).wait_send()
    mate_ids().wait_send()
    mate_tok().wait_send()

    @pl.loop(1, n_ex)
    def _(k):
        dy_copy(ex_peer(k), me).wait_send()

    @pl.loop(1, half)
    def _(k):
        x_copy(0, half_peer(k), me).wait_send()
        x_copy(1, half_peer(k), mate).wait_send()

    for i in range(n_dp):

        @pl.loop(1, n_ex)
        def _(k, i=i):
            ret_copy(i, 0, ex_peer(k), me).wait_send()

    for copy in stored:
        copy.wait()
    for i in range(1, n_dp):
        in_copy(i, my_dp, dp_from(i)).wait_send()
        in_copy(i, dp_peer(i), dp_from(i)).wait_recv()


def finish(in_h, proj_h, in_ref, proj_ref, rows, proj, load_s, store_s):
    n = proj.shape[0]
    loads = [pltpu.make_async_copy(proj_h.at[t], proj.at[t], load_s.at[t]) for t in range(n)]
    loads.append(pltpu.make_async_copy(in_h, rows, load_s.at[n]))
    stores = [
        pltpu.make_async_copy(proj.at[t], proj_ref.at[0, t], store_s.at[t]) for t in range(n)
    ]
    stores.append(pltpu.make_async_copy(rows, in_ref, store_s.at[n]))
    for copy in loads:
        copy.start()
    for load, store in zip(loads, stores):
        load.wait()
        store.start()
    for copy in stores:
        copy.wait()


def body(
    tokens, out_grad, expert_ids, gate_probs, saved_pre, gate_weight, up_weight, down_weight, basis
):
    n_dp, n_ex = lax.axis_size("dp"), lax.axis_size("expert")
    tok_rows, width = tokens.shape
    topk = expert_ids.shape[1]
    slots, hidden2 = saved_pre.shape[2:]
    hidden = hidden2 // 2
    cap = slots // n_ex
    cp = max(16, 1 << (cap - 1).bit_length())
    rows = n_ex * cp
    nl = n_ex // LEVELS
    lrows = nl * cp
    lpad = -(-nl * cap // 16) * 16
    part = gate_weight.shape[1]
    rank = basis.shape[2]
    rk = rank // n_dp
    hbm = pl.BlockSpec(memory_space=pl.ANY)
    dma = pltpu.SemaphoreType.DMA
    scratch = [
        pltpu.VMEM((topk, tok_rows), jnp.int32),
        pltpu.VMEM((topk, tok_rows), F32),
        pltpu.VMEM((tok_rows, width), BF16),
        pltpu.VMEM((tok_rows, width), BF16),
        pltpu.VMEM((tok_rows, width), BF16),
        pltpu.VMEM((topk, tok_rows), jnp.int32),
        pltpu.VMEM((n_dp - 1, topk, tok_rows), jnp.int32),
        pltpu.VMEM((n_dp, rows, tok_rows), BF16),
        pltpu.VMEM((rows // 2, tok_rows), BF16),
        pltpu.VMEM((2, rows // 2, width), BF16),
        pltpu.VMEM((rows, width), BF16),
        pltpu.VMEM((rows, width), BF16),
        pltpu.VMEM((rows, width), BF16),
        pltpu.VMEM((LEVELS, lpad, width), BF16),
        pltpu.VMEM((lpad, lrows), BF16),
        pltpu.VMEM((width, hidden), BF16),
        pltpu.VMEM((width, rank), BF16),
        pltpu.VMEM((part, hidden), BF16),
        pltpu.VMEM((part, hidden), BF16),
        pltpu.VMEM((LEVELS, lpad, hidden2), BF16),
        pltpu.VMEM((LEVELS, lpad, hidden), F32),
        pltpu.VMEM((LEVELS, lpad, hidden), F32),
        pltpu.VMEM((LEVELS, lpad, hidden), BF16),
        pltpu.VMEM((n_dp, LEVELS, 2, lpad, hidden), BF16),
        pltpu.VMEM((2 * n_dp - 1, LEVELS, lpad, rk), BF16),
        pltpu.VMEM((LEVELS, lpad, rank), BF16),
        pltpu.VMEM((n_dp, LEVELS, lrows, part), BF16),
        pltpu.VMEM((n_dp, rows, part), BF16),
        pltpu.VMEM((n_dp, tok_rows, part), BF16),
        pltpu.VMEM((n_dp - 1, rk, hidden), BF16),
        pltpu.VMEM((n_dp - 1, rk, hidden), BF16),
        pltpu.VMEM((rank, hidden), F32),
        pltpu.VMEM((3, rk, hidden), F32),
        dma((8,)), dma((LEVELS,)),
        dma((n_ex,)), dma((n_ex,)), dma((2, n_ex // 2)), dma((n_ex,)), dma, dma,
        dma((n_dp,)), dma((n_dp,)), dma((n_dp,)), dma((n_dp,)),
        dma((n_dp, LEVELS)), dma((n_dp, LEVELS)), dma((n_dp, n_ex)), dma((n_dp, n_ex)),
        dma((n_dp,)), dma((n_dp,)), dma((n_dp,)), dma((n_dp,)),
        dma((n_dp,)), dma((n_dp,)), dma((n_dp,)), dma((n_dp,)), dma((4,)),
    ]
    in_part, proj = pl.pallas_call(
        functools.partial(kernel, n_dp, n_ex, cap, cp),
        out_shape=(
            jax.ShapeDtypeStruct((tok_rows, width), BF16),
            jax.ShapeDtypeStruct((3, rk, hidden), F32),
        ),
        in_specs=[hbm] * 9,
        out_specs=(hbm, hbm),
        scratch_shapes=scratch,
        compiler_params=pltpu.CompilerParams(
            collective_id=0, has_side_effects=True, vmem_limit_bytes=60 * 1024 * 1024
        ),
    )(
        expert_ids.T, gate_probs.T, tokens, out_grad, saved_pre,
        gate_weight, up_weight, down_weight, basis,
    )
    return pl.pallas_call(
        finish,
        out_shape=(
            jax.ShapeDtypeStruct((tok_rows, width), BF16),
            jax.ShapeDtypeStruct((1, 3, rk, hidden), F32),
        ),
        in_specs=[hbm, hbm],
        out_specs=(hbm, hbm),
        scratch_shapes=[
            pltpu.VMEM((tok_rows, width), BF16),
            pltpu.VMEM((3, rk, hidden), F32),
            dma((4,)), dma((4,)),
        ],
    )(in_part, proj)


def solution(mesh):
    return jax.shard_map(
        body,
        mesh=mesh,
        in_specs=(
            P(("dp", "expert"), None),
            P(("dp", "expert"), None),
            P(("dp", "expert"), None),
            P(("dp", "expert"), None),
            P("dp", "expert", None, None),
            P("expert", "dp", None),
            P("expert", "dp", None),
            P("expert", "dp", None),
            P("expert", "dp", None),
        ),
        out_specs=(P(("dp", "expert"), None), P("expert", None, "dp", None)),
        check_vma=False,
    )
```

```python
import functools
import jax
import jax.numpy as jnp
from jax import lax
from jax.experimental import pallas as pl
from jax.experimental.pallas import tpu as pltpu
from jax.sharding import PartitionSpec as P

MESH = pl.DeviceIdType.MESH
F32 = jnp.float32
BF16 = jnp.bfloat16
LEVELS = 4


def dot(left, right, dims):
    return lax.dot_general(left, right, (dims, ((), ())), preferred_element_type=F32)


NN = ((1,), (0,))
TN = ((0,), (0,))
NT = ((1,), (1,))


def kernel(
    n_dp, n_ex, cap, cp,
    ids_h, probs_h, tok_h, og_h, pre_h, gw_h, uw_h, dw, bs,
    in_h, proj_h,
    ids, probs, tok, og, tok2, og2, ids2, probs2, idsd, pick_v, sx, sg, rx, rg, dyc, spr, dfull, bfull, gw, uw, pre,
    act_a, act_b, hid, gu, px, pdy, rs, rr, in_v, psend, prec, term, total,
    local_sem, pre_sem, dy_s, dy_r, x_s, x_r, mate_s, mate_r, down_s, down_r, base_s, base_r,
    gu_s, gu_r, ret_s, ret_r, px_s, px_r, proj_s, proj_r, in_s, in_r, ids_s, ids_r, out_s,
):
    my_dp = lax.axis_index("dp")
    me = lax.axis_index("expert")
    rows = n_ex * cp
    half = n_ex // 2
    nl = n_ex // LEVELS
    lrows = nl * cp
    lcap = nl * cap
    tokens, width = tok.shape
    topk = ids.shape[0]
    hidden = dfull.shape[1]
    part = width // n_dp
    rank = bfull.shape[1]
    rk = rank // n_dp
    shift = cp.bit_length() - 1
    fw = 256

    z = lax.div(me, nl)
    spot = lax.rem(me, nl)
    mate = lax.rem(me + half, n_ex)
    half0 = lax.div(me, half) * half
    levels = [z + 1 - 2 * lax.rem(z, 2), lax.rem(z + 2, LEVELS), LEVELS - 1 - z, z]
    own = LEVELS - 1

    def block(owner):
        return pl.ds(pl.multiple_of(owner * cp, cp), cp)

    def wpart(owner):
        return pl.ds(pl.multiple_of(owner * part, part), part)

    def rpart(owner):
        return pl.ds(pl.multiple_of(owner * rk, rk), rk)

    def rank_cols(owner):
        line = lax.broadcasted_iota(jnp.int32, (rank, rk), 0)
        lane = lax.broadcasted_iota(jnp.int32, (rank, rk), 1) + owner * rk
        return jnp.where(line == lane, one, zero).astype(BF16)

    def lpart(j):
        return pl.ds(pl.multiple_of(levels[j] * lrows, lrows), lrows)

    def ex_peer(k):
        return lax.rem(me + k, n_ex)

    def half_peer(k):
        return half0 + lax.rem(me - half0 + k, half)

    def in_level(j, t):
        return levels[j] * nl + lax.rem(spot + t, nl)

    def dp_peer(i):
        return lax.rem(my_dp + i, n_dp)

    def dp_from(i):
        return lax.rem(my_dp + n_dp - i, n_dp)

    first = [
        pltpu.make_async_copy(ids_h, ids, local_sem.at[6]),
        pltpu.make_async_copy(probs_h, probs, local_sem.at[7]),
    ]
    for copy in first:
        copy.start()

    pad = gu.shape[3] - lcap
    if pad:
        for j in range(LEVELS):
            pre[j, lcap:, :] = jnp.zeros((pad, 2 * hidden), BF16)
            for i in range(1, n_dp):
                for s in range(2):
                    gu[i, j, s, lcap:, :] = jnp.zeros((pad, hidden), BF16)

    barrier = pltpu.get_barrier_semaphore()

    for i in range(1, n_dp):
        pl.semaphore_signal(barrier, inc=1, device_id={"dp": dp_peer(i)}, device_id_type=MESH)

    @pl.loop(1, n_ex)
    def _(k):
        pl.semaphore_signal(barrier, inc=1, device_id={"expert": ex_peer(k)}, device_id_type=MESH)

    local = [
        pltpu.make_async_copy(og_h, og, local_sem.at[0]),
        pltpu.make_async_copy(tok_h, tok, local_sem.at[1]),
        pltpu.make_async_copy(dw.at[0], dfull.at[wpart(my_dp)], local_sem.at[2]),
        pltpu.make_async_copy(bs.at[0], bfull.at[wpart(my_dp)], local_sem.at[3]),
        pltpu.make_async_copy(gw_h.at[0], gw, local_sem.at[4]),
        pltpu.make_async_copy(uw_h.at[0], uw, local_sem.at[5]),
    ]
    pre_copy = []
    for j in range(LEVELS):
        src = pl.ds(pl.multiple_of(levels[j] * lcap, 8), lcap)
        pre_copy.append(
            pltpu.make_async_copy(pre_h.at[0, 0, src], pre.at[j, pl.ds(0, lcap)], pre_sem.at[j])
        )
    for copy in local[:2] + pre_copy + local[2:]:
        copy.start()

    one, zero = jnp.ones((), F32), jnp.zeros((), F32)
    earlier = lax.broadcasted_iota(jnp.int32, (tokens, tokens), 0) < lax.broadcasted_iota(
        jnp.int32, (tokens, tokens), 1
    )
    earlier = jnp.where(earlier, one, zero).astype(BF16)

    def pick_of(names_of, first, count):
        line = lax.broadcasted_iota(jnp.int32, (count, tokens), 0)
        line_expert = lax.shift_right_logical(line, shift) + first
        line_slot = lax.bitwise_and(line, cp - 1)
        names = [names_of[k : k + 1, :] == line_expert for k in range(topk)]
        any_name = functools.reduce(jnp.logical_or, names)
        named = jnp.where(any_name, one, zero).astype(BF16)
        before = dot(named, earlier, NN)
        at_slot = before == line_slot.astype(F32)
        pick = jnp.where(jnp.logical_and(any_name, at_slot), one, zero).astype(BF16)
        return pick, names, at_slot

    def half_pick(names_of, weights_of):
        pick, names, at_slot = pick_of(names_of, half0, half * cp)
        weights = functools.reduce(
            jnp.add, [jnp.where(name, weights_of[k : k + 1, :], zero) for k, name in enumerate(names)]
        )
        return pick, jnp.sum(jnp.where(at_slot, weights, zero), axis=1, keepdims=True)

    for copy in first:
        copy.wait()
    pick, weight = half_pick(ids, probs)

    pl.semaphore_wait(barrier, n_ex - 1 + n_dp - 1)

    def down_copy(i, owner, peer):
        return pltpu.make_async_remote_copy(
            dw.at[0], dfull.at[wpart(owner)], down_s.at[i], down_r.at[i],
            device_id={"dp": peer}, device_id_type=MESH,
        )

    def base_copy(i, owner, peer):
        return pltpu.make_async_remote_copy(
            bs.at[0], bfull.at[wpart(owner)], base_s.at[i], base_r.at[i],
            device_id={"dp": peer}, device_id_type=MESH,
        )

    def ids_copy(i, peer):
        return pltpu.make_async_remote_copy(
            ids, idsd.at[i - 1], ids_s.at[i], ids_r.at[i],
            device_id={"dp": peer}, device_id_type=MESH,
        )

    def mate_copy(n):
        src, dst = ((og, og2), (tok, tok2), (ids, ids2), (probs, probs2))[n]
        return pltpu.make_async_remote_copy(
            src, dst, mate_s.at[n], mate_r.at[n], device_id={"expert": mate}, device_id_type=MESH
        )

    def dy_copy(m, peer, owner, j):
        return pltpu.make_async_remote_copy(
            sg.at[m, block(peer - half0)], rg.at[block(owner)], dy_s.at[m], dy_r.at[j],
            device_id={"expert": peer}, device_id_type=MESH,
        )

    def x_copy(m, peer, owner):
        return pltpu.make_async_remote_copy(
            sx.at[m, block(peer - half0)], rx.at[block(owner)], x_s.at[m], x_r.at[0],
            device_id={"expert": peer}, device_id_type=MESH,
        )

    def blocks(buffer, count, send, recv):
        span = buffer.at[pl.ds(0, count * cp)]
        return pltpu.make_async_remote_copy(
            span, span, send, recv, device_id={"expert": mate}, device_id_type=MESH
        )

    def gu_copy(i, j, peer):
        used = pl.ds(0, lcap)
        return pltpu.make_async_remote_copy(
            gu.at[0, j, :, used], gu.at[i, j, :, used], gu_s.at[i, j], gu_r.at[i, j],
            device_id={"dp": peer}, device_id_type=MESH,
        )

    def px_copy(i, peer):
        return pltpu.make_async_remote_copy(
            px.at[i - 1], px.at[n_dp - 1 + i], px_s.at[i], px_r.at[i],
            device_id={"dp": peer}, device_id_type=MESH,
        )

    def ret_copy(i, j, peer, owner):
        return pltpu.make_async_remote_copy(
            rs.at[i, j, block(lax.rem(peer, nl))], rr.at[i, block(owner)],
            ret_s.at[i], ret_r.at[i],
            device_id={"expert": peer}, device_id_type=MESH,
        )

    def proj_copy(i, peer):
        return pltpu.make_async_remote_copy(
            psend.at[i - 1], prec.at[i - 1], proj_s.at[i], proj_r.at[i],
            device_id={"dp": peer}, device_id_type=MESH,
        )

    def in_copy(i, owner, peer):
        return pltpu.make_async_remote_copy(
            in_v.at[i], in_h.at[:, wpart(owner)], in_s.at[i], in_r.at[i],
            device_id={"dp": peer}, device_id_type=MESH,
        )

    for i in range(1, n_dp):
        down_copy(i, my_dp, dp_peer(i)).start()
    mate_copy(2).start()
    mate_copy(3).start()
    local[0].wait()
    mate_copy(0).start()
    for i in range(1, n_dp):
        base_copy(i, my_dp, dp_peer(i)).start()
    for i in range(1, n_dp):
        ids_copy(i, dp_peer(i)).start()

    def dispatch_dy(m, owner):
        for near, tag in ((0, 0 if m == 0 else 2), (own, own if m == 0 else 1)):

            @pl.loop(int(near == own), nl)
            def _(t):
                dy_copy(m, in_level(near, t), owner, tag).start()

        rg[block(owner), :] = sg[m, block(me - half0), :]

    def dispatch_x(m, owner):
        @pl.loop(1, half)
        def _(k):
            x_copy(m, half_peer(k), owner).start()

        rx[block(owner), :] = sx[m, block(me - half0), :]

    sg[0] = (dot(pick, og[...], NN) * weight).astype(BF16)
    dispatch_dy(0, me)
    local[1].wait()
    mate_copy(1).start()
    sx[0] = dot(pick, tok[...], NN).astype(BF16)
    dispatch_x(0, me)

    grid = (gu.shape[3], lrows)
    line = lax.broadcasted_iota(jnp.int32, grid, 1)
    inner = lax.bitwise_and(line, cp - 1)
    target = lax.shift_right_logical(line, shift) * cap + inner
    spread = jnp.logical_and(target == lax.broadcasted_iota(jnp.int32, grid, 0), inner < cap)
    spr[...] = jnp.where(spread, one, zero).astype(BF16)

    for j in range(LEVELS):
        pre_copy[j].wait()
        for f in range(0, hidden, fw):
            cols = slice(f, f + fw)
            g = pre[j, :, f : f + fw].astype(F32)
            u = pre[j, :, hidden + f : hidden + f + fw].astype(F32)
            sig = jax.nn.sigmoid(g)
            gs = g * sig
            act_a[j, :, cols] = gs
            hid[j, :, cols] = (gs * u).astype(BF16)
            act_b[j, :, cols] = u * sig * (1.0 + g * (1.0 - sig))

    def row_grad(i, j):
        out = dot(gu[i, j, 0], gw[...], NT) + dot(gu[i, j, 1], uw[...], NT)
        rs[i, j] = dot(spr[...], out.astype(BF16), TN).astype(BF16)

        @pl.loop(int(j == own), nl)
        def _(t):
            ret_copy(i, j, in_level(j, t), me).start()

        if j == own:
            rr[i, block(me), :] = rs[i, j, block(spot), :]

    pick_v[0] = pick_of(ids, 0, rows)[0]
    for i in range(1, n_dp):
        ids_copy(i, dp_peer(i)).wait_recv()
        pick_v[i] = pick_of(idsd.at[i - 1], 0, rows)[0]

    mate_copy(2).wait_recv()
    mate_copy(3).wait_recv()
    pick2, weight2 = half_pick(ids2, probs2)
    mate_copy(0).wait_recv()
    sg[1] = (dot(pick2, og2[...], NN) * weight2).astype(BF16)
    dispatch_dy(1, mate)

    local[2].wait()
    for i in range(1, n_dp):
        down_copy(i, dp_from(i), dp_peer(i)).wait_recv()

    for j in range(LEVELS):

        blocks(rg, nl - j % 2, dy_s.at[0], dy_r.at[j]).wait_recv()
        dyc[j] = dot(spr[...], rg[lpart(j), :], NN).astype(BF16)
        for f in range(0, hidden, fw):
            cols = slice(f, f + fw)
            hg = dot(dyc[j], dfull[:, cols], NN)
            gu[0, j, 1, :, cols] = (hg * act_a[j, :, cols]).astype(BF16)
            gu[0, j, 0, :, cols] = (hg * act_b[j, :, cols]).astype(BF16)
        for i in range(1, n_dp):
            gu_copy(i, j, dp_peer(i)).start()
        if j == 0:
            local[4].wait()
            local[5].wait()
        row_grad(0, j)

    local[3].wait()
    for i in range(1, n_dp):
        base_copy(i, dp_from(i), dp_peer(i)).wait_recv()
    for j in range(LEVELS):
        pdy[j] = dot(dyc[j], bfull[...], NN).astype(BF16)

    def project(left, right):
        return functools.reduce(jnp.add, [dot(left(j), right(j), TN) for j in range(LEVELS)])

    term[...] = project(lambda j: pdy[j], lambda j: hid[j])
    for i in range(1, n_dp):
        psend[i - 1] = term[rpart(dp_peer(i)), :].astype(BF16)
        proj_copy(i, dp_peer(i)).start()
    total[2] = term[rpart(my_dp), :]

    mate_copy(1).wait_recv()
    sx[1] = dot(pick2, tok2[...], NN).astype(BF16)
    dispatch_x(1, mate)

    def theirs(j):
        for i in range(1, n_dp):
            gu_copy(i, j, dp_peer(i)).wait_recv()
            row_grad(i, j)

    theirs(0)

    theirs(1)

    blocks(rx, n_ex - 2, x_s.at[0], x_r.at[0]).wait_recv()
    for j in range(LEVELS):
        xj = dot(spr[...], rx[lpart(j), :], NN).astype(BF16)
        if rk % 128:
            xp = dot(xj, bfull[...], NN).astype(BF16)
        for i in range(n_dp):
            if rk % 128:
                pj = dot(xp, rank_cols(dp_peer(i)), NN)
            else:
                pj = dot(xj, bfull[:, rpart(dp_peer(i))], NN)
            px[(i + n_dp - 1) % n_dp, j] = pj.astype(BF16)
    for i in range(1, n_dp):
        px_copy(i, dp_peer(i)).start()

    theirs(2)

    def x_term(s, i):
        left = px.at[n_dp - 1 + i]
        return project(lambda j: left[j], lambda j: gu[i, j, s])

    for s in range(2):
        total[s] = x_term(s, 0)

    stored = []

    def combine(i):
        blocks(rr.at[i], n_ex - 1, ret_s.at[i], ret_r.at[i]).wait_recv()
        in_v[i] = dot(pick_v[i], rr[i], TN).astype(BF16)

    combine(0)
    stored.append(pltpu.make_async_copy(in_v.at[0], in_h.at[:, wpart(my_dp)], out_s.at[3]))
    stored[-1].start()

    theirs(3)
    for i in range(1, n_dp):
        combine(i)
        in_copy(i, my_dp, dp_from(i)).start()

    for i in range(1, n_dp):
        proj_copy(i, dp_peer(i)).wait_recv()
        total[2] += prec[i - 1].astype(F32)
    stored.append(pltpu.make_async_copy(total.at[2], proj_h.at[2], out_s.at[2]))
    stored[-1].start()
    for i in range(1, n_dp):
        px_copy(i, dp_peer(i)).wait_recv()
        for s in range(2):
            total[s] += x_term(s, i)
    for s in range(2):
        stored.append(pltpu.make_async_copy(total.at[s], proj_h.at[s], out_s.at[s]))
        stored[-1].start()

    for i in range(1, n_dp):
        down_copy(i, my_dp, dp_peer(i)).wait_send()
        base_copy(i, my_dp, dp_peer(i)).wait_send()
        ids_copy(i, dp_peer(i)).wait_send()
        px_copy(i, dp_peer(i)).wait_send()
        proj_copy(i, dp_peer(i)).wait_send()
        for j in range(LEVELS):
            gu_copy(i, j, dp_peer(i)).wait_send()
    for n in range(4):
        mate_copy(n).wait_send()
    for m in range(2):
        blocks(rg, half - 1, dy_s.at[m], dy_r.at[0]).wait_send()
        blocks(rx, half - 1, x_s.at[m], x_r.at[0]).wait_send()
    for i in range(n_dp):
        blocks(rr.at[i], n_ex - 1, ret_s.at[i], ret_r.at[i]).wait_send()
    for copy in stored:
        copy.wait()
    for i in range(1, n_dp):
        in_copy(i, my_dp, dp_from(i)).wait_send()
        in_copy(i, dp_peer(i), dp_from(i)).wait_recv()


def finish(in_h, proj_h, in_ref, proj_ref, rows, proj, load_s, store_s):
    n = proj.shape[0]
    loads = [pltpu.make_async_copy(proj_h.at[t], proj.at[t], load_s.at[t]) for t in range(n)]
    loads.append(pltpu.make_async_copy(in_h, rows, load_s.at[n]))
    stores = [
        pltpu.make_async_copy(proj.at[t], proj_ref.at[0, t], store_s.at[t]) for t in range(n)
    ]
    stores.append(pltpu.make_async_copy(rows, in_ref, store_s.at[n]))
    for copy in loads:
        copy.start()
    for load, store in zip(loads, stores):
        load.wait()
        store.start()
    for copy in stores:
        copy.wait()


def body(
    tokens, out_grad, expert_ids, gate_probs, saved_pre, gate_weight, up_weight, down_weight, basis
):
    n_dp, n_ex = lax.axis_size("dp"), lax.axis_size("expert")
    tok_rows, width = tokens.shape
    topk = expert_ids.shape[1]
    slots, hidden2 = saved_pre.shape[2:]
    hidden = hidden2 // 2
    cap = slots // n_ex
    cp = max(16, 1 << (cap - 1).bit_length())
    rows = n_ex * cp
    nl = n_ex // LEVELS
    lrows = nl * cp
    lpad = -(-nl * cap // 16) * 16
    part = gate_weight.shape[1]
    rank = basis.shape[2]
    rk = rank // n_dp
    hbm = pl.BlockSpec(memory_space=pl.ANY)
    dma = pltpu.SemaphoreType.DMA
    scratch = [
        pltpu.VMEM((topk, tok_rows), jnp.int32),
        pltpu.VMEM((topk, tok_rows), F32),
        pltpu.VMEM((tok_rows, width), BF16),
        pltpu.VMEM((tok_rows, width), BF16),
        pltpu.VMEM((tok_rows, width), BF16),
        pltpu.VMEM((tok_rows, width), BF16),
        pltpu.VMEM((topk, tok_rows), jnp.int32),
        pltpu.VMEM((topk, tok_rows), F32),
        pltpu.VMEM((n_dp - 1, topk, tok_rows), jnp.int32),
        pltpu.VMEM((n_dp, rows, tok_rows), BF16),
        pltpu.VMEM((2, rows // 2, width), BF16),
        pltpu.VMEM((2, rows // 2, width), BF16),
        pltpu.VMEM((rows, width), BF16),
        pltpu.VMEM((rows, width), BF16),
        pltpu.VMEM((LEVELS, lpad, width), BF16),
        pltpu.VMEM((lpad, lrows), BF16),
        pltpu.VMEM((width, hidden), BF16),
        pltpu.VMEM((width, rank), BF16),
        pltpu.VMEM((part, hidden), BF16),
        pltpu.VMEM((part, hidden), BF16),
        pltpu.VMEM((LEVELS, lpad, hidden2), BF16),
        pltpu.VMEM((LEVELS, lpad, hidden), F32),
        pltpu.VMEM((LEVELS, lpad, hidden), F32),
        pltpu.VMEM((LEVELS, lpad, hidden), BF16),
        pltpu.VMEM((n_dp, LEVELS, 2, lpad, hidden), BF16),
        pltpu.VMEM((2 * n_dp - 1, LEVELS, lpad, rk), BF16),
        pltpu.VMEM((LEVELS, lpad, rank), BF16),
        pltpu.VMEM((n_dp, LEVELS, lrows, part), BF16),
        pltpu.VMEM((n_dp, rows, part), BF16),
        pltpu.VMEM((n_dp, tok_rows, part), BF16),
        pltpu.VMEM((n_dp - 1, rk, hidden), BF16),
        pltpu.VMEM((n_dp - 1, rk, hidden), BF16),
        pltpu.VMEM((rank, hidden), F32),
        pltpu.VMEM((3, rk, hidden), F32),
        dma((8,)), dma((LEVELS,)),
        dma((2,)), dma((LEVELS,)), dma((2,)), dma((1,)), dma((4,)), dma((4,)),
        dma((n_dp,)), dma((n_dp,)), dma((n_dp,)), dma((n_dp,)),
        dma((n_dp, LEVELS)), dma((n_dp, LEVELS)), dma((n_dp,)), dma((n_dp,)),
        dma((n_dp,)), dma((n_dp,)), dma((n_dp,)), dma((n_dp,)),
        dma((n_dp,)), dma((n_dp,)), dma((n_dp,)), dma((n_dp,)), dma((4,)),
    ]
    in_part, proj = pl.pallas_call(
        functools.partial(kernel, n_dp, n_ex, cap, cp),
        out_shape=(
            jax.ShapeDtypeStruct((tok_rows, width), BF16),
            jax.ShapeDtypeStruct((3, rk, hidden), F32),
        ),
        in_specs=[hbm] * 9,
        out_specs=(hbm, hbm),
        scratch_shapes=scratch,
        compiler_params=pltpu.CompilerParams(
            collective_id=0, has_side_effects=True, vmem_limit_bytes=60 * 1024 * 1024
        ),
    )(
        expert_ids.T, gate_probs.T, tokens, out_grad, saved_pre,
        gate_weight, up_weight, down_weight, basis,
    )
    return pl.pallas_call(
        finish,
        out_shape=(
            jax.ShapeDtypeStruct((tok_rows, width), BF16),
            jax.ShapeDtypeStruct((1, 3, rk, hidden), F32),
        ),
        in_specs=[hbm, hbm],
        out_specs=(hbm, hbm),
        scratch_shapes=[
            pltpu.VMEM((tok_rows, width), BF16),
            pltpu.VMEM((3, rk, hidden), F32),
            dma((4,)), dma((4,)),
        ],
    )(in_part, proj)


def solution(mesh):
    return jax.shard_map(
        body,
        mesh=mesh,
        in_specs=(
            P(("dp", "expert"), None),
            P(("dp", "expert"), None),
            P(("dp", "expert"), None),
            P(("dp", "expert"), None),
            P("dp", "expert", None, None),
            P("expert", "dp", None),
            P("expert", "dp", None),
            P("expert", "dp", None),
            P("expert", "dp", None),
        ),
        out_specs=(P(("dp", "expert"), None), P("expert", None, "dp", None)),
        check_vma=False,
    )
```

```python
import functools
import jax
import jax.numpy as jnp
from jax import lax
from jax.experimental import pallas as pl
from jax.experimental.pallas import tpu as pltpu
from jax.sharding import PartitionSpec as P

MESH = pl.DeviceIdType.MESH
F32 = jnp.float32
BF16 = jnp.bfloat16
LEVELS = 4


def dot(left, right, dims):
    return lax.dot_general(left, right, (dims, ((), ())), preferred_element_type=F32)


NN = ((1,), (0,))
TN = ((0,), (0,))
NT = ((1,), (1,))


def kernel(
    n_dp, n_ex, cap, cp,
    ids_h, probs_h, tok_h, og_h, pre_h, gw_h, uw_h, dw, bs,
    in_h, proj_h,
    ids, probs, tok, og, tok2, og2, ids2, probs2, idsd, pick_v, sx, sg, rx, rg, dyc, spr, dfull, bfull, gw, uw, pre,
    act_a, act_b, hid, gu, px, pdy, rs, rr, in_v, psend, prec, term, total,
    local_sem, pre_sem, dy_s, dy_r, x_s, x_r, mate_s, mate_r, down_s, down_r, base_s, base_r,
    gu_s, gu_r, ret_s, ret_r, px_s, px_r, proj_s, proj_r, in_s, in_r, ids_s, ids_r, out_s,
):
    my_dp = lax.axis_index("dp")
    me = lax.axis_index("expert")
    rows = n_ex * cp
    half = n_ex // 2
    nl = n_ex // LEVELS
    lrows = nl * cp
    lcap = nl * cap
    tokens, width = tok.shape
    topk = ids.shape[0]
    hidden = dfull.shape[1]
    part = width // n_dp
    rank = bfull.shape[1]
    rk = rank // n_dp
    shift = cp.bit_length() - 1
    fw = 256

    z = lax.div(me, nl)
    spot = lax.rem(me, nl)
    mate = lax.rem(me + half, n_ex)
    half0 = lax.div(me, half) * half
    levels = [z + 1 - 2 * lax.rem(z, 2), lax.rem(z + 2, LEVELS), LEVELS - 1 - z, z]
    own = LEVELS - 1

    def block(owner):
        return pl.ds(pl.multiple_of(owner * cp, cp), cp)

    def wpart(owner):
        return pl.ds(pl.multiple_of(owner * part, part), part)

    def rpart(owner):
        return pl.ds(pl.multiple_of(owner * rk, rk), rk)

    def rank_cols(owner):
        line = lax.broadcasted_iota(jnp.int32, (rank, rk), 0)
        lane = lax.broadcasted_iota(jnp.int32, (rank, rk), 1) + owner * rk
        return jnp.where(line == lane, one, zero).astype(BF16)

    def lpart(j):
        return pl.ds(pl.multiple_of(levels[j] * lrows, lrows), lrows)

    def ex_peer(k):
        return lax.rem(me + k, n_ex)

    def half_peer(k):
        return half0 + lax.rem(me - half0 + k, half)

    def in_level(j, t):
        return levels[j] * nl + lax.rem(spot + t, nl)

    def dp_peer(i):
        return lax.rem(my_dp + i, n_dp)

    def dp_from(i):
        return lax.rem(my_dp + n_dp - i, n_dp)

    first = [
        pltpu.make_async_copy(ids_h, ids, local_sem.at[6]),
        pltpu.make_async_copy(probs_h, probs, local_sem.at[7]),
    ]
    for copy in first:
        copy.start()

    pad = gu.shape[3] - lcap
    if pad:
        for j in range(LEVELS):
            pre[j, lcap:, :] = jnp.zeros((pad, 2 * hidden), BF16)
            for i in range(1, n_dp):
                for s in range(2):
                    gu[i, j, s, lcap:, :] = jnp.zeros((pad, hidden), BF16)

    barrier = pltpu.get_barrier_semaphore()

    for i in range(1, n_dp):
        pl.semaphore_signal(barrier, inc=1, device_id={"dp": dp_peer(i)}, device_id_type=MESH)

    @pl.loop(1, n_ex)
    def _(k):
        pl.semaphore_signal(barrier, inc=1, device_id={"expert": ex_peer(k)}, device_id_type=MESH)

    local = [
        pltpu.make_async_copy(og_h, og, local_sem.at[0]),
        pltpu.make_async_copy(tok_h, tok, local_sem.at[1]),
        pltpu.make_async_copy(dw.at[0], dfull.at[wpart(my_dp)], local_sem.at[2]),
        pltpu.make_async_copy(bs.at[0], bfull.at[wpart(my_dp)], local_sem.at[3]),
        pltpu.make_async_copy(gw_h.at[0], gw, local_sem.at[4]),
        pltpu.make_async_copy(uw_h.at[0], uw, local_sem.at[5]),
    ]
    pre_copy = []
    for j in range(LEVELS):
        src = pl.ds(pl.multiple_of(levels[j] * lcap, 8), lcap)
        pre_copy.append(
            pltpu.make_async_copy(pre_h.at[0, 0, src], pre.at[j, pl.ds(0, lcap)], pre_sem.at[j])
        )
    for copy in local[:2] + pre_copy + local[2:]:
        copy.start()

    one, zero = jnp.ones((), F32), jnp.zeros((), F32)
    earlier = lax.broadcasted_iota(jnp.int32, (tokens, tokens), 0) < lax.broadcasted_iota(
        jnp.int32, (tokens, tokens), 1
    )
    earlier = jnp.where(earlier, one, zero).astype(BF16)

    def pick_of(names_of, first, count):
        line = lax.broadcasted_iota(jnp.int32, (count, tokens), 0)
        line_expert = lax.shift_right_logical(line, shift) + first
        line_slot = lax.bitwise_and(line, cp - 1)
        names = [names_of[k : k + 1, :] == line_expert for k in range(topk)]
        any_name = functools.reduce(jnp.logical_or, names)
        named = jnp.where(any_name, one, zero).astype(BF16)
        before = dot(named, earlier, NN)
        at_slot = before == line_slot.astype(F32)
        pick = jnp.where(jnp.logical_and(any_name, at_slot), one, zero).astype(BF16)
        return pick, names, at_slot

    def half_pick(names_of, weights_of):
        pick, names, at_slot = pick_of(names_of, half0, half * cp)
        weights = functools.reduce(
            jnp.add, [jnp.where(name, weights_of[k : k + 1, :], zero) for k, name in enumerate(names)]
        )
        return pick, jnp.sum(jnp.where(at_slot, weights, zero), axis=1, keepdims=True)

    for copy in first:
        copy.wait()
    pick, weight = half_pick(ids, probs)

    pl.semaphore_wait(barrier, n_ex - 1 + n_dp - 1)

    def down_copy(i, owner, peer):
        return pltpu.make_async_remote_copy(
            dw.at[0], dfull.at[wpart(owner)], down_s.at[i], down_r.at[i],
            device_id={"dp": peer}, device_id_type=MESH,
        )

    def base_copy(i, owner, peer):
        return pltpu.make_async_remote_copy(
            bs.at[0], bfull.at[wpart(owner)], base_s.at[i], base_r.at[i],
            device_id={"dp": peer}, device_id_type=MESH,
        )

    def ids_copy(i, peer):
        return pltpu.make_async_remote_copy(
            ids, idsd.at[i - 1], ids_s.at[i], ids_r.at[i],
            device_id={"dp": peer}, device_id_type=MESH,
        )

    def mate_copy(n):
        src, dst = ((og, og2), (tok, tok2), (ids, ids2), (probs, probs2))[n]
        return pltpu.make_async_remote_copy(
            src, dst, mate_s.at[n], mate_r.at[n], device_id={"expert": mate}, device_id_type=MESH
        )

    def dy_copy(m, peer, owner, j):
        return pltpu.make_async_remote_copy(
            sg.at[m, block(peer - half0)], rg.at[block(owner)], dy_s.at[m], dy_r.at[j],
            device_id={"expert": peer}, device_id_type=MESH,
        )

    def x_copy(m, peer, owner):
        return pltpu.make_async_remote_copy(
            sx.at[m, block(peer - half0)], rx.at[block(owner)], x_s.at[m], x_r.at[0],
            device_id={"expert": peer}, device_id_type=MESH,
        )

    def blocks(buffer, count, send, recv):
        span = buffer.at[pl.ds(0, count * cp)]
        return pltpu.make_async_remote_copy(
            span, span, send, recv, device_id={"expert": mate}, device_id_type=MESH
        )

    def gu_copy(i, j, peer):
        used = pl.ds(0, lcap)
        return pltpu.make_async_remote_copy(
            gu.at[0, j, :, used], gu.at[i, j, :, used], gu_s.at[i, j], gu_r.at[i, j],
            device_id={"dp": peer}, device_id_type=MESH,
        )

    def px_copy(i, peer):
        return pltpu.make_async_remote_copy(
            px.at[i - 1], px.at[n_dp - 1 + i], px_s.at[i], px_r.at[i],
            device_id={"dp": peer}, device_id_type=MESH,
        )

    def ret_copy(i, j, peer, owner):
        return pltpu.make_async_remote_copy(
            rs.at[i, j, block(lax.rem(peer, nl))], rr.at[i, block(owner)],
            ret_s.at[i], ret_r.at[i],
            device_id={"expert": peer}, device_id_type=MESH,
        )

    def proj_copy(i, peer):
        return pltpu.make_async_remote_copy(
            psend.at[i - 1], prec.at[i - 1], proj_s.at[i], proj_r.at[i],
            device_id={"dp": peer}, device_id_type=MESH,
        )

    def in_copy(i, owner, peer):
        return pltpu.make_async_remote_copy(
            in_v.at[i], in_h.at[:, wpart(owner)], in_s.at[i], in_r.at[i],
            device_id={"dp": peer}, device_id_type=MESH,
        )

    for i in range(1, n_dp):
        ids_copy(i, dp_peer(i)).start()
    for i in range(1, n_dp):
        down_copy(i, my_dp, dp_peer(i)).start()
    mate_copy(2).start()
    mate_copy(3).start()
    local[0].wait()
    mate_copy(0).start()
    for i in range(1, n_dp):
        base_copy(i, my_dp, dp_peer(i)).start()

    def dispatch_dy(m, owner):
        for near, tag in ((0, 0 if m == 0 else 2), (own, own if m == 0 else 1)):

            @pl.loop(int(near == own), nl)
            def _(t):
                dy_copy(m, in_level(near, t), owner, tag).start()

        rg[block(owner), :] = sg[m, block(me - half0), :]

    def dispatch_x(m, owner):
        @pl.loop(1, half)
        def _(k):
            x_copy(m, half_peer(k), owner).start()

        rx[block(owner), :] = sx[m, block(me - half0), :]

    sg[0] = (dot(pick, og[...], NN) * weight).astype(BF16)
    dispatch_dy(0, me)
    local[1].wait()
    mate_copy(1).start()
    sx[0] = dot(pick, tok[...], NN).astype(BF16)
    dispatch_x(0, me)

    grid = (gu.shape[3], lrows)
    line = lax.broadcasted_iota(jnp.int32, grid, 1)
    inner = lax.bitwise_and(line, cp - 1)
    target = lax.shift_right_logical(line, shift) * cap + inner
    spread = jnp.logical_and(target == lax.broadcasted_iota(jnp.int32, grid, 0), inner < cap)
    spr[...] = jnp.where(spread, one, zero).astype(BF16)

    for j in range(LEVELS):
        pre_copy[j].wait()
        for f in range(0, hidden, fw):
            cols = slice(f, f + fw)
            g = pre[j, :, f : f + fw].astype(F32)
            u = pre[j, :, hidden + f : hidden + f + fw].astype(F32)
            sig = jax.nn.sigmoid(g)
            gs = g * sig
            act_a[j, :, cols] = gs
            hid[j, :, cols] = (gs * u).astype(BF16)
            act_b[j, :, cols] = u * sig * (1.0 + g * (1.0 - sig))

    def row_grad(i, j):
        out = dot(gu[i, j, 0], gw[...], NT) + dot(gu[i, j, 1], uw[...], NT)
        rs[i, j] = dot(spr[...], out.astype(BF16), TN).astype(BF16)

        @pl.loop(int(j == own), nl)
        def _(t):
            ret_copy(i, j, in_level(j, t), me).start()

        if j == own:
            rr[i, block(me), :] = rs[i, j, block(spot), :]

    pick_v[0] = pick_of(ids, 0, rows)[0]
    for i in range(1, n_dp):
        ids_copy(i, dp_peer(i)).wait_recv()
        pick_v[i] = pick_of(idsd.at[i - 1], 0, rows)[0]

    mate_copy(2).wait_recv()
    mate_copy(3).wait_recv()
    pick2, weight2 = half_pick(ids2, probs2)
    mate_copy(0).wait_recv()
    sg[1] = (dot(pick2, og2[...], NN) * weight2).astype(BF16)
    dispatch_dy(1, mate)

    local[2].wait()
    for i in range(1, n_dp):
        down_copy(i, dp_from(i), dp_peer(i)).wait_recv()

    for j in range(LEVELS):

        blocks(rg, nl - j % 2, dy_s.at[0], dy_r.at[j]).wait_recv()
        dyc[j] = dot(spr[...], rg[lpart(j), :], NN).astype(BF16)
        for f in range(0, hidden, fw):
            cols = slice(f, f + fw)
            hg = dot(dyc[j], dfull[:, cols], NN)
            gu[0, j, 1, :, cols] = (hg * act_a[j, :, cols]).astype(BF16)
            gu[0, j, 0, :, cols] = (hg * act_b[j, :, cols]).astype(BF16)
        for i in range(1, n_dp):
            gu_copy(i, j, dp_peer(i)).start()
        if j == 0:
            local[4].wait()
            local[5].wait()
        row_grad(0, j)

    local[3].wait()
    for i in range(1, n_dp):
        base_copy(i, dp_from(i), dp_peer(i)).wait_recv()
    for j in range(LEVELS):
        pdy[j] = dot(dyc[j], bfull[...], NN).astype(BF16)

    def project(left, right):
        return functools.reduce(jnp.add, [dot(left(j), right(j), TN) for j in range(LEVELS)])

    term[...] = project(lambda j: pdy[j], lambda j: hid[j])
    for i in range(1, n_dp):
        psend[i - 1] = term[rpart(dp_peer(i)), :].astype(BF16)
        proj_copy(i, dp_peer(i)).start()
    total[2] = term[rpart(my_dp), :]

    mate_copy(1).wait_recv()
    sx[1] = dot(pick2, tok2[...], NN).astype(BF16)
    dispatch_x(1, mate)

    def theirs(j):
        for i in range(1, n_dp):
            gu_copy(i, j, dp_peer(i)).wait_recv()
            row_grad(i, j)

    theirs(0)

    theirs(1)

    blocks(rx, n_ex - 2, x_s.at[0], x_r.at[0]).wait_recv()
    for j in range(LEVELS):
        xj = dot(spr[...], rx[lpart(j), :], NN).astype(BF16)
        if rk % 128:
            xp = dot(xj, bfull[...], NN).astype(BF16)
        for i in range(n_dp):
            if rk % 128:
                pj = dot(xp, rank_cols(dp_peer(i)), NN)
            else:
                pj = dot(xj, bfull[:, rpart(dp_peer(i))], NN)
            px[(i + n_dp - 1) % n_dp, j] = pj.astype(BF16)
    for i in range(1, n_dp):
        px_copy(i, dp_peer(i)).start()

    theirs(2)

    def x_term(s, i):
        left = px.at[n_dp - 1 + i]
        return project(lambda j: left[j], lambda j: gu[i, j, s])

    for s in range(2):
        total[s] = x_term(s, 0)

    stored = []

    def combine(i):
        blocks(rr.at[i], n_ex - 1, ret_s.at[i], ret_r.at[i]).wait_recv()
        in_v[i] = dot(pick_v[i], rr[i], TN).astype(BF16)

    combine(0)
    stored.append(pltpu.make_async_copy(in_v.at[0], in_h.at[:, wpart(my_dp)], out_s.at[3]))
    stored[-1].start()

    theirs(3)
    for i in range(1, n_dp):
        combine(i)
        in_copy(i, my_dp, dp_from(i)).start()

    for i in range(1, n_dp):
        proj_copy(i, dp_peer(i)).wait_recv()
        total[2] += prec[i - 1].astype(F32)
    stored.append(pltpu.make_async_copy(total.at[2], proj_h.at[2], out_s.at[2]))
    stored[-1].start()
    for i in range(1, n_dp):
        px_copy(i, dp_peer(i)).wait_recv()
        for s in range(2):
            total[s] += x_term(s, i)
    for s in range(2):
        stored.append(pltpu.make_async_copy(total.at[s], proj_h.at[s], out_s.at[s]))
        stored[-1].start()

    for i in range(1, n_dp):
        down_copy(i, my_dp, dp_peer(i)).wait_send()
        base_copy(i, my_dp, dp_peer(i)).wait_send()
        ids_copy(i, dp_peer(i)).wait_send()
        px_copy(i, dp_peer(i)).wait_send()
        proj_copy(i, dp_peer(i)).wait_send()
        for j in range(LEVELS):
            gu_copy(i, j, dp_peer(i)).wait_send()
    for n in range(4):
        mate_copy(n).wait_send()
    for m in range(2):
        blocks(rg, half - 1, dy_s.at[m], dy_r.at[0]).wait_send()
        blocks(rx, half - 1, x_s.at[m], x_r.at[0]).wait_send()
    for i in range(n_dp):
        blocks(rr.at[i], n_ex - 1, ret_s.at[i], ret_r.at[i]).wait_send()
    for copy in stored:
        copy.wait()
    for i in range(1, n_dp):
        in_copy(i, my_dp, dp_from(i)).wait_send()
        in_copy(i, dp_peer(i), dp_from(i)).wait_recv()


def finish(in_h, proj_h, in_ref, proj_ref, rows, proj, load_s, store_s):
    n = proj.shape[0]
    loads = [pltpu.make_async_copy(proj_h.at[t], proj.at[t], load_s.at[t]) for t in range(n)]
    loads.append(pltpu.make_async_copy(in_h, rows, load_s.at[n]))
    stores = [
        pltpu.make_async_copy(proj.at[t], proj_ref.at[0, t], store_s.at[t]) for t in range(n)
    ]
    stores.append(pltpu.make_async_copy(rows, in_ref, store_s.at[n]))
    for copy in loads:
        copy.start()
    for load, store in zip(loads, stores):
        load.wait()
        store.start()
    for copy in stores:
        copy.wait()


def body(
    tokens, out_grad, expert_ids, gate_probs, saved_pre, gate_weight, up_weight, down_weight, basis
):
    n_dp, n_ex = lax.axis_size("dp"), lax.axis_size("expert")
    tok_rows, width = tokens.shape
    topk = expert_ids.shape[1]
    slots, hidden2 = saved_pre.shape[2:]
    hidden = hidden2 // 2
    cap = slots // n_ex
    cp = max(16, 1 << (cap - 1).bit_length())
    rows = n_ex * cp
    nl = n_ex // LEVELS
    lrows = nl * cp
    lpad = -(-nl * cap // 16) * 16
    part = gate_weight.shape[1]
    rank = basis.shape[2]
    rk = rank // n_dp
    hbm = pl.BlockSpec(memory_space=pl.ANY)
    dma = pltpu.SemaphoreType.DMA
    scratch = [
        pltpu.VMEM((topk, tok_rows), jnp.int32),
        pltpu.VMEM((topk, tok_rows), F32),
        pltpu.VMEM((tok_rows, width), BF16),
        pltpu.VMEM((tok_rows, width), BF16),
        pltpu.VMEM((tok_rows, width), BF16),
        pltpu.VMEM((tok_rows, width), BF16),
        pltpu.VMEM((topk, tok_rows), jnp.int32),
        pltpu.VMEM((topk, tok_rows), F32),
        pltpu.VMEM((n_dp - 1, topk, tok_rows), jnp.int32),
        pltpu.VMEM((n_dp, rows, tok_rows), BF16),
        pltpu.VMEM((2, rows // 2, width), BF16),
        pltpu.VMEM((2, rows // 2, width), BF16),
        pltpu.VMEM((rows, width), BF16),
        pltpu.VMEM((rows, width), BF16),
        pltpu.VMEM((LEVELS, lpad, width), BF16),
        pltpu.VMEM((lpad, lrows), BF16),
        pltpu.VMEM((width, hidden), BF16),
        pltpu.VMEM((width, rank), BF16),
        pltpu.VMEM((part, hidden), BF16),
        pltpu.VMEM((part, hidden), BF16),
        pltpu.VMEM((LEVELS, lpad, hidden2), BF16),
        pltpu.VMEM((LEVELS, lpad, hidden), F32),
        pltpu.VMEM((LEVELS, lpad, hidden), F32),
        pltpu.VMEM((LEVELS, lpad, hidden), BF16),
        pltpu.VMEM((n_dp, LEVELS, 2, lpad, hidden), BF16),
        pltpu.VMEM((2 * n_dp - 1, LEVELS, lpad, rk), BF16),
        pltpu.VMEM((LEVELS, lpad, rank), BF16),
        pltpu.VMEM((n_dp, LEVELS, lrows, part), BF16),
        pltpu.VMEM((n_dp, rows, part), BF16),
        pltpu.VMEM((n_dp, tok_rows, part), BF16),
        pltpu.VMEM((n_dp - 1, rk, hidden), BF16),
        pltpu.VMEM((n_dp - 1, rk, hidden), BF16),
        pltpu.VMEM((rank, hidden), F32),
        pltpu.VMEM((3, rk, hidden), F32),
        dma((8,)), dma((LEVELS,)),
        dma((2,)), dma((LEVELS,)), dma((2,)), dma((1,)), dma((4,)), dma((4,)),
        dma((n_dp,)), dma((n_dp,)), dma((n_dp,)), dma((n_dp,)),
        dma((n_dp, LEVELS)), dma((n_dp, LEVELS)), dma((n_dp,)), dma((n_dp,)),
        dma((n_dp,)), dma((n_dp,)), dma((n_dp,)), dma((n_dp,)),
        dma((n_dp,)), dma((n_dp,)), dma((n_dp,)), dma((n_dp,)), dma((4,)),
    ]
    in_part, proj = pl.pallas_call(
        functools.partial(kernel, n_dp, n_ex, cap, cp),
        out_shape=(
            jax.ShapeDtypeStruct((tok_rows, width), BF16),
            jax.ShapeDtypeStruct((3, rk, hidden), F32),
        ),
        in_specs=[hbm] * 9,
        out_specs=(hbm, hbm),
        scratch_shapes=scratch,
        compiler_params=pltpu.CompilerParams(
            collective_id=0, has_side_effects=True, vmem_limit_bytes=60 * 1024 * 1024
        ),
    )(
        expert_ids.T, gate_probs.T, tokens, out_grad, saved_pre,
        gate_weight, up_weight, down_weight, basis,
    )
    return pl.pallas_call(
        finish,
        out_shape=(
            jax.ShapeDtypeStruct((tok_rows, width), BF16),
            jax.ShapeDtypeStruct((1, 3, rk, hidden), F32),
        ),
        in_specs=[hbm, hbm],
        out_specs=(hbm, hbm),
        scratch_shapes=[
            pltpu.VMEM((tok_rows, width), BF16),
            pltpu.VMEM((3, rk, hidden), F32),
            dma((4,)), dma((4,)),
        ],
    )(in_part, proj)


def solution(mesh):
    return jax.shard_map(
        body,
        mesh=mesh,
        in_specs=(
            P(("dp", "expert"), None),
            P(("dp", "expert"), None),
            P(("dp", "expert"), None),
            P(("dp", "expert"), None),
            P("dp", "expert", None, None),
            P("expert", "dp", None),
            P("expert", "dp", None),
            P("expert", "dp", None),
            P("expert", "dp", None),
        ),
        out_specs=(P(("dp", "expert"), None), P("expert", None, "dp", None)),
        check_vma=False,
    )
```

```python
import functools
import jax
import jax.numpy as jnp
from jax import lax
from jax.experimental import pallas as pl
from jax.experimental.pallas import tpu as pltpu
from jax.sharding import PartitionSpec as P

MESH = pl.DeviceIdType.MESH
F32 = jnp.float32
BF16 = jnp.bfloat16
LEVELS = 4
VMEM_BYTES = 67043328


def dot(left, right, dims):
    return lax.dot_general(left, right, (dims, ((), ())), preferred_element_type=F32)


NN = ((1,), (0,))
TN = ((0,), (0,))
NT = ((1,), (1,))


def kernel(
    n_dp, n_ex, cap, cp,
    ids_h, probs_h, tok_h, og_h, pre_h, gw_h, uw_h, dw, bs,
    in_out, total,
    ids, probs, tok, og, tok2, og2, ids2, probs2, idsd, pick_v, sx, sg, rx, rg, dyc, spr, dfull, bfull, gw, uw, pre,
    act_a, act_b, hid, gu, px, pdy, rs, rr, in_v, psend, prec, term,
    local_sem, pre_sem, dy_s, dy_r, x_s, x_r, mate_s, mate_r, down_s, down_r, base_s, base_r,
    gu_s, gu_r, ret_s, ret_r, px_s, px_r, proj_s, proj_r, in_s, in_r, ids_s, ids_r,
):
    my_dp = lax.axis_index("dp")
    me = lax.axis_index("expert")
    rows = n_ex * cp
    half = n_ex // 2
    nl = n_ex // LEVELS
    lrows = nl * cp
    lcap = nl * cap
    tokens, width = tok.shape
    topk = ids.shape[0]
    hidden = dfull.shape[1]
    part = width // n_dp
    rank = bfull.shape[1]
    rk = rank // n_dp
    shift = cp.bit_length() - 1
    fw = 256

    z = lax.div(me, nl)
    spot = lax.rem(me, nl)
    mate = lax.rem(me + half, n_ex)
    half0 = lax.div(me, half) * half
    levels = [z + 1 - 2 * lax.rem(z, 2), lax.rem(z + 2, LEVELS), LEVELS - 1 - z, z]
    own = LEVELS - 1

    def block(owner):
        return pl.ds(pl.multiple_of(owner * cp, cp), cp)

    def wpart(owner):
        return pl.ds(pl.multiple_of(owner * part, part), part)

    def rpart(owner):
        return pl.ds(pl.multiple_of(owner * rk, rk), rk)

    def rank_cols(owner):
        line = lax.broadcasted_iota(jnp.int32, (rank, rk), 0)
        lane = lax.broadcasted_iota(jnp.int32, (rank, rk), 1) + owner * rk
        return jnp.where(line == lane, one, zero).astype(BF16)

    def lpart(j):
        return pl.ds(pl.multiple_of(levels[j] * lrows, lrows), lrows)

    def ex_peer(k):
        return lax.rem(me + k, n_ex)

    def half_peer(k):
        return half0 + lax.rem(me - half0 + k, half)

    def in_level(j, t):
        return levels[j] * nl + lax.rem(spot + t, nl)

    def dp_peer(i):
        return lax.rem(my_dp + i, n_dp)

    def dp_from(i):
        return lax.rem(my_dp + n_dp - i, n_dp)

    first = [
        pltpu.make_async_copy(ids_h, ids, local_sem.at[6]),
        pltpu.make_async_copy(probs_h, probs, local_sem.at[7]),
    ]
    for copy in first:
        copy.start()

    pad = gu.shape[3] - lcap
    if pad:
        for j in range(LEVELS):
            pre[j, lcap:, :] = jnp.zeros((pad, 2 * hidden), BF16)
            for i in range(1, n_dp):
                for s in range(2):
                    gu[i, j, s, lcap:, :] = jnp.zeros((pad, hidden), BF16)

    barrier = pltpu.get_barrier_semaphore()

    for i in range(1, n_dp):
        pl.semaphore_signal(barrier, inc=1, device_id={"dp": dp_peer(i)}, device_id_type=MESH)

    @pl.loop(1, n_ex)
    def _(k):
        pl.semaphore_signal(barrier, inc=1, device_id={"expert": ex_peer(k)}, device_id_type=MESH)

    local = [
        pltpu.make_async_copy(og_h, og, local_sem.at[0]),
        pltpu.make_async_copy(tok_h, tok, local_sem.at[1]),
        pltpu.make_async_copy(dw.at[0], dfull.at[wpart(my_dp)], local_sem.at[2]),
        pltpu.make_async_copy(bs.at[0], bfull.at[wpart(my_dp)], local_sem.at[3]),
        pltpu.make_async_copy(gw_h.at[0], gw, local_sem.at[4]),
        pltpu.make_async_copy(uw_h.at[0], uw, local_sem.at[5]),
    ]
    pre_copy = []
    for j in range(LEVELS):
        src = pl.ds(pl.multiple_of(levels[j] * lcap, 8), lcap)
        pre_copy.append(
            pltpu.make_async_copy(pre_h.at[0, 0, src], pre.at[j, pl.ds(0, lcap)], pre_sem.at[j])
        )
    for copy in local[:2] + pre_copy + local[2:]:
        copy.start()

    one, zero = jnp.ones((), F32), jnp.zeros((), F32)
    earlier = lax.broadcasted_iota(jnp.int32, (tokens, tokens), 0) < lax.broadcasted_iota(
        jnp.int32, (tokens, tokens), 1
    )
    earlier = jnp.where(earlier, one, zero).astype(BF16)

    def pick_of(names_of, first, count):
        line = lax.broadcasted_iota(jnp.int32, (count, tokens), 0)
        line_expert = lax.shift_right_logical(line, shift) + first
        line_slot = lax.bitwise_and(line, cp - 1)
        names = [names_of[k : k + 1, :] == line_expert for k in range(topk)]
        any_name = functools.reduce(jnp.logical_or, names)
        named = jnp.where(any_name, one, zero).astype(BF16)
        before = dot(named, earlier, NN)
        at_slot = before == line_slot.astype(F32)
        pick = jnp.where(jnp.logical_and(any_name, at_slot), one, zero).astype(BF16)
        return pick, names, at_slot

    def half_pick(names_of, weights_of):
        pick, names, at_slot = pick_of(names_of, half0, half * cp)
        weights = functools.reduce(
            jnp.add, [jnp.where(name, weights_of[k : k + 1, :], zero) for k, name in enumerate(names)]
        )
        return pick, jnp.sum(jnp.where(at_slot, weights, zero), axis=1, keepdims=True)

    for copy in first:
        copy.wait()
    pick, weight = half_pick(ids, probs)

    pl.semaphore_wait(barrier, n_ex - 1 + n_dp - 1)

    def down_copy(i, owner, peer):
        return pltpu.make_async_remote_copy(
            dw.at[0], dfull.at[wpart(owner)], down_s.at[i], down_r.at[i],
            device_id={"dp": peer}, device_id_type=MESH,
        )

    def base_copy(i, owner, peer):
        return pltpu.make_async_remote_copy(
            bs.at[0], bfull.at[wpart(owner)], base_s.at[i], base_r.at[i],
            device_id={"dp": peer}, device_id_type=MESH,
        )

    def ids_copy(i, peer):
        return pltpu.make_async_remote_copy(
            ids, idsd.at[i - 1], ids_s.at[i], ids_r.at[i],
            device_id={"dp": peer}, device_id_type=MESH,
        )

    def mate_copy(n):
        src, dst = ((og, og2), (tok, tok2), (ids, ids2), (probs, probs2))[n]
        return pltpu.make_async_remote_copy(
            src, dst, mate_s.at[n], mate_r.at[n], device_id={"expert": mate}, device_id_type=MESH
        )

    def dy_copy(m, peer, owner, j):
        return pltpu.make_async_remote_copy(
            sg.at[m, block(peer - half0)], rg.at[block(owner)], dy_s.at[m], dy_r.at[j],
            device_id={"expert": peer}, device_id_type=MESH,
        )

    def x_copy(m, peer, owner):
        return pltpu.make_async_remote_copy(
            sx.at[m, block(peer - half0)], rx.at[block(owner)], x_s.at[m], x_r.at[0],
            device_id={"expert": peer}, device_id_type=MESH,
        )

    def blocks(buffer, count, send, recv):
        span = buffer.at[pl.ds(0, count * cp)]
        return pltpu.make_async_remote_copy(
            span, span, send, recv, device_id={"expert": mate}, device_id_type=MESH
        )

    def gu_copy(i, j, peer):
        used = pl.ds(0, lcap)
        return pltpu.make_async_remote_copy(
            gu.at[0, j, :, used], gu.at[i, j, :, used], gu_s.at[i, j], gu_r.at[i, j],
            device_id={"dp": peer}, device_id_type=MESH,
        )

    def px_copy(i, peer):
        return pltpu.make_async_remote_copy(
            px.at[i - 1], px.at[n_dp - 1 + i], px_s.at[i], px_r.at[i],
            device_id={"dp": peer}, device_id_type=MESH,
        )

    def ret_copy(i, j, peer, owner):
        return pltpu.make_async_remote_copy(
            rs.at[i, j, block(lax.rem(peer, nl))], rr.at[i, block(owner)],
            ret_s.at[i], ret_r.at[i],
            device_id={"expert": peer}, device_id_type=MESH,
        )

    def proj_copy(i, peer):
        return pltpu.make_async_remote_copy(
            psend.at[i - 1], prec.at[i - 1], proj_s.at[i], proj_r.at[i],
            device_id={"dp": peer}, device_id_type=MESH,
        )

    def in_copy(i, owner, peer):
        return pltpu.make_async_remote_copy(
            in_v.at[i - 1], in_out.at[:, wpart(owner)], in_s.at[i], in_r.at[i],
            device_id={"dp": peer}, device_id_type=MESH,
        )

    for i in range(1, n_dp):
        ids_copy(i, dp_peer(i)).start()
    for i in range(1, n_dp):
        down_copy(i, my_dp, dp_peer(i)).start()
    mate_copy(2).start()
    mate_copy(3).start()
    local[0].wait()
    mate_copy(0).start()
    for i in range(1, n_dp):
        base_copy(i, my_dp, dp_peer(i)).start()

    def dispatch_dy(m, owner):
        for near, tag in ((0, 0 if m == 0 else 2), (own, own if m == 0 else 1)):

            @pl.loop(int(near == own), nl)
            def _(t):
                dy_copy(m, in_level(near, t), owner, tag).start()

        rg[block(owner), :] = sg[m, block(me - half0), :]

    def dispatch_x(m, owner):
        @pl.loop(1, half)
        def _(k):
            x_copy(m, half_peer(k), owner).start()

        rx[block(owner), :] = sx[m, block(me - half0), :]

    sg[0] = (dot(pick, og[...], NN) * weight).astype(BF16)
    dispatch_dy(0, me)
    local[1].wait()
    mate_copy(1).start()
    sx[0] = dot(pick, tok[...], NN).astype(BF16)
    dispatch_x(0, me)

    grid = (gu.shape[3], lrows)
    line = lax.broadcasted_iota(jnp.int32, grid, 1)
    inner = lax.bitwise_and(line, cp - 1)
    target = lax.shift_right_logical(line, shift) * cap + inner
    spread = jnp.logical_and(target == lax.broadcasted_iota(jnp.int32, grid, 0), inner < cap)
    spr[...] = jnp.where(spread, one, zero).astype(BF16)

    for j in range(LEVELS):
        pre_copy[j].wait()
        for f in range(0, hidden, fw):
            cols = slice(f, f + fw)
            g = pre[j, :, f : f + fw].astype(F32)
            u = pre[j, :, hidden + f : hidden + f + fw].astype(F32)
            sig = jax.nn.sigmoid(g)
            gs = g * sig
            act_a[j, :, cols] = gs
            hid[j, :, cols] = (gs * u).astype(BF16)
            act_b[j, :, cols] = u * sig * (1.0 + g * (1.0 - sig))

    def row_grad(i, j):
        out = dot(gu[i, j, 0], gw[...], NT) + dot(gu[i, j, 1], uw[...], NT)
        rs[i, j] = dot(spr[...], out.astype(BF16), TN).astype(BF16)

        @pl.loop(int(j == own), nl)
        def _(t):
            ret_copy(i, j, in_level(j, t), me).start()

        if j == own:
            rr[i, block(me), :] = rs[i, j, block(spot), :]

    pick_v[0] = pick_of(ids, 0, rows)[0]
    for i in range(1, n_dp):
        ids_copy(i, dp_peer(i)).wait_recv()
        pick_v[i] = pick_of(idsd.at[i - 1], 0, rows)[0]

    mate_copy(2).wait_recv()
    mate_copy(3).wait_recv()
    pick2, weight2 = half_pick(ids2, probs2)
    mate_copy(0).wait_recv()
    sg[1] = (dot(pick2, og2[...], NN) * weight2).astype(BF16)
    dispatch_dy(1, mate)

    local[2].wait()
    for i in range(1, n_dp):
        down_copy(i, dp_from(i), dp_peer(i)).wait_recv()

    for j in range(LEVELS):

        blocks(rg, nl - j % 2, dy_s.at[0], dy_r.at[j]).wait_recv()
        dyc[j] = dot(spr[...], rg[lpart(j), :], NN).astype(BF16)
        for f in range(0, hidden, fw):
            cols = slice(f, f + fw)
            hg = dot(dyc[j], dfull[:, cols], NN)
            gu[0, j, 1, :, cols] = (hg * act_a[j, :, cols]).astype(BF16)
            gu[0, j, 0, :, cols] = (hg * act_b[j, :, cols]).astype(BF16)
        for i in range(1, n_dp):
            gu_copy(i, j, dp_peer(i)).start()
        if j == 0:
            local[4].wait()
            local[5].wait()
        row_grad(0, j)

    local[3].wait()
    for i in range(1, n_dp):
        base_copy(i, dp_from(i), dp_peer(i)).wait_recv()
    for j in range(LEVELS):
        pdy[j] = dot(dyc[j], bfull[...], NN).astype(BF16)

    def project(left, right):
        return functools.reduce(jnp.add, [dot(left(j), right(j), TN) for j in range(LEVELS)])

    term[...] = project(lambda j: pdy[j], lambda j: hid[j])
    for i in range(1, n_dp):
        psend[i - 1] = term[rpart(dp_peer(i)), :].astype(BF16)
        proj_copy(i, dp_peer(i)).start()
    total[2] = term[rpart(my_dp), :]

    mate_copy(1).wait_recv()
    sx[1] = dot(pick2, tok2[...], NN).astype(BF16)
    dispatch_x(1, mate)

    def theirs(j):
        for i in range(1, n_dp):
            gu_copy(i, j, dp_peer(i)).wait_recv()
            row_grad(i, j)

    theirs(0)

    theirs(1)

    blocks(rx, n_ex - 2, x_s.at[0], x_r.at[0]).wait_recv()
    for j in range(LEVELS):
        xj = dot(spr[...], rx[lpart(j), :], NN).astype(BF16)
        if rk % 128:
            xp = dot(xj, bfull[...], NN).astype(BF16)
        for i in range(n_dp):
            if rk % 128:
                pj = dot(xp, rank_cols(dp_peer(i)), NN)
            else:
                pj = dot(xj, bfull[:, rpart(dp_peer(i))], NN)
            px[(i + n_dp - 1) % n_dp, j] = pj.astype(BF16)
    for i in range(1, n_dp):
        px_copy(i, dp_peer(i)).start()

    theirs(2)

    def x_term(s, i):
        left = px.at[n_dp - 1 + i]
        return project(lambda j: left[j], lambda j: gu[i, j, s])

    for s in range(2):
        total[s] = x_term(s, 0)

    def combine(i):
        blocks(rr.at[i], n_ex - 1, ret_s.at[i], ret_r.at[i]).wait_recv()
        return dot(pick_v[i], rr[i], TN).astype(BF16)

    in_out[:, wpart(my_dp)] = combine(0)

    theirs(3)
    for i in range(1, n_dp):
        in_v[i - 1] = combine(i)
        in_copy(i, my_dp, dp_from(i)).start()

    for i in range(1, n_dp):
        proj_copy(i, dp_peer(i)).wait_recv()
        total[2] += prec[i - 1].astype(F32)
    for i in range(1, n_dp):
        px_copy(i, dp_peer(i)).wait_recv()
        for s in range(2):
            total[s] += x_term(s, i)

    for i in range(1, n_dp):
        down_copy(i, my_dp, dp_peer(i)).wait_send()
        base_copy(i, my_dp, dp_peer(i)).wait_send()
        ids_copy(i, dp_peer(i)).wait_send()
        px_copy(i, dp_peer(i)).wait_send()
        proj_copy(i, dp_peer(i)).wait_send()
        for j in range(LEVELS):
            gu_copy(i, j, dp_peer(i)).wait_send()
    for n in range(4):
        mate_copy(n).wait_send()
    for m in range(2):
        blocks(rg, half - 1, dy_s.at[m], dy_r.at[0]).wait_send()
        blocks(rx, half - 1, x_s.at[m], x_r.at[0]).wait_send()
    for i in range(n_dp):
        blocks(rr.at[i], n_ex - 1, ret_s.at[i], ret_r.at[i]).wait_send()
    for i in range(1, n_dp):
        in_copy(i, my_dp, dp_from(i)).wait_send()
        in_copy(i, dp_peer(i), dp_from(i)).wait_recv()


def finish(in_h, proj_h, in_ref, proj_ref, sems):
    n = proj_h.shape[0]
    copies = [pltpu.make_async_copy(proj_h.at[t], proj_ref.at[0, t], sems.at[t]) for t in range(n)]
    copies.append(pltpu.make_async_copy(in_h, in_ref, sems.at[n]))
    for copy in copies:
        copy.start()
    for copy in copies:
        copy.wait()


def body(
    tokens, out_grad, expert_ids, gate_probs, saved_pre, gate_weight, up_weight, down_weight, basis
):
    n_dp, n_ex = lax.axis_size("dp"), lax.axis_size("expert")
    tok_rows, width = tokens.shape
    topk = expert_ids.shape[1]
    slots, hidden2 = saved_pre.shape[2:]
    hidden = hidden2 // 2
    cap = slots // n_ex
    cp = max(16, 1 << (cap - 1).bit_length())
    rows = n_ex * cp
    nl = n_ex // LEVELS
    lrows = nl * cp
    lpad = -(-nl * cap // 16) * 16
    part = gate_weight.shape[1]
    rank = basis.shape[2]
    rk = rank // n_dp
    vmem = pl.BlockSpec(memory_space=pltpu.VMEM)
    hbm = pl.BlockSpec(memory_space=pl.ANY)
    dma = pltpu.SemaphoreType.DMA
    scratch = [
        pltpu.VMEM((topk, tok_rows), jnp.int32),
        pltpu.VMEM((topk, tok_rows), F32),
        pltpu.VMEM((tok_rows, width), BF16),
        pltpu.VMEM((tok_rows, width), BF16),
        pltpu.VMEM((tok_rows, width), BF16),
        pltpu.VMEM((tok_rows, width), BF16),
        pltpu.VMEM((topk, tok_rows), jnp.int32),
        pltpu.VMEM((topk, tok_rows), F32),
        pltpu.VMEM((n_dp - 1, topk, tok_rows), jnp.int32),
        pltpu.VMEM((n_dp, rows, tok_rows), BF16),
        pltpu.VMEM((2, rows // 2, width), BF16),
        pltpu.VMEM((2, rows // 2, width), BF16),
        pltpu.VMEM((rows, width), BF16),
        pltpu.VMEM((rows, width), BF16),
        pltpu.VMEM((LEVELS, lpad, width), BF16),
        pltpu.VMEM((lpad, lrows), BF16),
        pltpu.VMEM((width, hidden), BF16),
        pltpu.VMEM((width, rank), BF16),
        pltpu.VMEM((part, hidden), BF16),
        pltpu.VMEM((part, hidden), BF16),
        pltpu.VMEM((LEVELS, lpad, hidden2), BF16),
        pltpu.VMEM((LEVELS, lpad, hidden), F32),
        pltpu.VMEM((LEVELS, lpad, hidden), F32),
        pltpu.VMEM((LEVELS, lpad, hidden), BF16),
        pltpu.VMEM((n_dp, LEVELS, 2, lpad, hidden), BF16),
        pltpu.VMEM((2 * n_dp - 1, LEVELS, lpad, rk), BF16),
        pltpu.VMEM((LEVELS, lpad, rank), BF16),
        pltpu.VMEM((n_dp, LEVELS, lrows, part), BF16),
        pltpu.VMEM((n_dp, rows, part), BF16),
        pltpu.VMEM((n_dp - 1, tok_rows, part), BF16),
        pltpu.VMEM((n_dp - 1, rk, hidden), BF16),
        pltpu.VMEM((n_dp - 1, rk, hidden), BF16),
        pltpu.VMEM((rank, hidden), F32),
        dma((8,)), dma((LEVELS,)),
        dma((2,)), dma((LEVELS,)), dma((2,)), dma((1,)), dma((4,)), dma((4,)),
        dma((n_dp,)), dma((n_dp,)), dma((n_dp,)), dma((n_dp,)),
        dma((n_dp, LEVELS)), dma((n_dp, LEVELS)), dma((n_dp,)), dma((n_dp,)),
        dma((n_dp,)), dma((n_dp,)), dma((n_dp,)), dma((n_dp,)),
        dma((n_dp,)), dma((n_dp,)), dma((n_dp,)), dma((n_dp,)),
    ]
    outputs = tok_rows * width * 2 + 3 * rk * hidden * 4
    in_part, proj = pl.pallas_call(
        functools.partial(kernel, n_dp, n_ex, cap, cp),
        out_shape=(pltpu.VMEM((tok_rows, width), BF16), pltpu.VMEM((3, rk, hidden), F32)),
        in_specs=[hbm] * 9,
        out_specs=(vmem, vmem),
        scratch_shapes=scratch,
        compiler_params=pltpu.CompilerParams(
            collective_id=0, has_side_effects=True, vmem_limit_bytes=VMEM_BYTES - outputs
        ),
    )(
        expert_ids.T, gate_probs.T, tokens, out_grad, saved_pre,
        gate_weight, up_weight, down_weight, basis,
    )
    return pl.pallas_call(
        finish,
        out_shape=(
            jax.ShapeDtypeStruct((tok_rows, width), BF16),
            jax.ShapeDtypeStruct((1, 3, rk, hidden), F32),
        ),
        in_specs=[hbm, hbm],
        out_specs=(hbm, hbm),
        scratch_shapes=[dma((4,))],
        compiler_params=pltpu.CompilerParams(vmem_limit_bytes=1024 * 1024),
    )(in_part, proj)


def solution(mesh):
    return jax.shard_map(
        body,
        mesh=mesh,
        in_specs=(
            P(("dp", "expert"), None),
            P(("dp", "expert"), None),
            P(("dp", "expert"), None),
            P(("dp", "expert"), None),
            P("dp", "expert", None, None),
            P("expert", "dp", None),
            P("expert", "dp", None),
            P("expert", "dp", None),
            P("expert", "dp", None),
        ),
        out_specs=(P(("dp", "expert"), None), P("expert", None, "dp", None)),
        check_vma=False,
    )
```

```python
import functools
import jax
import jax.numpy as jnp
from jax import lax
from jax.experimental import pallas as pl
from jax.experimental.pallas import tpu as pltpu
from jax.sharding import PartitionSpec as P

MESH = pl.DeviceIdType.MESH
F32 = jnp.float32
BF16 = jnp.bfloat16
LEVELS = 4
VMEM_BYTES = 67043328


def dot(left, right, dims):
    return lax.dot_general(left, right, (dims, ((), ())), preferred_element_type=F32)


NN = ((1,), (0,))
TN = ((0,), (0,))
NT = ((1,), (1,))


def kernel(
    n_dp, n_ex, cap, cp,
    ids_h, probs_h, tok_h, og_h, pre_h, gw_h, uw_h, dw, bs,
    in_out, total,
    ids, probs, tok, og, tok2, og2, ids2, probs2, idsd, pick_v, sx, sg, rx, rg, dyc, spr, dfull, bfull, gw, uw, pre,
    act_a, act_b, hid, gu, px, pdy, rs, rr, in_v, psend, prec, term,
    local_sem, pre_sem, dy_s, dy_r, x_s, x_r, mate_s, mate_r, down_s, down_r, base_s, base_r,
    gu_s, gu_r, ret_s, ret_r, px_s, px_r, proj_s, proj_r, in_s, in_r, ids_s, ids_r, ready,
):
    my_dp = lax.axis_index("dp")
    me = lax.axis_index("expert")
    rows = n_ex * cp
    half = n_ex // 2
    nl = n_ex // LEVELS
    lrows = nl * cp
    lcap = nl * cap
    tokens, width = tok.shape
    topk = ids.shape[0]
    hidden = dfull.shape[1]
    part = width // n_dp
    rank = bfull.shape[1]
    rk = rank // n_dp
    shift = cp.bit_length() - 1
    fw = 256

    z = lax.div(me, nl)
    spot = lax.rem(me, nl)
    mate = lax.rem(me + half, n_ex)
    half0 = lax.div(me, half) * half
    levels = [z + 1 - 2 * lax.rem(z, 2), lax.rem(z + 2, LEVELS), LEVELS - 1 - z, z]
    own = LEVELS - 1

    def block(owner):
        return pl.ds(pl.multiple_of(owner * cp, cp), cp)

    def wpart(owner):
        return pl.ds(pl.multiple_of(owner * part, part), part)

    def rpart(owner):
        return pl.ds(pl.multiple_of(owner * rk, rk), rk)

    def rank_cols(owner):
        line = lax.broadcasted_iota(jnp.int32, (rank, rk), 0)
        lane = lax.broadcasted_iota(jnp.int32, (rank, rk), 1) + owner * rk
        return jnp.where(line == lane, one, zero).astype(BF16)

    def lpart(j):
        return pl.ds(pl.multiple_of(levels[j] * lrows, lrows), lrows)

    def ex_peer(k):
        return lax.rem(me + k, n_ex)

    def half_peer(k):
        return half0 + lax.rem(me - half0 + k, half)

    def in_level(j, t):
        return levels[j] * nl + lax.rem(spot + t, nl)

    def dp_peer(i):
        return lax.rem(my_dp + i, n_dp)

    def dp_from(i):
        return lax.rem(my_dp + n_dp - i, n_dp)

    first = [
        pltpu.make_async_copy(ids_h, ids, local_sem.at[6]),
        pltpu.make_async_copy(probs_h, probs, local_sem.at[7]),
    ]
    for copy in first:
        copy.start()

    pad = gu.shape[3] - lcap
    if pad:
        for j in range(LEVELS):
            pre[j, lcap:, :] = jnp.zeros((pad, 2 * hidden), BF16)
            for i in range(1, n_dp):
                for s in range(2):
                    gu[i, j, s, lcap:, :] = jnp.zeros((pad, hidden), BF16)

    barrier = pltpu.get_barrier_semaphore()

    for i in range(1, n_dp):
        pl.semaphore_signal(barrier, inc=1, device_id={"dp": dp_peer(i)}, device_id_type=MESH)

    odd = lax.rem(me, 2)

    @pl.loop(odd, half)
    def _(k):
        hub = lax.rem(me + 1 - odd + 2 * k, n_ex)
        pl.semaphore_signal(barrier, inc=1, device_id={"expert": hub}, device_id_type=MESH)

    @pl.when(odd == 1)
    def _():
        pl.semaphore_signal(barrier, inc=1, device_id={"expert": me - 1}, device_id_type=MESH)

    local = [
        pltpu.make_async_copy(og_h, og, local_sem.at[0]),
        pltpu.make_async_copy(tok_h, tok, local_sem.at[1]),
        pltpu.make_async_copy(dw.at[0], dfull.at[wpart(my_dp)], local_sem.at[2]),
        pltpu.make_async_copy(bs.at[0], bfull.at[wpart(my_dp)], local_sem.at[3]),
        pltpu.make_async_copy(gw_h.at[0], gw, local_sem.at[4]),
        pltpu.make_async_copy(uw_h.at[0], uw, local_sem.at[5]),
    ]
    pre_copy = []
    for j in range(LEVELS):
        src = pl.ds(pl.multiple_of(levels[j] * lcap, 8), lcap)
        pre_copy.append(
            pltpu.make_async_copy(pre_h.at[0, 0, src], pre.at[j, pl.ds(0, lcap)], pre_sem.at[j])
        )
    for copy in local[:2] + pre_copy + local[2:]:
        copy.start()

    one, zero = jnp.ones((), F32), jnp.zeros((), F32)
    earlier = lax.broadcasted_iota(jnp.int32, (tokens, tokens), 0) < lax.broadcasted_iota(
        jnp.int32, (tokens, tokens), 1
    )
    earlier = jnp.where(earlier, one, zero).astype(BF16)

    def pick_of(names_of, first, count):
        line = lax.broadcasted_iota(jnp.int32, (count, tokens), 0)
        line_expert = lax.shift_right_logical(line, shift) + first
        line_slot = lax.bitwise_and(line, cp - 1)
        names = [names_of[k : k + 1, :] == line_expert for k in range(topk)]
        any_name = functools.reduce(jnp.logical_or, names)
        named = jnp.where(any_name, one, zero).astype(BF16)
        before = dot(named, earlier, NN)
        at_slot = before == line_slot.astype(F32)
        pick = jnp.where(jnp.logical_and(any_name, at_slot), one, zero).astype(BF16)
        return pick, names, at_slot

    def half_pick(names_of, weights_of):
        pick, names, at_slot = pick_of(names_of, half0, half * cp)
        weights = functools.reduce(
            jnp.add, [jnp.where(name, weights_of[k : k + 1, :], zero) for k, name in enumerate(names)]
        )
        return pick, jnp.sum(jnp.where(at_slot, weights, zero), axis=1, keepdims=True)

    for copy in first:
        copy.wait()
    pick, weight = half_pick(ids, probs)

    pl.semaphore_wait(barrier, n_dp + odd * (n_ex - 2))

    def down_copy(i, owner, peer):
        return pltpu.make_async_remote_copy(
            dw.at[0], dfull.at[wpart(owner)], down_s.at[i], down_r.at[i],
            device_id={"dp": peer}, device_id_type=MESH,
        )

    def base_copy(i, owner, peer):
        return pltpu.make_async_remote_copy(
            bs.at[0], bfull.at[wpart(owner)], base_s.at[i], base_r.at[i],
            device_id={"dp": peer}, device_id_type=MESH,
        )

    def ids_copy(i, peer):
        return pltpu.make_async_remote_copy(
            ids, idsd.at[i - 1], ids_s.at[i], ids_r.at[i],
            device_id={"dp": peer}, device_id_type=MESH,
        )

    def mate_copy(n):
        src, dst = ((og, og2), (tok, tok2), (ids, ids2), (probs, probs2))[n]
        return pltpu.make_async_remote_copy(
            src, dst, mate_s.at[n], mate_r.at[n], device_id={"expert": mate}, device_id_type=MESH
        )

    def dy_copy(m, peer, owner, j):
        return pltpu.make_async_remote_copy(
            sg.at[m, block(peer - half0)], rg.at[block(owner)], dy_s.at[m], dy_r.at[j],
            device_id={"expert": peer}, device_id_type=MESH,
        )

    def x_copy(m, peer, owner):
        return pltpu.make_async_remote_copy(
            sx.at[m, block(peer - half0)], rx.at[block(owner)], x_s.at[m], x_r.at[0],
            device_id={"expert": peer}, device_id_type=MESH,
        )

    def blocks(buffer, count, send, recv):
        span = buffer.at[pl.ds(0, count * cp)]
        return pltpu.make_async_remote_copy(
            span, span, send, recv, device_id={"expert": mate}, device_id_type=MESH
        )

    def gu_copy(i, j, peer):
        used = pl.ds(0, lcap)
        return pltpu.make_async_remote_copy(
            gu.at[0, j, :, used], gu.at[i, j, :, used], gu_s.at[i, j], gu_r.at[i, j],
            device_id={"dp": peer}, device_id_type=MESH,
        )

    def px_copy(i, peer):
        return pltpu.make_async_remote_copy(
            px.at[i - 1], px.at[n_dp - 1 + i], px_s.at[i], px_r.at[i],
            device_id={"dp": peer}, device_id_type=MESH,
        )

    def ret_copy(i, j, peer, owner):
        return pltpu.make_async_remote_copy(
            rs.at[i, j, block(lax.rem(peer, nl))], rr.at[i, block(owner)],
            ret_s.at[i], ret_r.at[i],
            device_id={"expert": peer}, device_id_type=MESH,
        )

    def proj_copy(i, peer):
        return pltpu.make_async_remote_copy(
            psend.at[i - 1], prec.at[i - 1], proj_s.at[i], proj_r.at[i],
            device_id={"dp": peer}, device_id_type=MESH,
        )

    def in_copy(i, owner, peer):
        return pltpu.make_async_remote_copy(
            in_v.at[i - 1], in_out.at[:, wpart(owner)], in_s.at[i], in_r.at[i],
            device_id={"dp": peer}, device_id_type=MESH,
        )

    for i in range(1, n_dp):
        ids_copy(i, dp_peer(i)).start()
    for i in range(1, n_dp):
        down_copy(i, my_dp, dp_peer(i)).start()
    for i in range(1, n_dp):
        base_copy(i, my_dp, dp_peer(i)).start()

    @pl.when(odd == 1)
    def _():
        pl.semaphore_signal(ready, inc=1, device_id={"expert": me - 1}, device_id_type=MESH)

    local[0].wait()
    sg[0] = (dot(pick, og[...], NN) * weight).astype(BF16)

    @pl.when(odd == 0)
    def _():
        pl.semaphore_wait(ready, 1)

    mate_copy(2).start()
    mate_copy(3).start()
    mate_copy(0).start()

    def dispatch_dy(m, owner):
        for near, tag in ((0, 0 if m == 0 else 2), (own, own if m == 0 else 1)):

            @pl.loop(int(near == own), nl)
            def _(t):
                dy_copy(m, in_level(near, t), owner, tag).start()

        rg[block(owner), :] = sg[m, block(me - half0), :]

    def dispatch_x(m, owner):
        @pl.loop(1, half)
        def _(k):
            x_copy(m, half_peer(k), owner).start()

        rx[block(owner), :] = sx[m, block(me - half0), :]

    dispatch_dy(0, me)
    local[1].wait()
    mate_copy(1).start()
    sx[0] = dot(pick, tok[...], NN).astype(BF16)
    dispatch_x(0, me)

    grid = (gu.shape[3], lrows)
    line = lax.broadcasted_iota(jnp.int32, grid, 1)
    inner = lax.bitwise_and(line, cp - 1)
    target = lax.shift_right_logical(line, shift) * cap + inner
    spread = jnp.logical_and(target == lax.broadcasted_iota(jnp.int32, grid, 0), inner < cap)
    spr[...] = jnp.where(spread, one, zero).astype(BF16)

    for j in range(LEVELS):
        pre_copy[j].wait()
        for f in range(0, hidden, fw):
            cols = slice(f, f + fw)
            g = pre[j, :, f : f + fw].astype(F32)
            u = pre[j, :, hidden + f : hidden + f + fw].astype(F32)
            sig = jax.nn.sigmoid(g)
            gs = g * sig
            act_a[j, :, cols] = gs
            hid[j, :, cols] = (gs * u).astype(BF16)
            act_b[j, :, cols] = u * sig * (1.0 + g * (1.0 - sig))

    def row_grad(i, j):
        out = dot(gu[i, j, 0], gw[...], NT) + dot(gu[i, j, 1], uw[...], NT)
        rs[i, j] = dot(spr[...], out.astype(BF16), TN).astype(BF16)

        @pl.loop(int(j == own), nl)
        def _(t):
            ret_copy(i, j, in_level(j, t), me).start()

        if j == own:
            rr[i, block(me), :] = rs[i, j, block(spot), :]

    pick_v[0] = pick_of(ids, 0, rows)[0]
    for i in range(1, n_dp):
        ids_copy(i, dp_peer(i)).wait_recv()
        pick_v[i] = pick_of(idsd.at[i - 1], 0, rows)[0]

    mate_copy(2).wait_recv()
    mate_copy(3).wait_recv()
    pick2, weight2 = half_pick(ids2, probs2)
    mate_copy(0).wait_recv()
    sg[1] = (dot(pick2, og2[...], NN) * weight2).astype(BF16)
    dispatch_dy(1, mate)

    local[2].wait()
    for i in range(1, n_dp):
        down_copy(i, dp_from(i), dp_peer(i)).wait_recv()

    for j in range(LEVELS):

        blocks(rg, nl - j % 2, dy_s.at[0], dy_r.at[j]).wait_recv()
        dyc[j] = dot(spr[...], rg[lpart(j), :], NN).astype(BF16)
        for f in range(0, hidden, fw):
            cols = slice(f, f + fw)
            hg = dot(dyc[j], dfull[:, cols], NN)
            gu[0, j, 1, :, cols] = (hg * act_a[j, :, cols]).astype(BF16)
            gu[0, j, 0, :, cols] = (hg * act_b[j, :, cols]).astype(BF16)
        for i in range(1, n_dp):
            gu_copy(i, j, dp_peer(i)).start()
        if j == 0:
            local[4].wait()
            local[5].wait()
        row_grad(0, j)

    local[3].wait()
    for i in range(1, n_dp):
        base_copy(i, dp_from(i), dp_peer(i)).wait_recv()
    for j in range(LEVELS):
        pdy[j] = dot(dyc[j], bfull[...], NN).astype(BF16)

    def project(left, right):
        return functools.reduce(jnp.add, [dot(left(j), right(j), TN) for j in range(LEVELS)])

    term[...] = project(lambda j: pdy[j], lambda j: hid[j])
    for i in range(1, n_dp):
        psend[i - 1] = term[rpart(dp_peer(i)), :].astype(BF16)
        proj_copy(i, dp_peer(i)).start()
    total[2] = term[rpart(my_dp), :]

    mate_copy(1).wait_recv()
    sx[1] = dot(pick2, tok2[...], NN).astype(BF16)
    dispatch_x(1, mate)

    def theirs(j):
        for i in range(1, n_dp):
            gu_copy(i, j, dp_peer(i)).wait_recv()
            row_grad(i, j)

    theirs(0)

    theirs(1)

    blocks(rx, n_ex - 2, x_s.at[0], x_r.at[0]).wait_recv()
    for j in range(LEVELS):
        xj = dot(spr[...], rx[lpart(j), :], NN).astype(BF16)
        if rk % 128:
            xp = dot(xj, bfull[...], NN).astype(BF16)
        for i in range(n_dp):
            if rk % 128:
                pj = dot(xp, rank_cols(dp_peer(i)), NN)
            else:
                pj = dot(xj, bfull[:, rpart(dp_peer(i))], NN)
            px[(i + n_dp - 1) % n_dp, j] = pj.astype(BF16)
    for i in range(1, n_dp):
        px_copy(i, dp_peer(i)).start()

    theirs(2)

    def x_term(s, i):
        left = px.at[n_dp - 1 + i]
        return project(lambda j: left[j], lambda j: gu[i, j, s])

    for s in range(2):
        total[s] = x_term(s, 0)

    def combine(i):
        blocks(rr.at[i], n_ex - 1, ret_s.at[i], ret_r.at[i]).wait_recv()
        return dot(pick_v[i], rr[i], TN).astype(BF16)

    in_out[:, wpart(my_dp)] = combine(0)

    theirs(3)
    for i in range(1, n_dp):
        in_v[i - 1] = combine(i)
        in_copy(i, my_dp, dp_from(i)).start()

    for i in range(1, n_dp):
        proj_copy(i, dp_peer(i)).wait_recv()
        total[2] += prec[i - 1].astype(F32)
    for i in range(1, n_dp):
        px_copy(i, dp_peer(i)).wait_recv()
        for s in range(2):
            total[s] += x_term(s, i)

    for i in range(1, n_dp):
        down_copy(i, my_dp, dp_peer(i)).wait_send()
        base_copy(i, my_dp, dp_peer(i)).wait_send()
        ids_copy(i, dp_peer(i)).wait_send()
        px_copy(i, dp_peer(i)).wait_send()
        proj_copy(i, dp_peer(i)).wait_send()
        for j in range(LEVELS):
            gu_copy(i, j, dp_peer(i)).wait_send()
    for n in range(4):
        mate_copy(n).wait_send()
    for m in range(2):
        blocks(rg, half - 1, dy_s.at[m], dy_r.at[0]).wait_send()
        blocks(rx, half - 1, x_s.at[m], x_r.at[0]).wait_send()
    for i in range(n_dp):
        blocks(rr.at[i], n_ex - 1, ret_s.at[i], ret_r.at[i]).wait_send()
    for i in range(1, n_dp):
        in_copy(i, my_dp, dp_from(i)).wait_send()
        in_copy(i, dp_peer(i), dp_from(i)).wait_recv()


def finish(in_h, proj_h, in_ref, proj_ref, sems):
    n = proj_h.shape[0]
    copies = [pltpu.make_async_copy(proj_h.at[t], proj_ref.at[0, t], sems.at[t]) for t in range(n)]
    copies.append(pltpu.make_async_copy(in_h, in_ref, sems.at[n]))
    for copy in copies:
        copy.start()
    for copy in copies:
        copy.wait()


def body(
    tokens, out_grad, expert_ids, gate_probs, saved_pre, gate_weight, up_weight, down_weight, basis
):
    n_dp, n_ex = lax.axis_size("dp"), lax.axis_size("expert")
    tok_rows, width = tokens.shape
    topk = expert_ids.shape[1]
    slots, hidden2 = saved_pre.shape[2:]
    hidden = hidden2 // 2
    cap = slots // n_ex
    cp = max(16, 1 << (cap - 1).bit_length())
    rows = n_ex * cp
    nl = n_ex // LEVELS
    lrows = nl * cp
    lpad = -(-nl * cap // 16) * 16
    part = gate_weight.shape[1]
    rank = basis.shape[2]
    rk = rank // n_dp
    vmem = pl.BlockSpec(memory_space=pltpu.VMEM)
    hbm = pl.BlockSpec(memory_space=pl.ANY)
    dma = pltpu.SemaphoreType.DMA
    scratch = [
        pltpu.VMEM((topk, tok_rows), jnp.int32),
        pltpu.VMEM((topk, tok_rows), F32),
        pltpu.VMEM((tok_rows, width), BF16),
        pltpu.VMEM((tok_rows, width), BF16),
        pltpu.VMEM((tok_rows, width), BF16),
        pltpu.VMEM((tok_rows, width), BF16),
        pltpu.VMEM((topk, tok_rows), jnp.int32),
        pltpu.VMEM((topk, tok_rows), F32),
        pltpu.VMEM((n_dp - 1, topk, tok_rows), jnp.int32),
        pltpu.VMEM((n_dp, rows, tok_rows), BF16),
        pltpu.VMEM((2, rows // 2, width), BF16),
        pltpu.VMEM((2, rows // 2, width), BF16),
        pltpu.VMEM((rows, width), BF16),
        pltpu.VMEM((rows, width), BF16),
        pltpu.VMEM((LEVELS, lpad, width), BF16),
        pltpu.VMEM((lpad, lrows), BF16),
        pltpu.VMEM((width, hidden), BF16),
        pltpu.VMEM((width, rank), BF16),
        pltpu.VMEM((part, hidden), BF16),
        pltpu.VMEM((part, hidden), BF16),
        pltpu.VMEM((LEVELS, lpad, hidden2), BF16),
        pltpu.VMEM((LEVELS, lpad, hidden), F32),
        pltpu.VMEM((LEVELS, lpad, hidden), F32),
        pltpu.VMEM((LEVELS, lpad, hidden), BF16),
        pltpu.VMEM((n_dp, LEVELS, 2, lpad, hidden), BF16),
        pltpu.VMEM((2 * n_dp - 1, LEVELS, lpad, rk), BF16),
        pltpu.VMEM((LEVELS, lpad, rank), BF16),
        pltpu.VMEM((n_dp, LEVELS, lrows, part), BF16),
        pltpu.VMEM((n_dp, rows, part), BF16),
        pltpu.VMEM((n_dp - 1, tok_rows, part), BF16),
        pltpu.VMEM((n_dp - 1, rk, hidden), BF16),
        pltpu.VMEM((n_dp - 1, rk, hidden), BF16),
        pltpu.VMEM((rank, hidden), F32),
        dma((8,)), dma((LEVELS,)),
        dma((2,)), dma((LEVELS,)), dma((2,)), dma((1,)), dma((4,)), dma((4,)),
        dma((n_dp,)), dma((n_dp,)), dma((n_dp,)), dma((n_dp,)),
        dma((n_dp, LEVELS)), dma((n_dp, LEVELS)), dma((n_dp,)), dma((n_dp,)),
        dma((n_dp,)), dma((n_dp,)), dma((n_dp,)), dma((n_dp,)),
        dma((n_dp,)), dma((n_dp,)), dma((n_dp,)), dma((n_dp,)),
        pltpu.SemaphoreType.REGULAR,
    ]
    outputs = tok_rows * width * 2 + 3 * rk * hidden * 4
    in_part, proj = pl.pallas_call(
        functools.partial(kernel, n_dp, n_ex, cap, cp),
        out_shape=(pltpu.VMEM((tok_rows, width), BF16), pltpu.VMEM((3, rk, hidden), F32)),
        in_specs=[hbm] * 9,
        out_specs=(vmem, vmem),
        scratch_shapes=scratch,
        compiler_params=pltpu.CompilerParams(
            collective_id=0, has_side_effects=True, vmem_limit_bytes=VMEM_BYTES - outputs
        ),
    )(
        expert_ids.T, gate_probs.T, tokens, out_grad, saved_pre,
        gate_weight, up_weight, down_weight, basis,
    )
    return pl.pallas_call(
        finish,
        out_shape=(
            jax.ShapeDtypeStruct((tok_rows, width), BF16),
            jax.ShapeDtypeStruct((1, 3, rk, hidden), F32),
        ),
        in_specs=[hbm, hbm],
        out_specs=(hbm, hbm),
        scratch_shapes=[dma((4,))],
        compiler_params=pltpu.CompilerParams(vmem_limit_bytes=1024 * 1024),
    )(in_part, proj)


def solution(mesh):
    return jax.shard_map(
        body,
        mesh=mesh,
        in_specs=(
            P(("dp", "expert"), None),
            P(("dp", "expert"), None),
            P(("dp", "expert"), None),
            P(("dp", "expert"), None),
            P("dp", "expert", None, None),
            P("expert", "dp", None),
            P("expert", "dp", None),
            P("expert", "dp", None),
            P("expert", "dp", None),
        ),
        out_specs=(P(("dp", "expert"), None), P("expert", None, "dp", None)),
        check_vma=False,
    )
```

```python
import functools
import jax
import jax.numpy as jnp
from jax import lax
from jax.experimental import pallas as pl
from jax.experimental.pallas import tpu as pltpu
from jax.sharding import PartitionSpec as P

MESH = pl.DeviceIdType.MESH
F32 = jnp.float32
BF16 = jnp.bfloat16
LEVELS = 4
VMEM_BYTES = 67043328


def dot(left, right, dims):
    return lax.dot_general(left, right, (dims, ((), ())), preferred_element_type=F32)


NN = ((1,), (0,))
TN = ((0,), (0,))
NT = ((1,), (1,))


def kernel(
    n_dp, n_ex, cap, cp,
    ids_h, probs_h, tok_h, og_h, pre_h, gw_h, uw_h, dw, bs,
    in_out, total,
    ids, probs, tok, og, tok2, og2, ids2, probs2, idsd, pick_v, sx, sg, rx, rg, dyc, spr, dfull, bfull, gw, uw, pre,
    act_a, act_b, hid, gu, px, pdy, rs, rr, in_v, psend, prec, term,
    local_sem, pre_sem, dy_s, dy_r, x_s, x_r, mate_s, mate_r, down_s, down_r, base_s, base_r,
    gu_s, gu_r, ret_s, ret_r, px_s, px_r, proj_s, proj_r, in_s, in_r, ids_s, ids_r, ready,
):
    my_dp = lax.axis_index("dp")
    me = lax.axis_index("expert")
    rows = n_ex * cp
    half = n_ex // 2
    nl = n_ex // LEVELS
    lrows = nl * cp
    lcap = nl * cap
    tokens, width = tok.shape
    topk = ids.shape[0]
    hidden = dfull.shape[1]
    part = width // n_dp
    rank = bfull.shape[1]
    rk = rank // n_dp
    shift = cp.bit_length() - 1
    fw = 256

    z = lax.div(me, nl)
    spot = lax.rem(me, nl)
    mate = lax.rem(me + half, n_ex)
    half0 = lax.div(me, half) * half
    levels = [z + 1 - 2 * lax.rem(z, 2), lax.rem(z + 2, LEVELS), LEVELS - 1 - z, z]
    own = LEVELS - 1

    def block(owner):
        return pl.ds(pl.multiple_of(owner * cp, cp), cp)

    def wpart(owner):
        return pl.ds(pl.multiple_of(owner * part, part), part)

    def rpart(owner):
        return pl.ds(pl.multiple_of(owner * rk, rk), rk)

    def rank_cols(owner):
        line = lax.broadcasted_iota(jnp.int32, (rank, rk), 0)
        lane = lax.broadcasted_iota(jnp.int32, (rank, rk), 1) + owner * rk
        return jnp.where(line == lane, one, zero).astype(BF16)

    def lpart(j):
        return pl.ds(pl.multiple_of(levels[j] * lrows, lrows), lrows)

    def ex_peer(k):
        return lax.rem(me + k, n_ex)

    def half_peer(k):
        return half0 + lax.rem(me - half0 + k, half)

    def in_level(j, t):
        return levels[j] * nl + lax.rem(spot + t, nl)

    def dp_peer(i):
        return lax.rem(my_dp + i, n_dp)

    def dp_from(i):
        return lax.rem(my_dp + n_dp - i, n_dp)

    first = [
        pltpu.make_async_copy(ids_h, ids, local_sem.at[6]),
        pltpu.make_async_copy(probs_h, probs, local_sem.at[7]),
    ]
    for copy in first:
        copy.start()

    pad = gu.shape[3] - lcap
    if pad:
        for j in range(LEVELS):
            pre[j, lcap:, :] = jnp.zeros((pad, 2 * hidden), BF16)
            for i in range(1, n_dp):
                px[n_dp - 1 + i, j, lcap:, :] = jnp.zeros((pad, rk), BF16)
                for s in range(2):
                    gu[i, j, s, lcap:, :] = jnp.zeros((pad, hidden), BF16)

    barrier = pltpu.get_barrier_semaphore()

    for i in range(1, n_dp):
        pl.semaphore_signal(barrier, inc=1, device_id={"dp": dp_peer(i)}, device_id_type=MESH)

    odd = lax.rem(me, 2)

    @pl.loop(odd, half)
    def _(k):
        hub = lax.rem(me + 1 - odd + 2 * k, n_ex)
        pl.semaphore_signal(barrier, inc=1, device_id={"expert": hub}, device_id_type=MESH)

    @pl.when(odd == 1)
    def _():
        pl.semaphore_signal(barrier, inc=1, device_id={"expert": me - 1}, device_id_type=MESH)

    local = [
        pltpu.make_async_copy(og_h, og, local_sem.at[0]),
        pltpu.make_async_copy(tok_h, tok, local_sem.at[1]),
        pltpu.make_async_copy(dw.at[0], dfull.at[wpart(my_dp)], local_sem.at[2]),
        pltpu.make_async_copy(bs.at[0], bfull.at[wpart(my_dp)], local_sem.at[3]),
        pltpu.make_async_copy(gw_h.at[0], gw, local_sem.at[4]),
        pltpu.make_async_copy(uw_h.at[0], uw, local_sem.at[5]),
    ]
    pre_copy = []
    for j in range(LEVELS):
        src = pl.ds(pl.multiple_of(levels[j] * lcap, 8), lcap)
        pre_copy.append(
            pltpu.make_async_copy(pre_h.at[0, 0, src], pre.at[j, pl.ds(0, lcap)], pre_sem.at[j])
        )
    for copy in local[:2] + pre_copy + local[2:]:
        copy.start()

    def down_copy(i, owner, peer):
        return pltpu.make_async_remote_copy(
            dw.at[0], dfull.at[wpart(owner)], down_s.at[i], down_r.at[i],
            device_id={"dp": peer}, device_id_type=MESH,
        )

    def base_copy(i, owner, peer):
        return pltpu.make_async_remote_copy(
            bs.at[0], bfull.at[wpart(owner)], base_s.at[i], base_r.at[i],
            device_id={"dp": peer}, device_id_type=MESH,
        )

    def ids_copy(i, peer):
        return pltpu.make_async_remote_copy(
            ids_h, idsd.at[i - 1], ids_s.at[i], ids_r.at[i],
            device_id={"dp": peer}, device_id_type=MESH,
        )

    def mate_copy(n):
        src, dst = ((og, og2), (tok, tok2), (ids, ids2), (probs, probs2))[n]
        return pltpu.make_async_remote_copy(
            src, dst, mate_s.at[n], mate_r.at[n], device_id={"expert": mate}, device_id_type=MESH
        )

    def dy_copy(m, peer, owner, j):
        return pltpu.make_async_remote_copy(
            sg.at[m, block(peer - half0)], rg.at[block(owner)], dy_s.at[m], dy_r.at[j],
            device_id={"expert": peer}, device_id_type=MESH,
        )

    def x_copy(m, peer, owner):
        return pltpu.make_async_remote_copy(
            sx.at[m, block(peer - half0)], rx.at[block(owner)], x_s.at[m], x_r.at[0],
            device_id={"expert": peer}, device_id_type=MESH,
        )

    def blocks(buffer, count, send, recv):
        span = buffer.at[pl.ds(0, count * cp)]
        return pltpu.make_async_remote_copy(
            span, span, send, recv, device_id={"expert": mate}, device_id_type=MESH
        )

    used = pl.ds(0, lcap)

    def gu_copy(i, j, peer):
        return pltpu.make_async_remote_copy(
            gu.at[0, j, :, used], gu.at[i, j, :, used], gu_s.at[i, j], gu_r.at[i, j],
            device_id={"dp": peer}, device_id_type=MESH,
        )

    def px_copy(i, peer):
        return pltpu.make_async_remote_copy(
            px.at[i - 1, :, used], px.at[n_dp - 1 + i, :, used], px_s.at[i], px_r.at[i],
            device_id={"dp": peer}, device_id_type=MESH,
        )

    def ret_copy(i, j, peer, owner):
        return pltpu.make_async_remote_copy(
            rs.at[i, j, block(lax.rem(peer, nl))], rr.at[i, block(owner)],
            ret_s.at[i], ret_r.at[i],
            device_id={"expert": peer}, device_id_type=MESH,
        )

    def proj_copy(i, peer):
        return pltpu.make_async_remote_copy(
            psend.at[i - 1], prec.at[i - 1], proj_s.at[i], proj_r.at[i],
            device_id={"dp": peer}, device_id_type=MESH,
        )

    def in_copy(i, owner, peer):
        return pltpu.make_async_remote_copy(
            in_v.at[i - 1], in_out.at[owner], in_s.at[i], in_r.at[i],
            device_id={"dp": peer}, device_id_type=MESH,
        )

    def start_dp():
        for i in range(1, n_dp):
            ids_copy(i, dp_peer(i)).start()
        for i in range(1, n_dp):
            down_copy(i, my_dp, dp_peer(i)).start()
        for i in range(1, n_dp):
            base_copy(i, my_dp, dp_peer(i)).start()

    @pl.when(odd == 0)
    def _():
        pl.semaphore_wait(barrier, n_dp)
        start_dp()

    one, zero = jnp.ones((), F32), jnp.zeros((), F32)
    earlier = lax.broadcasted_iota(jnp.int32, (tokens, tokens), 0) < lax.broadcasted_iota(
        jnp.int32, (tokens, tokens), 1
    )
    earlier = jnp.where(earlier, one, zero).astype(BF16)

    def pick_of(names_of, first, count):
        line = lax.broadcasted_iota(jnp.int32, (count, tokens), 0)
        line_expert = lax.shift_right_logical(line, shift) + first
        line_slot = lax.bitwise_and(line, cp - 1)
        names = [names_of[k : k + 1, :] == line_expert for k in range(topk)]
        any_name = functools.reduce(jnp.logical_or, names)
        named = jnp.where(any_name, one, zero).astype(BF16)
        before = dot(named, earlier, NN)
        at_slot = before == line_slot.astype(F32)
        pick = jnp.where(jnp.logical_and(any_name, at_slot), one, zero).astype(BF16)
        return pick, names, at_slot

    def half_pick(names_of, weights_of):
        pick, names, at_slot = pick_of(names_of, half0, half * cp)
        weights = functools.reduce(
            jnp.add, [jnp.where(name, weights_of[k : k + 1, :], zero) for k, name in enumerate(names)]
        )
        return pick, jnp.sum(jnp.where(at_slot, weights, zero), axis=1, keepdims=True)

    for copy in first:
        copy.wait()
    pick, weight = half_pick(ids, probs)

    local[0].wait()
    sg[0] = (dot(pick, og[...], NN) * weight).astype(BF16)

    @pl.when(odd == 1)
    def _():
        pl.semaphore_wait(barrier, n_dp + n_ex - 2)
        start_dp()
        pl.semaphore_signal(ready, inc=1, device_id={"expert": me - 1}, device_id_type=MESH)

    @pl.when(odd == 0)
    def _():
        pl.semaphore_wait(ready, 1)

    mate_copy(2).start()
    mate_copy(3).start()
    mate_copy(0).start()

    def dispatch_dy(m, owner):
        for near, tag in ((0, 0 if m == 0 else 2), (own, own if m == 0 else 1)):

            @pl.loop(int(near == own), nl)
            def _(t):
                dy_copy(m, in_level(near, t), owner, tag).start()

        rg[block(owner), :] = sg[m, block(me - half0), :]

    def dispatch_x(m, owner):
        @pl.loop(1, half)
        def _(k):
            x_copy(m, half_peer(k), owner).start()

        rx[block(owner), :] = sx[m, block(me - half0), :]

    dispatch_dy(0, me)
    grid = (gu.shape[3], lrows)
    line = lax.broadcasted_iota(jnp.int32, grid, 1)
    inner = lax.bitwise_and(line, cp - 1)
    target = lax.shift_right_logical(line, shift) * cap + inner
    spread = jnp.logical_and(target == lax.broadcasted_iota(jnp.int32, grid, 0), inner < cap)
    spr[...] = jnp.where(spread, one, zero).astype(BF16)

    for j in range(LEVELS):
        pre_copy[j].wait()
        for f in range(0, hidden, fw):
            cols = slice(f, f + fw)
            g = pre[j, :, f : f + fw].astype(F32)
            u = pre[j, :, hidden + f : hidden + f + fw].astype(F32)
            sig = jax.nn.sigmoid(g)
            gs = g * sig
            act_a[j, :, cols] = gs
            hid[j, :, cols] = (gs * u).astype(BF16)
            act_b[j, :, cols] = u * sig * (1.0 + g * (1.0 - sig))

    def row_grad(i, j):
        out = dot(gu[i, j, 0], gw[...], NT) + dot(gu[i, j, 1], uw[...], NT)
        rs[i, j] = dot(spr[...], out.astype(BF16), TN).astype(BF16)

        @pl.loop(int(j == own), nl)
        def _(t):
            ret_copy(i, j, in_level(j, t), me).start()

        if j == own:
            rr[i, block(me), :] = rs[i, j, block(spot), :]

    pick_v[0] = pick_of(ids, 0, rows)[0]
    for i in range(1, n_dp):
        ids_copy(i, dp_peer(i)).wait_recv()
        pick_v[i] = pick_of(idsd.at[i - 1], 0, rows)[0]

    mate_copy(2).wait_recv()
    mate_copy(3).wait_recv()
    pick2, weight2 = half_pick(ids2, probs2)
    mate_copy(0).wait_recv()
    sg[1] = (dot(pick2, og2[...], NN) * weight2).astype(BF16)
    dispatch_dy(1, mate)

    local[1].wait()
    mate_copy(1).start()
    sx[0] = dot(pick, tok[...], NN).astype(BF16)
    dispatch_x(0, me)

    local[2].wait()
    for i in range(1, n_dp):
        down_copy(i, dp_from(i), dp_peer(i)).wait_recv()

    for j in range(LEVELS):

        blocks(rg, nl - j % 2, dy_s.at[0], dy_r.at[j]).wait_recv()
        dyc[j] = dot(spr[...], rg[lpart(j), :], NN).astype(BF16)
        for f in range(0, hidden, fw):
            cols = slice(f, f + fw)
            hg = dot(dyc[j], dfull[:, cols], NN)
            gu[0, j, 1, :, cols] = (hg * act_a[j, :, cols]).astype(BF16)
            gu[0, j, 0, :, cols] = (hg * act_b[j, :, cols]).astype(BF16)
        for i in range(1, n_dp):
            gu_copy(i, j, dp_peer(i)).start()
        if j == 0:
            local[4].wait()
            local[5].wait()
        row_grad(0, j)

    local[3].wait()
    for i in range(1, n_dp):
        base_copy(i, dp_from(i), dp_peer(i)).wait_recv()
    for j in range(LEVELS):
        pdy[j] = dot(dyc[j], bfull[...], NN).astype(BF16)

    def project(left, right):
        return functools.reduce(jnp.add, [dot(left(j), right(j), TN) for j in range(LEVELS)])

    term[...] = project(lambda j: pdy[j], lambda j: hid[j])
    for i in range(1, n_dp):
        psend[i - 1] = term[rpart(dp_peer(i)), :].astype(BF16)
    total[2] = term[rpart(my_dp), :]

    mate_copy(1).wait_recv()
    sx[1] = dot(pick2, tok2[...], NN).astype(BF16)
    dispatch_x(1, mate)

    def theirs(j):
        for i in range(1, n_dp):
            gu_copy(i, j, dp_peer(i)).wait_recv()
            if j == own and i == n_dp - 1:
                pl.when(odd == 0)(start_projections)
            row_grad(i, j)

    theirs(0)

    theirs(1)

    blocks(rx, n_ex - 2, x_s.at[0], x_r.at[0]).wait_recv()
    for j in range(LEVELS):
        xj = dot(spr[...], rx[lpart(j), :], NN).astype(BF16)
        if rk % 128:
            xp = dot(xj, bfull[...], NN).astype(BF16)
        for i in range(n_dp):
            if rk % 128:
                pj = dot(xp, rank_cols(dp_peer(i)), NN)
            else:
                pj = dot(xj, bfull[:, rpart(dp_peer(i))], NN)
            px[(i + n_dp - 1) % n_dp, j] = pj.astype(BF16)

    def start_projections():
        for i in range(1, n_dp):
            proj_copy(i, dp_peer(i)).start()
            px_copy(i, dp_peer(i)).start()

    pl.when(odd == 1)(start_projections)

    theirs(2)

    def x_term(s, i):
        left = px.at[n_dp - 1 + i]
        return project(lambda j: left[j], lambda j: gu[i, j, s])

    for s in range(2):
        total[s] = x_term(s, 0)

    def combine(i):
        blocks(rr.at[i], n_ex - 1, ret_s.at[i], ret_r.at[i]).wait_recv()
        return dot(pick_v[i], rr[i], TN).astype(BF16)

    in_out[my_dp] = combine(0)

    theirs(3)
    for i in range(1, n_dp):
        in_v[i - 1] = combine(i)
        in_copy(i, my_dp, dp_from(i)).start()

    for i in range(1, n_dp):
        proj_copy(i, dp_peer(i)).wait_recv()
        total[2] += prec[i - 1].astype(F32)
    for i in range(1, n_dp):
        px_copy(i, dp_peer(i)).wait_recv()
        for s in range(2):
            total[s] += x_term(s, i)

    for i in range(1, n_dp):
        down_copy(i, my_dp, dp_peer(i)).wait_send()
        base_copy(i, my_dp, dp_peer(i)).wait_send()
        ids_copy(i, dp_peer(i)).wait_send()
        px_copy(i, dp_peer(i)).wait_send()
        proj_copy(i, dp_peer(i)).wait_send()
        for j in range(LEVELS):
            gu_copy(i, j, dp_peer(i)).wait_send()
    for n in range(4):
        mate_copy(n).wait_send()
    for m in range(2):
        blocks(rg, half - 1, dy_s.at[m], dy_r.at[0]).wait_send()
        blocks(rx, half - 1, x_s.at[m], x_r.at[0]).wait_send()
    for i in range(n_dp):
        blocks(rr.at[i], n_ex - 1, ret_s.at[i], ret_r.at[i]).wait_send()
    for i in range(1, n_dp):
        in_copy(i, my_dp, dp_from(i)).wait_send()
        in_copy(i, dp_peer(i), dp_from(i)).wait_recv()


def finish(in_h, proj_h, in_ref, proj_ref, proj_s, in_s):
    parts, _, part = in_h.shape
    n = proj_h.shape[0]
    copies = [pltpu.make_async_copy(proj_h.at[t], proj_ref.at[0, t], proj_s.at[t]) for t in range(n)]
    for d in range(parts):
        cols = pl.ds(d * part, part)
        copies.append(pltpu.make_async_copy(in_h.at[d], in_ref.at[:, cols], in_s.at[d]))
    for copy in copies:
        copy.start()
    for copy in copies:
        copy.wait()


def body(
    tokens, out_grad, expert_ids, gate_probs, saved_pre, gate_weight, up_weight, down_weight, basis
):
    n_dp, n_ex = lax.axis_size("dp"), lax.axis_size("expert")
    tok_rows, width = tokens.shape
    topk = expert_ids.shape[1]
    slots, hidden2 = saved_pre.shape[2:]
    hidden = hidden2 // 2
    cap = slots // n_ex
    cp = max(16, 1 << (cap - 1).bit_length())
    rows = n_ex * cp
    nl = n_ex // LEVELS
    lrows = nl * cp
    lpad = -(-nl * cap // 16) * 16
    part = gate_weight.shape[1]
    rank = basis.shape[2]
    rk = rank // n_dp
    vmem = pl.BlockSpec(memory_space=pltpu.VMEM)
    hbm = pl.BlockSpec(memory_space=pl.ANY)
    dma = pltpu.SemaphoreType.DMA
    scratch = [
        pltpu.VMEM((topk, tok_rows), jnp.int32),
        pltpu.VMEM((topk, tok_rows), F32),
        pltpu.VMEM((tok_rows, width), BF16),
        pltpu.VMEM((tok_rows, width), BF16),
        pltpu.VMEM((tok_rows, width), BF16),
        pltpu.VMEM((tok_rows, width), BF16),
        pltpu.VMEM((topk, tok_rows), jnp.int32),
        pltpu.VMEM((topk, tok_rows), F32),
        pltpu.VMEM((n_dp - 1, topk, tok_rows), jnp.int32),
        pltpu.VMEM((n_dp, rows, tok_rows), BF16),
        pltpu.VMEM((2, rows // 2, width), BF16),
        pltpu.VMEM((2, rows // 2, width), BF16),
        pltpu.VMEM((rows, width), BF16),
        pltpu.VMEM((rows, width), BF16),
        pltpu.VMEM((LEVELS, lpad, width), BF16),
        pltpu.VMEM((lpad, lrows), BF16),
        pltpu.VMEM((width, hidden), BF16),
        pltpu.VMEM((width, rank), BF16),
        pltpu.VMEM((part, hidden), BF16),
        pltpu.VMEM((part, hidden), BF16),
        pltpu.VMEM((LEVELS, lpad, hidden2), BF16),
        pltpu.VMEM((LEVELS, lpad, hidden), F32),
        pltpu.VMEM((LEVELS, lpad, hidden), F32),
        pltpu.VMEM((LEVELS, lpad, hidden), BF16),
        pltpu.VMEM((n_dp, LEVELS, 2, lpad, hidden), BF16),
        pltpu.VMEM((2 * n_dp - 1, LEVELS, lpad, rk), BF16),
        pltpu.VMEM((LEVELS, lpad, rank), BF16),
        pltpu.VMEM((n_dp, LEVELS, lrows, part), BF16),
        pltpu.VMEM((n_dp, rows, part), BF16),
        pltpu.VMEM((n_dp - 1, tok_rows, part), BF16),
        pltpu.VMEM((n_dp - 1, rk, hidden), BF16),
        pltpu.VMEM((n_dp - 1, rk, hidden), BF16),
        pltpu.VMEM((rank, hidden), F32),
        dma((8,)), dma((LEVELS,)),
        dma((2,)), dma((LEVELS,)), dma((2,)), dma((1,)), dma((4,)), dma((4,)),
        dma((n_dp,)), dma((n_dp,)), dma((n_dp,)), dma((n_dp,)),
        dma((n_dp, LEVELS)), dma((n_dp, LEVELS)), dma((n_dp,)), dma((n_dp,)),
        dma((n_dp,)), dma((n_dp,)), dma((n_dp,)), dma((n_dp,)),
        dma((n_dp,)), dma((n_dp,)), dma((n_dp,)), dma((n_dp,)),
        pltpu.SemaphoreType.REGULAR,
    ]
    outputs = tok_rows * width * 2 + 3 * rk * hidden * 4
    in_part, proj = pl.pallas_call(
        functools.partial(kernel, n_dp, n_ex, cap, cp),
        out_shape=(pltpu.VMEM((n_dp, tok_rows, part), BF16), pltpu.VMEM((3, rk, hidden), F32)),
        in_specs=[hbm] * 9,
        out_specs=(vmem, vmem),
        scratch_shapes=scratch,
        compiler_params=pltpu.CompilerParams(
            collective_id=0, has_side_effects=True, vmem_limit_bytes=VMEM_BYTES - outputs
        ),
    )(
        expert_ids.T, gate_probs.T, tokens, out_grad, saved_pre,
        gate_weight, up_weight, down_weight, basis,
    )
    return pl.pallas_call(
        finish,
        out_shape=(
            jax.ShapeDtypeStruct((tok_rows, width), BF16),
            jax.ShapeDtypeStruct((1, 3, rk, hidden), F32),
        ),
        in_specs=[hbm, hbm],
        out_specs=(hbm, hbm),
        scratch_shapes=[dma((3,)), dma((n_dp,))],
        compiler_params=pltpu.CompilerParams(vmem_limit_bytes=1024 * 1024),
    )(in_part, proj)


def solution(mesh):
    return jax.shard_map(
        body,
        mesh=mesh,
        in_specs=(
            P(("dp", "expert"), None),
            P(("dp", "expert"), None),
            P(("dp", "expert"), None),
            P(("dp", "expert"), None),
            P("dp", "expert", None, None),
            P("expert", "dp", None),
            P("expert", "dp", None),
            P("expert", "dp", None),
            P("expert", "dp", None),
        ),
        out_specs=(P(("dp", "expert"), None), P("expert", None, "dp", None)),
        check_vma=False,
    )
```

```python
import functools
import jax
import jax.numpy as jnp
from jax import lax
from jax.experimental import pallas as pl
from jax.experimental.pallas import tpu as pltpu
from jax.sharding import PartitionSpec as P

MESH = pl.DeviceIdType.MESH
F32 = jnp.float32
BF16 = jnp.bfloat16
LEVELS = 4
VMEM_BYTES = 67043328


def dot(left, right, dims):
    return lax.dot_general(left, right, (dims, ((), ())), preferred_element_type=F32)


NN = ((1,), (0,))
TN = ((0,), (0,))
NT = ((1,), (1,))


def kernel(
    n_dp, n_ex, cap, cp,
    ids_h, probs_h, tok_h, og_h, pre_h, gw_h, uw_h, dw, bs,
    in_out, total,
    ids, probs, tok, og, tok2, og2, ids2, probs2, idsd, pick_v, sx, sg, rx, rg, dyc, spr, dfull, bfull, gw, uw, gwt, uwt, pre,
    act_a, act_b, hid, gu, px, pdy, rs, rr, in_v, psend, prec, term,
    local_sem, pre_sem, dy_s, dy_r, x_s, x_r, mate_s, mate_r, down_s, down_r, base_s, base_r,
    gu_s, gu_r, ret_s, ret_r, px_s, px_r, proj_s, proj_r, in_s, in_r, ids_s, ids_r, ready,
):
    my_dp = lax.axis_index("dp")
    me = lax.axis_index("expert")
    rows = n_ex * cp
    half = n_ex // 2
    nl = n_ex // LEVELS
    lrows = nl * cp
    lcap = nl * cap
    tokens, width = tok.shape
    topk = ids.shape[0]
    hidden = dfull.shape[1]
    part = width // n_dp
    rank = bfull.shape[1]
    rk = rank // n_dp
    shift = cp.bit_length() - 1
    fw = 256

    z = lax.div(me, nl)
    spot = lax.rem(me, nl)
    mate = lax.rem(me + half, n_ex)
    half0 = lax.div(me, half) * half
    levels = [z + 1 - 2 * lax.rem(z, 2), lax.rem(z + 2, LEVELS), LEVELS - 1 - z, z]
    own = LEVELS - 1

    def block(owner):
        return pl.ds(pl.multiple_of(owner * cp, cp), cp)

    def wpart(owner):
        return pl.ds(pl.multiple_of(owner * part, part), part)

    def rpart(owner):
        return pl.ds(pl.multiple_of(owner * rk, rk), rk)

    def rank_cols(owner):
        line = lax.broadcasted_iota(jnp.int32, (rank, rk), 0)
        lane = lax.broadcasted_iota(jnp.int32, (rank, rk), 1) + owner * rk
        return jnp.where(line == lane, one, zero).astype(BF16)

    def lpart(j):
        return pl.ds(pl.multiple_of(levels[j] * lrows, lrows), lrows)

    def ex_peer(k):
        return lax.rem(me + k, n_ex)

    def half_peer(k):
        return half0 + lax.rem(me - half0 + k, half)

    def in_level(j, t):
        return levels[j] * nl + lax.rem(spot + t, nl)

    def dp_peer(i):
        return lax.rem(my_dp + i, n_dp)

    def dp_from(i):
        return lax.rem(my_dp + n_dp - i, n_dp)

    first = [
        pltpu.make_async_copy(ids_h, ids, local_sem.at[6]),
        pltpu.make_async_copy(probs_h, probs, local_sem.at[7]),
    ]
    for copy in first:
        copy.start()

    barrier = pltpu.get_barrier_semaphore()

    for i in range(1, n_dp):
        pl.semaphore_signal(barrier, inc=1, device_id={"dp": dp_peer(i)}, device_id_type=MESH)

    odd = lax.rem(me, 2)

    @pl.loop(odd, half)
    def _(k):
        hub = lax.rem(me + 1 - odd + 2 * k, n_ex)
        pl.semaphore_signal(barrier, inc=1, device_id={"expert": hub}, device_id_type=MESH)

    @pl.when(odd == 1)
    def _():
        pl.semaphore_signal(barrier, inc=1, device_id={"expert": me - 1}, device_id_type=MESH)

    pad = gu.shape[3] - lcap
    if pad:
        for j in range(LEVELS):
            pre[j, lcap:, :] = jnp.zeros((pad, 2 * hidden), BF16)
            for i in range(1, n_dp):
                px[n_dp - 1 + i, j, lcap:, :] = jnp.zeros((pad, rk), BF16)
                for s in range(2):
                    gu[i, j, s, lcap:, :] = jnp.zeros((pad, hidden), BF16)

    local = [
        pltpu.make_async_copy(og_h, og, local_sem.at[0]),
        pltpu.make_async_copy(tok_h, tok, local_sem.at[1]),
        pltpu.make_async_copy(dw.at[0], dfull.at[wpart(my_dp)], local_sem.at[2]),
        pltpu.make_async_copy(bs.at[0], bfull.at[wpart(my_dp)], local_sem.at[3]),
        pltpu.make_async_copy(gw_h.at[0], gw, local_sem.at[4]),
        pltpu.make_async_copy(uw_h.at[0], uw, local_sem.at[5]),
    ]
    pre_copy = []
    for j in range(LEVELS):
        src = pl.ds(pl.multiple_of(levels[j] * lcap, 8), lcap)
        pre_copy.append(
            pltpu.make_async_copy(pre_h.at[0, 0, src], pre.at[j, pl.ds(0, lcap)], pre_sem.at[j])
        )
    for copy in local[:2] + pre_copy + local[2:]:
        copy.start()

    def down_copy(i, owner, peer):
        return pltpu.make_async_remote_copy(
            dw.at[0], dfull.at[wpart(owner)], down_s.at[i - 1], down_r.at[i - 1],
            device_id={"dp": peer}, device_id_type=MESH,
        )

    def base_copy(i, owner, peer):
        return pltpu.make_async_remote_copy(
            bs.at[0], bfull.at[wpart(owner)], base_s.at[i - 1], base_r.at[i - 1],
            device_id={"dp": peer}, device_id_type=MESH,
        )

    def ids_copy(i, peer):
        return pltpu.make_async_remote_copy(
            ids_h, idsd.at[i - 1], ids_s.at[i - 1], ids_r.at[i - 1],
            device_id={"dp": peer}, device_id_type=MESH,
        )

    def mate_copy(n):
        src, dst = ((og, og2), (tok, tok2), (ids, ids2), (probs, probs2))[n]
        return pltpu.make_async_remote_copy(
            src, dst, mate_s.at[n], mate_r.at[n], device_id={"expert": mate}, device_id_type=MESH
        )

    def dy_copy(m, peer, owner, j):
        return pltpu.make_async_remote_copy(
            sg.at[m, block(peer - half0)], rg.at[block(owner)], dy_s.at[m], dy_r.at[j],
            device_id={"expert": peer}, device_id_type=MESH,
        )

    def x_copy(m, peer, owner):
        return pltpu.make_async_remote_copy(
            sx.at[m, block(peer - half0)], rx.at[block(owner)], x_s.at[m], x_r.at[0],
            device_id={"expert": peer}, device_id_type=MESH,
        )

    def blocks(buffer, count, send, recv):
        span = buffer.at[pl.ds(0, count * cp)]
        return pltpu.make_async_remote_copy(
            span, span, send, recv, device_id={"expert": mate}, device_id_type=MESH
        )

    used = pl.ds(0, lcap)

    def gu_copy(i, j, peer):
        return pltpu.make_async_remote_copy(
            gu.at[0, j, :, used], gu.at[i, j, :, used], gu_s.at[i - 1, j], gu_r.at[i - 1, j],
            device_id={"dp": peer}, device_id_type=MESH,
        )

    def px_copy(i, peer):
        return pltpu.make_async_remote_copy(
            px.at[i - 1, :, used], px.at[n_dp - 1 + i, :, used], px_s.at[i - 1], px_r.at[i - 1],
            device_id={"dp": peer}, device_id_type=MESH,
        )

    def ret_copy(i, j, peer, owner, cols):
        return pltpu.make_async_remote_copy(
            rs.at[i, j, block(lax.rem(peer, nl)), cols], rr.at[i, block(owner), cols],
            ret_s.at[i], ret_r.at[i],
            device_id={"expert": peer}, device_id_type=MESH,
        )

    def proj_copy(i, peer):
        return pltpu.make_async_remote_copy(
            psend.at[i - 1], prec.at[i - 1], proj_s.at[i - 1], proj_r.at[i - 1],
            device_id={"dp": peer}, device_id_type=MESH,
        )

    def in_copy(i, owner, peer):
        return pltpu.make_async_remote_copy(
            in_v.at[i - 1], in_out.at[owner], in_s.at[i - 1], in_r.at[i - 1],
            device_id={"dp": peer}, device_id_type=MESH,
        )

    def start_dp():
        for i in range(1, n_dp):
            ids_copy(i, dp_peer(i)).start()
        for i in range(1, n_dp):
            down_copy(i, my_dp, dp_peer(i)).start()
        for i in range(1, n_dp):
            base_copy(i, my_dp, dp_peer(i)).start()

    @pl.when(odd == 0)
    def _():
        pl.semaphore_wait(barrier, n_dp)
        start_dp()

    one, zero = jnp.ones((), F32), jnp.zeros((), F32)
    earlier = lax.broadcasted_iota(jnp.int32, (tokens, tokens), 0) < lax.broadcasted_iota(
        jnp.int32, (tokens, tokens), 1
    )
    earlier = jnp.where(earlier, one, zero).astype(BF16)

    def pick_of(names_of, first, count):
        line = lax.broadcasted_iota(jnp.int32, (count, tokens), 0)
        line_expert = lax.shift_right_logical(line, shift) + first
        line_slot = lax.bitwise_and(line, cp - 1)
        names = [names_of[k : k + 1, :] == line_expert for k in range(topk)]
        any_name = functools.reduce(jnp.logical_or, names)
        named = jnp.where(any_name, one, zero).astype(BF16)
        before = dot(named, earlier, NN)
        at_slot = before == line_slot.astype(F32)
        pick = jnp.where(jnp.logical_and(any_name, at_slot), one, zero).astype(BF16)
        return pick, names, at_slot

    def half_pick(names_of, weights_of):
        pick, names, at_slot = pick_of(names_of, half0, half * cp)
        weights = functools.reduce(
            jnp.add, [jnp.where(name, weights_of[k : k + 1, :], zero) for k, name in enumerate(names)]
        )
        return pick, jnp.sum(jnp.where(at_slot, weights, zero), axis=1, keepdims=True)

    for copy in first:
        copy.wait()
    pick, weight = half_pick(ids, probs)

    local[0].wait()
    sg[0] = (dot(pick, og[...], NN) * weight).astype(BF16)

    @pl.when(odd == 1)
    def _():
        pl.semaphore_wait(barrier, n_dp + n_ex - 2)
        start_dp()
        pl.semaphore_signal(ready, inc=1, device_id={"expert": me - 1}, device_id_type=MESH)

    @pl.when(odd == 0)
    def _():
        pl.semaphore_wait(ready, 1)

    mate_copy(2).start()
    mate_copy(3).start()
    mate_copy(0).start()

    def dispatch_dy(m, owner):
        for near, tag in ((0, 0 if m == 0 else 2), (own, own if m == 0 else 1)):

            @pl.loop(int(near == own), nl)
            def _(t):
                dy_copy(m, in_level(near, t), owner, tag).start()

        rg[block(owner), :] = sg[m, block(me - half0), :]

    def dispatch_x(m, owner):
        @pl.loop(1, half)
        def _(k):
            x_copy(m, half_peer(k), owner).start()

        rx[block(owner), :] = sx[m, block(me - half0), :]

    dispatch_dy(0, me)
    grid = (gu.shape[3], lrows)
    line = lax.broadcasted_iota(jnp.int32, grid, 1)
    inner = lax.bitwise_and(line, cp - 1)
    target = lax.shift_right_logical(line, shift) * cap + inner
    spread = jnp.logical_and(target == lax.broadcasted_iota(jnp.int32, grid, 0), inner < cap)
    spr[...] = jnp.where(spread, one, zero).astype(BF16)

    for j in range(LEVELS):
        pre_copy[j].wait()
        for f in range(0, hidden, fw):
            cols = slice(f, f + fw)
            g = pre[j, :, f : f + fw].astype(F32)
            u = pre[j, :, hidden + f : hidden + f + fw].astype(F32)
            sig = jax.nn.sigmoid(g)
            gs = g * sig
            act_a[j, :, cols] = gs
            hid[j, :, cols] = (gs * u).astype(BF16)
            act_b[j, :, cols] = u * sig * (1.0 + g * (1.0 - sig))

    def row_grad(i, j, pieces=1):
        span = part // pieces
        for piece in range(pieces):
            cols = pl.ds(piece * span, span)
            out = dot(gu[i, j, 0], gwt[:, cols], NN) + dot(gu[i, j, 1], uwt[:, cols], NN)
            rs[i, j, :, cols] = dot(spr[...], out.astype(BF16), TN).astype(BF16)

            @pl.loop(int(j == own), nl)
            def _(t):
                ret_copy(i, j, in_level(j, t), me, cols).start()

        if j == own:
            rr[i, block(me), :] = rs[i, j, block(spot), :]

    same = lax.broadcasted_iota(jnp.int32, (fw, fw), 0) == lax.broadcasted_iota(jnp.int32, (fw, fw), 1)
    same = jnp.where(same, one, zero).astype(BF16)
    for copy, weights, turned in ((local[4], gw, gwt), (local[5], uw, uwt)):
        copy.wait()
        for f in range(0, hidden, fw):
            turned[f : f + fw, :] = dot(same, weights[:, f : f + fw], NT).astype(BF16)

    pick_v[0] = pick_of(ids, 0, rows)[0]
    for i in range(1, n_dp):
        ids_copy(i, dp_peer(i)).wait_recv()
        pick_v[i] = pick_of(idsd.at[i - 1], 0, rows)[0]

    mate_copy(2).wait_recv()
    mate_copy(3).wait_recv()
    pick2, weight2 = half_pick(ids2, probs2)
    mate_copy(0).wait_recv()
    sg[1] = (dot(pick2, og2[...], NN) * weight2).astype(BF16)
    dispatch_dy(1, mate)

    local[1].wait()
    mate_copy(1).start()
    sx[0] = dot(pick, tok[...], NN).astype(BF16)
    dispatch_x(0, me)

    local[2].wait()
    for i in range(1, n_dp):
        down_copy(i, dp_from(i), dp_peer(i)).wait_recv()

    for j in range(LEVELS):

        blocks(rg, nl - j % 2, dy_s.at[0], dy_r.at[j]).wait_recv()
        dyc[j] = dot(spr[...], rg[lpart(j), :], NN).astype(BF16)
        for f in range(0, hidden, fw):
            cols = slice(f, f + fw)
            hg = dot(dyc[j], dfull[:, cols], NN)
            gu[0, j, 1, :, cols] = (hg * act_a[j, :, cols]).astype(BF16)
            gu[0, j, 0, :, cols] = (hg * act_b[j, :, cols]).astype(BF16)
        for i in range(1, n_dp):
            gu_copy(i, j, dp_peer(i)).start()
        row_grad(0, j)

    local[3].wait()
    for i in range(1, n_dp):
        base_copy(i, dp_from(i), dp_peer(i)).wait_recv()
    for j in range(LEVELS):
        pdy[j] = dot(dyc[j], bfull[...], NN).astype(BF16)

    def project(left, right):
        return functools.reduce(jnp.add, [dot(left(j), right(j), TN) for j in range(LEVELS)])

    term[...] = project(lambda j: pdy[j], lambda j: hid[j])
    for i in range(1, n_dp):
        psend[i - 1] = term[rpart(dp_peer(i)), :].astype(BF16)
    total[2] = term[rpart(my_dp), :]

    mate_copy(1).wait_recv()
    sx[1] = dot(pick2, tok2[...], NN).astype(BF16)
    dispatch_x(1, mate)

    def theirs(j):
        for i in range(1, n_dp):
            gu_copy(i, j, dp_peer(i)).wait_recv()
            if j == own and i == n_dp - 1:
                pl.when(odd == 0)(start_projections)
            row_grad(i, j, 2 if j == own and part % 256 == 0 else 1)

    theirs(0)

    theirs(1)

    blocks(rx, n_ex - 2, x_s.at[0], x_r.at[0]).wait_recv()
    for j in range(LEVELS):
        xj = dot(spr[...], rx[lpart(j), :], NN).astype(BF16)
        if rk % 128:
            xp = dot(xj, bfull[...], NN).astype(BF16)
        for i in range(n_dp):
            if rk % 128:
                pj = dot(xp, rank_cols(dp_peer(i)), NN)
            else:
                pj = dot(xj, bfull[:, rpart(dp_peer(i))], NN)
            px[(i + n_dp - 1) % n_dp, j] = pj.astype(BF16)

    def start_projections():
        for i in range(1, n_dp):
            proj_copy(i, dp_peer(i)).start()
            px_copy(i, dp_peer(i)).start()

    pl.when(odd == 1)(start_projections)

    theirs(2)

    def x_term(s, i):
        left = px.at[n_dp - 1 + i]
        return project(lambda j: left[j], lambda j: gu[i, j, s])

    for s in range(2):
        total[s] = x_term(s, 0)

    def combine(i):
        blocks(rr.at[i], n_ex - 1, ret_s.at[i], ret_r.at[i]).wait_recv()
        return dot(pick_v[i], rr[i], TN).astype(BF16)

    in_out[my_dp] = combine(0)

    theirs(3)
    for i in range(1, n_dp):
        in_v[i - 1] = combine(i)
        in_copy(i, my_dp, dp_from(i)).start()

    for i in range(1, n_dp):
        proj_copy(i, dp_peer(i)).wait_recv()
        total[2] += prec[i - 1].astype(F32)
    for i in range(1, n_dp):
        px_copy(i, dp_peer(i)).wait_recv()
        for s in range(2):
            total[s] += x_term(s, i)

    for i in range(1, n_dp):
        down_copy(i, my_dp, dp_peer(i)).wait_send()
        base_copy(i, my_dp, dp_peer(i)).wait_send()
        ids_copy(i, dp_peer(i)).wait_send()
        px_copy(i, dp_peer(i)).wait_send()
        proj_copy(i, dp_peer(i)).wait_send()
        for j in range(LEVELS):
            gu_copy(i, j, dp_peer(i)).wait_send()
    for n in range(4):
        mate_copy(n).wait_send()
    for m in range(2):
        blocks(rg, half - 1, dy_s.at[m], dy_r.at[0]).wait_send()
        blocks(rx, half - 1, x_s.at[m], x_r.at[0]).wait_send()
    for i in range(n_dp):
        blocks(rr.at[i], n_ex - 1, ret_s.at[i], ret_r.at[i]).wait_send()
    for i in range(1, n_dp):
        in_copy(i, my_dp, dp_from(i)).wait_send()
        in_copy(i, dp_peer(i), dp_from(i)).wait_recv()


def finish(in_h, proj_h, in_ref, proj_ref, proj_s, in_s):
    parts, _, part = in_h.shape
    n = proj_h.shape[0]
    copies = [pltpu.make_async_copy(proj_h.at[t], proj_ref.at[0, t], proj_s.at[t]) for t in range(n)]
    for d in range(parts):
        cols = pl.ds(d * part, part)
        copies.append(pltpu.make_async_copy(in_h.at[d], in_ref.at[:, cols], in_s.at[d]))
    for copy in copies:
        copy.start()
    for copy in copies:
        copy.wait()


def body(
    tokens, out_grad, expert_ids, gate_probs, saved_pre, gate_weight, up_weight, down_weight, basis
):
    n_dp, n_ex = lax.axis_size("dp"), lax.axis_size("expert")
    tok_rows, width = tokens.shape
    topk = expert_ids.shape[1]
    slots, hidden2 = saved_pre.shape[2:]
    hidden = hidden2 // 2
    cap = slots // n_ex
    cp = max(16, 1 << (cap - 1).bit_length())
    rows = n_ex * cp
    nl = n_ex // LEVELS
    lrows = nl * cp
    lpad = -(-nl * cap // 16) * 16
    part = gate_weight.shape[1]
    rank = basis.shape[2]
    rk = rank // n_dp
    vmem = pl.BlockSpec(memory_space=pltpu.VMEM)
    hbm = pl.BlockSpec(memory_space=pl.ANY)
    dma = pltpu.SemaphoreType.DMA
    scratch = [
        pltpu.VMEM((topk, tok_rows), jnp.int32),
        pltpu.VMEM((topk, tok_rows), F32),
        pltpu.VMEM((tok_rows, width), BF16),
        pltpu.VMEM((tok_rows, width), BF16),
        pltpu.VMEM((tok_rows, width), BF16),
        pltpu.VMEM((tok_rows, width), BF16),
        pltpu.VMEM((topk, tok_rows), jnp.int32),
        pltpu.VMEM((topk, tok_rows), F32),
        pltpu.VMEM((n_dp - 1, topk, tok_rows), jnp.int32),
        pltpu.VMEM((n_dp, rows, tok_rows), BF16),
        pltpu.VMEM((2, rows // 2, width), BF16),
        pltpu.VMEM((2, rows // 2, width), BF16),
        pltpu.VMEM((rows, width), BF16),
        pltpu.VMEM((rows, width), BF16),
        pltpu.VMEM((LEVELS, lpad, width), BF16),
        pltpu.VMEM((lpad, lrows), BF16),
        pltpu.VMEM((width, hidden), BF16),
        pltpu.VMEM((width, rank), BF16),
        pltpu.VMEM((part, hidden), BF16),
        pltpu.VMEM((part, hidden), BF16),
        pltpu.VMEM((hidden, part), BF16),
        pltpu.VMEM((hidden, part), BF16),
        pltpu.VMEM((LEVELS, lpad, hidden2), BF16),
        pltpu.VMEM((LEVELS, lpad, hidden), F32),
        pltpu.VMEM((LEVELS, lpad, hidden), F32),
        pltpu.VMEM((LEVELS, lpad, hidden), BF16),
        pltpu.VMEM((n_dp, LEVELS, 2, lpad, hidden), BF16),
        pltpu.VMEM((2 * n_dp - 1, LEVELS, lpad, rk), BF16),
        pltpu.VMEM((LEVELS, lpad, rank), BF16),
        pltpu.VMEM((n_dp, LEVELS, lrows, part), BF16),
        pltpu.VMEM((n_dp, rows, part), BF16),
        pltpu.VMEM((n_dp - 1, tok_rows, part), BF16),
        pltpu.VMEM((n_dp - 1, rk, hidden), BF16),
        pltpu.VMEM((n_dp - 1, rk, hidden), BF16),
        pltpu.VMEM((rank, hidden), F32),
        dma((8,)), dma((LEVELS,)),
        dma((2,)), dma((LEVELS,)), dma((2,)), dma((1,)), dma((4,)), dma((4,)),
        dma((n_dp - 1,)), dma((n_dp - 1,)), dma((n_dp - 1,)), dma((n_dp - 1,)),
        dma((n_dp - 1, LEVELS)), dma((n_dp - 1, LEVELS)), dma((n_dp,)), dma((n_dp,)),
        dma((n_dp - 1,)), dma((n_dp - 1,)), dma((n_dp - 1,)), dma((n_dp - 1,)),
        dma((n_dp - 1,)), dma((n_dp - 1,)), dma((n_dp - 1,)), dma((n_dp - 1,)),
        pltpu.SemaphoreType.REGULAR,
    ]
    outputs = tok_rows * width * 2 + 3 * rk * hidden * 4
    in_part, proj = pl.pallas_call(
        functools.partial(kernel, n_dp, n_ex, cap, cp),
        out_shape=(pltpu.VMEM((n_dp, tok_rows, part), BF16), pltpu.VMEM((3, rk, hidden), F32)),
        in_specs=[hbm] * 9,
        out_specs=(vmem, vmem),
        scratch_shapes=scratch,
        compiler_params=pltpu.CompilerParams(
            collective_id=0, has_side_effects=True, vmem_limit_bytes=VMEM_BYTES - outputs
        ),
    )(
        expert_ids.T, gate_probs.T, tokens, out_grad, saved_pre,
        gate_weight, up_weight, down_weight, basis,
    )
    return pl.pallas_call(
        finish,
        out_shape=(
            jax.ShapeDtypeStruct((tok_rows, width), BF16),
            jax.ShapeDtypeStruct((1, 3, rk, hidden), F32),
        ),
        in_specs=[hbm, hbm],
        out_specs=(hbm, hbm),
        scratch_shapes=[dma((3,)), dma((n_dp,))],
        compiler_params=pltpu.CompilerParams(vmem_limit_bytes=1024 * 1024),
    )(in_part, proj)


def solution(mesh):
    return jax.shard_map(
        body,
        mesh=mesh,
        in_specs=(
            P(("dp", "expert"), None),
            P(("dp", "expert"), None),
            P(("dp", "expert"), None),
            P(("dp", "expert"), None),
            P("dp", "expert", None, None),
            P("expert", "dp", None),
            P("expert", "dp", None),
            P("expert", "dp", None),
            P("expert", "dp", None),
        ),
        out_specs=(P(("dp", "expert"), None), P("expert", None, "dp", None)),
        check_vma=False,
    )
```

```python
import functools
import jax
import jax.numpy as jnp
from jax import lax
from jax.experimental import pallas as pl
from jax.experimental.pallas import tpu as pltpu
from jax.sharding import PartitionSpec as P

MESH = pl.DeviceIdType.MESH
F32 = jnp.float32
BF16 = jnp.bfloat16
LEVELS = 4
VMEM_BYTES = 67043328


def dot(left, right, dims):
    return lax.dot_general(left, right, (dims, ((), ())), preferred_element_type=F32)


NN = ((1,), (0,))
TN = ((0,), (0,))
NT = ((1,), (1,))


def kernel(
    n_dp, n_ex, cap, cp,
    ids_h, probs_h, tok_h, og_h, pre_h, gw_h, uw_h, dw, bs,
    in_out, total,
    ids, probs, tok, og, tok2, og2, ids2, probs2, idsd, pick_v, sx, sg, rx, rg, dyc, spr, dfull, bfull, gw, uw, gwt, uwt, pre,
    act_a, act_b, hid, gu, px, pdy, rs, rr, in_v, psend, prec, term,
    local_sem, pre_sem, dy_s, dy_r, x_s, x_r, mate_s, mate_r, down_s, down_r, base_s, base_r,
    gu_s, gu_r, ret_s, ret_r, px_s, px_r, proj_s, proj_r, in_s, in_r, ids_s, ids_r, ready,
):
    my_dp = lax.axis_index("dp")
    me = lax.axis_index("expert")
    rows = n_ex * cp
    half = n_ex // 2
    nl = n_ex // LEVELS
    lrows = nl * cp
    lcap = nl * cap
    tokens, width = tok.shape
    topk = ids.shape[0]
    hidden = dfull.shape[1]
    part = width // n_dp
    rank = bfull.shape[1]
    rk = rank // n_dp
    shift = cp.bit_length() - 1
    fw = 256

    z = lax.div(me, nl)
    spot = lax.rem(me, nl)
    mate = lax.rem(me + half, n_ex)
    half0 = lax.div(me, half) * half
    levels = [z + 1 - 2 * lax.rem(z, 2), lax.rem(z + 2, LEVELS), LEVELS - 1 - z, z]
    own = LEVELS - 1

    def block(owner):
        return pl.ds(pl.multiple_of(owner * cp, cp), cp)

    def wpart(owner):
        return pl.ds(pl.multiple_of(owner * part, part), part)

    def rpart(owner):
        return pl.ds(pl.multiple_of(owner * rk, rk), rk)

    def rank_cols(owner):
        line = lax.broadcasted_iota(jnp.int32, (rank, rk), 0)
        lane = lax.broadcasted_iota(jnp.int32, (rank, rk), 1) + owner * rk
        return jnp.where(line == lane, one, zero).astype(BF16)

    def lpart(j):
        return pl.ds(pl.multiple_of(levels[j] * lrows, lrows), lrows)

    def ex_peer(k):
        return lax.rem(me + k, n_ex)

    def half_peer(k):
        return half0 + lax.rem(me - half0 + k, half)

    def in_level(j, t):
        return levels[j] * nl + lax.rem(spot + t, nl)

    def dp_peer(i):
        return lax.rem(my_dp + i, n_dp)

    def dp_from(i):
        return lax.rem(my_dp + n_dp - i, n_dp)

    first = [
        pltpu.make_async_copy(ids_h, ids, local_sem.at[6]),
        pltpu.make_async_copy(probs_h, probs, local_sem.at[7]),
    ]
    for copy in first:
        copy.start()

    barrier = pltpu.get_barrier_semaphore()

    for i in range(1, n_dp):
        pl.semaphore_signal(barrier, inc=1, device_id={"dp": dp_peer(i)}, device_id_type=MESH)

    odd = lax.rem(me, 2)

    @pl.loop(odd, half)
    def _(k):
        hub = lax.rem(me + 1 - odd + 2 * k, n_ex)
        pl.semaphore_signal(barrier, inc=1, device_id={"expert": hub}, device_id_type=MESH)

    @pl.when(odd == 1)
    def _():
        pl.semaphore_signal(barrier, inc=1, device_id={"expert": me - 1}, device_id_type=MESH)

    pad = gu.shape[3] - lcap
    if pad:
        for j in range(LEVELS):
            pre[j, lcap:, :] = jnp.zeros((pad, 2 * hidden), BF16)
            for i in range(1, n_dp):
                px[n_dp - 1 + i, j, lcap:, :] = jnp.zeros((pad, rk), BF16)
                for s in range(2):
                    gu[i, j, s, lcap:, :] = jnp.zeros((pad, hidden), BF16)

    local = [
        pltpu.make_async_copy(og_h, og, local_sem.at[0]),
        pltpu.make_async_copy(tok_h, tok, local_sem.at[1]),
        pltpu.make_async_copy(dw.at[0], dfull.at[wpart(my_dp)], local_sem.at[2]),
        pltpu.make_async_copy(bs.at[0], bfull.at[wpart(my_dp)], local_sem.at[3]),
        pltpu.make_async_copy(gw_h.at[0], gw, local_sem.at[4]),
        pltpu.make_async_copy(uw_h.at[0], uw, local_sem.at[5]),
    ]
    pre_copy = []
    for j in range(LEVELS):
        src = pl.ds(pl.multiple_of(levels[j] * lcap, 8), lcap)
        pre_copy.append(
            pltpu.make_async_copy(pre_h.at[0, 0, src], pre.at[j, pl.ds(0, lcap)], pre_sem.at[j])
        )
    for copy in local[:2] + pre_copy + local[2:]:
        copy.start()

    def down_copy(i, owner, peer):
        return pltpu.make_async_remote_copy(
            dw.at[0], dfull.at[wpart(owner)], down_s.at[i - 1], down_r.at[i - 1],
            device_id={"dp": peer}, device_id_type=MESH,
        )

    def base_copy(i, owner, peer):
        return pltpu.make_async_remote_copy(
            bs.at[0], bfull.at[wpart(owner)], base_s.at[i - 1], base_r.at[i - 1],
            device_id={"dp": peer}, device_id_type=MESH,
        )

    def ids_copy(i, peer):
        return pltpu.make_async_remote_copy(
            ids_h, idsd.at[i - 1], ids_s.at[i - 1], ids_r.at[i - 1],
            device_id={"dp": peer}, device_id_type=MESH,
        )

    def mate_copy(n):
        src, dst = ((og, og2), (tok, tok2), (ids, ids2), (probs, probs2))[n]
        return pltpu.make_async_remote_copy(
            src, dst, mate_s.at[n], mate_r.at[n], device_id={"expert": mate}, device_id_type=MESH
        )

    def dy_copy(m, peer, owner, j):
        return pltpu.make_async_remote_copy(
            sg.at[m, block(peer - half0)], rg.at[block(owner)], dy_s.at[m], dy_r.at[j],
            device_id={"expert": peer}, device_id_type=MESH,
        )

    def x_copy(m, peer, owner):
        return pltpu.make_async_remote_copy(
            sx.at[m, block(peer - half0)], rx.at[block(owner)], x_s.at[m], x_r.at[0],
            device_id={"expert": peer}, device_id_type=MESH,
        )

    def blocks(buffer, count, send, recv):
        span = buffer.at[pl.ds(0, count * cp)]
        return pltpu.make_async_remote_copy(
            span, span, send, recv, device_id={"expert": mate}, device_id_type=MESH
        )

    used = pl.ds(0, lcap)

    def gu_copy(i, j, peer):
        return pltpu.make_async_remote_copy(
            gu.at[0, j, :, used], gu.at[i, j, :, used], gu_s.at[i - 1, j], gu_r.at[i - 1, j],
            device_id={"dp": peer}, device_id_type=MESH,
        )

    def px_copy(i, peer):
        return pltpu.make_async_remote_copy(
            px.at[i - 1, :, used], px.at[n_dp - 1 + i, :, used], px_s.at[i - 1], px_r.at[i - 1],
            device_id={"dp": peer}, device_id_type=MESH,
        )

    halves = 2 if part % 256 == 0 else 1

    def cut(i):
        return halves if i else 1

    def piece_cols(i, piece):
        return pl.ds(piece * (part // cut(i)), part // cut(i))

    def ret_all(i, piece):
        span = rr.at[i, pl.ds(0, (n_ex - 1) * cp), piece_cols(i, piece)]
        return pltpu.make_async_remote_copy(
            span, span, ret_s.at[i, piece], ret_r.at[i, piece],
            device_id={"expert": mate}, device_id_type=MESH,
        )

    def ret_copy(i, j, peer, owner, piece):
        cols = piece_cols(i, piece)
        return pltpu.make_async_remote_copy(
            rs.at[i, j, block(lax.rem(peer, nl)), cols], rr.at[i, block(owner), cols],
            ret_s.at[i, piece], ret_r.at[i, piece],
            device_id={"expert": peer}, device_id_type=MESH,
        )

    def proj_copy(i, peer):
        return pltpu.make_async_remote_copy(
            psend.at[i - 1], prec.at[i - 1], proj_s.at[i - 1], proj_r.at[i - 1],
            device_id={"dp": peer}, device_id_type=MESH,
        )

    def in_copy(i, piece, owner, peer):
        cols = piece_cols(i, piece)
        return pltpu.make_async_remote_copy(
            in_v.at[i - 1, :, cols], in_out.at[owner, :, cols],
            in_s.at[i - 1, piece], in_r.at[i - 1, piece],
            device_id={"dp": peer}, device_id_type=MESH,
        )

    def start_dp():
        for i in range(1, n_dp):
            ids_copy(i, dp_peer(i)).start()
        for i in range(1, n_dp):
            down_copy(i, my_dp, dp_peer(i)).start()
        for i in range(1, n_dp):
            base_copy(i, my_dp, dp_peer(i)).start()

    @pl.when(odd == 0)
    def _():
        pl.semaphore_wait(barrier, n_dp)
        start_dp()

    one, zero = jnp.ones((), F32), jnp.zeros((), F32)
    earlier = lax.broadcasted_iota(jnp.int32, (tokens, tokens), 0) < lax.broadcasted_iota(
        jnp.int32, (tokens, tokens), 1
    )
    earlier = jnp.where(earlier, one, zero).astype(BF16)

    def pick_of(names_of, first, count):
        line = lax.broadcasted_iota(jnp.int32, (count, tokens), 0)
        line_expert = lax.shift_right_logical(line, shift) + first
        line_slot = lax.bitwise_and(line, cp - 1)
        names = [names_of[k : k + 1, :] == line_expert for k in range(topk)]
        any_name = functools.reduce(jnp.logical_or, names)
        named = jnp.where(any_name, one, zero).astype(BF16)
        before = dot(named, earlier, NN)
        at_slot = before == line_slot.astype(F32)
        pick = jnp.where(jnp.logical_and(any_name, at_slot), one, zero).astype(BF16)
        return pick, names, at_slot

    def half_pick(names_of, weights_of):
        pick, names, at_slot = pick_of(names_of, half0, half * cp)
        weights = functools.reduce(
            jnp.add, [jnp.where(name, weights_of[k : k + 1, :], zero) for k, name in enumerate(names)]
        )
        return pick, jnp.sum(jnp.where(at_slot, weights, zero), axis=1, keepdims=True)

    for copy in first:
        copy.wait()
    pick, weight = half_pick(ids, probs)

    local[0].wait()
    sg[0] = (dot(pick, og[...], NN) * weight).astype(BF16)

    @pl.when(odd == 1)
    def _():
        pl.semaphore_wait(barrier, n_dp + n_ex - 2)
        start_dp()
        pl.semaphore_signal(ready, inc=1, device_id={"expert": me - 1}, device_id_type=MESH)

    @pl.when(odd == 0)
    def _():
        pl.semaphore_wait(ready, 1)

    mate_copy(2).start()
    mate_copy(3).start()
    mate_copy(0).start()

    def dispatch_dy(m, owner):
        for near, tag in ((0, 0 if m == 0 else 2), (own, own if m == 0 else 1)):

            @pl.loop(int(near == own), nl)
            def _(t):
                dy_copy(m, in_level(near, t), owner, tag).start()

        rg[block(owner), :] = sg[m, block(me - half0), :]

    def dispatch_x(m, owner):
        @pl.loop(1, half)
        def _(k):
            x_copy(m, half_peer(k), owner).start()

        rx[block(owner), :] = sx[m, block(me - half0), :]

    dispatch_dy(0, me)
    grid = (gu.shape[3], lrows)
    line = lax.broadcasted_iota(jnp.int32, grid, 1)
    inner = lax.bitwise_and(line, cp - 1)
    target = lax.shift_right_logical(line, shift) * cap + inner
    spread = jnp.logical_and(target == lax.broadcasted_iota(jnp.int32, grid, 0), inner < cap)
    spr[...] = jnp.where(spread, one, zero).astype(BF16)

    for j in range(LEVELS):
        pre_copy[j].wait()
        for f in range(0, hidden, fw):
            cols = slice(f, f + fw)
            g = pre[j, :, f : f + fw].astype(F32)
            u = pre[j, :, hidden + f : hidden + f + fw].astype(F32)
            sig = jax.nn.sigmoid(g)
            gs = g * sig
            act_a[j, :, cols] = gs
            hid[j, :, cols] = (gs * u).astype(BF16)
            act_b[j, :, cols] = u * sig * (1.0 + g * (1.0 - sig))

    def row_grad(i, j):
        for piece in range(cut(i)):
            cols = piece_cols(i, piece)
            out = dot(gu[i, j, 0], gwt[:, cols], NN) + dot(gu[i, j, 1], uwt[:, cols], NN)
            rs[i, j, :, cols] = dot(spr[...], out.astype(BF16), TN).astype(BF16)

            @pl.loop(int(j == own), nl)
            def _(t):
                ret_copy(i, j, in_level(j, t), me, piece).start()

        if j == own:
            rr[i, block(me), :] = rs[i, j, block(spot), :]

    same = lax.broadcasted_iota(jnp.int32, (fw, fw), 0) == lax.broadcasted_iota(jnp.int32, (fw, fw), 1)
    same = jnp.where(same, one, zero).astype(BF16)
    for copy, weights, turned in ((local[4], gw, gwt), (local[5], uw, uwt)):
        copy.wait()
        for f in range(0, hidden, fw):
            turned[f : f + fw, :] = dot(same, weights[:, f : f + fw], NT).astype(BF16)

    pick_v[0] = pick_of(ids, 0, rows)[0]
    for i in range(1, n_dp):
        ids_copy(i, dp_peer(i)).wait_recv()
        pick_v[i] = pick_of(idsd.at[i - 1], 0, rows)[0]

    mate_copy(2).wait_recv()
    mate_copy(3).wait_recv()
    pick2, weight2 = half_pick(ids2, probs2)
    mate_copy(0).wait_recv()
    sg[1] = (dot(pick2, og2[...], NN) * weight2).astype(BF16)
    dispatch_dy(1, mate)

    local[1].wait()
    mate_copy(1).start()
    sx[0] = dot(pick, tok[...], NN).astype(BF16)
    dispatch_x(0, me)

    local[2].wait()
    for i in range(1, n_dp):
        down_copy(i, dp_from(i), dp_peer(i)).wait_recv()

    for j in range(LEVELS):

        blocks(rg, nl - j % 2, dy_s.at[0], dy_r.at[j]).wait_recv()
        dyc[j] = dot(spr[...], rg[lpart(j), :], NN).astype(BF16)
        for f in range(0, hidden, fw):
            cols = slice(f, f + fw)
            hg = dot(dyc[j], dfull[:, cols], NN)
            gu[0, j, 1, :, cols] = (hg * act_a[j, :, cols]).astype(BF16)
            gu[0, j, 0, :, cols] = (hg * act_b[j, :, cols]).astype(BF16)
        for i in range(1, n_dp):
            gu_copy(i, j, dp_peer(i)).start()
        row_grad(0, j)

    local[3].wait()
    for i in range(1, n_dp):
        base_copy(i, dp_from(i), dp_peer(i)).wait_recv()
    for j in range(LEVELS):
        pdy[j] = dot(dyc[j], bfull[...], NN).astype(BF16)

    def project(left, right):
        return functools.reduce(jnp.add, [dot(left(j), right(j), TN) for j in range(LEVELS)])

    term[...] = project(lambda j: pdy[j], lambda j: hid[j])
    for i in range(1, n_dp):
        psend[i - 1] = term[rpart(dp_peer(i)), :].astype(BF16)
    total[2] = term[rpart(my_dp), :]

    mate_copy(1).wait_recv()
    sx[1] = dot(pick2, tok2[...], NN).astype(BF16)
    dispatch_x(1, mate)

    def theirs(j):
        for i in range(1, n_dp):
            gu_copy(i, j, dp_peer(i)).wait_recv()
            if j == own and i == n_dp - 1:
                pl.when(odd == 0)(start_projections)
            row_grad(i, j)

    theirs(0)

    theirs(1)

    blocks(rx, n_ex - 2, x_s.at[0], x_r.at[0]).wait_recv()
    for j in range(LEVELS):
        xj = dot(spr[...], rx[lpart(j), :], NN).astype(BF16)
        if rk % 128:
            xp = dot(xj, bfull[...], NN).astype(BF16)
        for i in range(n_dp):
            if rk % 128:
                pj = dot(xp, rank_cols(dp_peer(i)), NN)
            else:
                pj = dot(xj, bfull[:, rpart(dp_peer(i))], NN)
            px[(i + n_dp - 1) % n_dp, j] = pj.astype(BF16)

    def start_projections():
        for i in range(1, n_dp):
            proj_copy(i, dp_peer(i)).start()
            px_copy(i, dp_peer(i)).start()

    pl.when(odd == 1)(start_projections)

    theirs(2)

    def x_term(s, i):
        left = px.at[n_dp - 1 + i]
        return project(lambda j: left[j], lambda j: gu[i, j, s])

    for s in range(2):
        total[s] = x_term(s, 0)

    def combine(i, piece):
        ret_all(i, piece).wait_recv()
        return dot(pick_v[i], rr[i, :, piece_cols(i, piece)], TN).astype(BF16)

    in_out[my_dp] = combine(0, 0)

    theirs(3)
    for i in range(1, n_dp):
        for piece in range(cut(i)):
            in_v[i - 1, :, piece_cols(i, piece)] = combine(i, piece)
            in_copy(i, piece, my_dp, dp_from(i)).start()

    for i in range(1, n_dp):
        proj_copy(i, dp_peer(i)).wait_recv()
        total[2] += prec[i - 1].astype(F32)
    for i in range(1, n_dp):
        px_copy(i, dp_peer(i)).wait_recv()
        for s in range(2):
            total[s] += x_term(s, i)

    for i in range(1, n_dp):
        down_copy(i, my_dp, dp_peer(i)).wait_send()
        base_copy(i, my_dp, dp_peer(i)).wait_send()
        ids_copy(i, dp_peer(i)).wait_send()
        px_copy(i, dp_peer(i)).wait_send()
        proj_copy(i, dp_peer(i)).wait_send()
        for j in range(LEVELS):
            gu_copy(i, j, dp_peer(i)).wait_send()
    for n in range(4):
        mate_copy(n).wait_send()
    for m in range(2):
        blocks(rg, half - 1, dy_s.at[m], dy_r.at[0]).wait_send()
        blocks(rx, half - 1, x_s.at[m], x_r.at[0]).wait_send()
    for i in range(n_dp):
        for piece in range(cut(i)):
            ret_all(i, piece).wait_send()
    for i in range(1, n_dp):
        for piece in range(cut(i)):
            in_copy(i, piece, my_dp, dp_from(i)).wait_send()
            in_copy(i, piece, dp_peer(i), dp_from(i)).wait_recv()


def finish(in_h, proj_h, in_ref, proj_ref, proj_s, in_s):
    parts, _, part = in_h.shape
    n = proj_h.shape[0]
    copies = [pltpu.make_async_copy(proj_h.at[t], proj_ref.at[0, t], proj_s.at[t]) for t in range(n)]
    for d in range(parts):
        cols = pl.ds(d * part, part)
        copies.append(pltpu.make_async_copy(in_h.at[d], in_ref.at[:, cols], in_s.at[d]))
    for copy in copies:
        copy.start()
    for copy in copies:
        copy.wait()


def body(
    tokens, out_grad, expert_ids, gate_probs, saved_pre, gate_weight, up_weight, down_weight, basis
):
    n_dp, n_ex = lax.axis_size("dp"), lax.axis_size("expert")
    tok_rows, width = tokens.shape
    topk = expert_ids.shape[1]
    slots, hidden2 = saved_pre.shape[2:]
    hidden = hidden2 // 2
    cap = slots // n_ex
    cp = max(16, 1 << (cap - 1).bit_length())
    rows = n_ex * cp
    nl = n_ex // LEVELS
    lrows = nl * cp
    lpad = -(-nl * cap // 16) * 16
    part = gate_weight.shape[1]
    rank = basis.shape[2]
    rk = rank // n_dp
    vmem = pl.BlockSpec(memory_space=pltpu.VMEM)
    hbm = pl.BlockSpec(memory_space=pl.ANY)
    dma = pltpu.SemaphoreType.DMA
    scratch = [
        pltpu.VMEM((topk, tok_rows), jnp.int32),
        pltpu.VMEM((topk, tok_rows), F32),
        pltpu.VMEM((tok_rows, width), BF16),
        pltpu.VMEM((tok_rows, width), BF16),
        pltpu.VMEM((tok_rows, width), BF16),
        pltpu.VMEM((tok_rows, width), BF16),
        pltpu.VMEM((topk, tok_rows), jnp.int32),
        pltpu.VMEM((topk, tok_rows), F32),
        pltpu.VMEM((n_dp - 1, topk, tok_rows), jnp.int32),
        pltpu.VMEM((n_dp, rows, tok_rows), BF16),
        pltpu.VMEM((2, rows // 2, width), BF16),
        pltpu.VMEM((2, rows // 2, width), BF16),
        pltpu.VMEM((rows, width), BF16),
        pltpu.VMEM((rows, width), BF16),
        pltpu.VMEM((LEVELS, lpad, width), BF16),
        pltpu.VMEM((lpad, lrows), BF16),
        pltpu.VMEM((width, hidden), BF16),
        pltpu.VMEM((width, rank), BF16),
        pltpu.VMEM((part, hidden), BF16),
        pltpu.VMEM((part, hidden), BF16),
        pltpu.VMEM((hidden, part), BF16),
        pltpu.VMEM((hidden, part), BF16),
        pltpu.VMEM((LEVELS, lpad, hidden2), BF16),
        pltpu.VMEM((LEVELS, lpad, hidden), F32),
        pltpu.VMEM((LEVELS, lpad, hidden), F32),
        pltpu.VMEM((LEVELS, lpad, hidden), BF16),
        pltpu.VMEM((n_dp, LEVELS, 2, lpad, hidden), BF16),
        pltpu.VMEM((2 * n_dp - 1, LEVELS, lpad, rk), BF16),
        pltpu.VMEM((LEVELS, lpad, rank), BF16),
        pltpu.VMEM((n_dp, LEVELS, lrows, part), BF16),
        pltpu.VMEM((n_dp, rows, part), BF16),
        pltpu.VMEM((n_dp - 1, tok_rows, part), BF16),
        pltpu.VMEM((n_dp - 1, rk, hidden), BF16),
        pltpu.VMEM((n_dp - 1, rk, hidden), BF16),
        pltpu.VMEM((rank, hidden), F32),
        dma((8,)), dma((LEVELS,)),
        dma((2,)), dma((LEVELS,)), dma((2,)), dma((1,)), dma((4,)), dma((4,)),
        dma((n_dp - 1,)), dma((n_dp - 1,)), dma((n_dp - 1,)), dma((n_dp - 1,)),
        dma((n_dp - 1, LEVELS)), dma((n_dp - 1, LEVELS)), dma((n_dp, 2)), dma((n_dp, 2)),
        dma((n_dp - 1,)), dma((n_dp - 1,)), dma((n_dp - 1,)), dma((n_dp - 1,)),
        dma((n_dp - 1, 2)), dma((n_dp - 1, 2)), dma((n_dp - 1,)), dma((n_dp - 1,)),
        pltpu.SemaphoreType.REGULAR,
    ]
    outputs = tok_rows * width * 2 + 3 * rk * hidden * 4
    in_part, proj = pl.pallas_call(
        functools.partial(kernel, n_dp, n_ex, cap, cp),
        out_shape=(pltpu.VMEM((n_dp, tok_rows, part), BF16), pltpu.VMEM((3, rk, hidden), F32)),
        in_specs=[hbm] * 9,
        out_specs=(vmem, vmem),
        scratch_shapes=scratch,
        compiler_params=pltpu.CompilerParams(
            collective_id=0, has_side_effects=True, vmem_limit_bytes=VMEM_BYTES - outputs
        ),
    )(
        expert_ids.T, gate_probs.T, tokens, out_grad, saved_pre,
        gate_weight, up_weight, down_weight, basis,
    )
    return pl.pallas_call(
        finish,
        out_shape=(
            jax.ShapeDtypeStruct((tok_rows, width), BF16),
            jax.ShapeDtypeStruct((1, 3, rk, hidden), F32),
        ),
        in_specs=[hbm, hbm],
        out_specs=(hbm, hbm),
        scratch_shapes=[dma((3,)), dma((n_dp,))],
        compiler_params=pltpu.CompilerParams(vmem_limit_bytes=1024 * 1024),
    )(in_part, proj)


def solution(mesh):
    return jax.shard_map(
        body,
        mesh=mesh,
        in_specs=(
            P(("dp", "expert"), None),
            P(("dp", "expert"), None),
            P(("dp", "expert"), None),
            P(("dp", "expert"), None),
            P("dp", "expert", None, None),
            P("expert", "dp", None),
            P("expert", "dp", None),
            P("expert", "dp", None),
            P("expert", "dp", None),
        ),
        out_specs=(P(("dp", "expert"), None), P("expert", None, "dp", None)),
        check_vma=False,
    )
```
